8 devices in a mesh: data: 1 (over z), sp: 8 (over y, x, core).
Axes of the slice: x: 2, y: 2, z: 1, core: 2. Of those that a mesh axis runs over, the one named last changes fastest.
Arguments:
- latents: bfloat16 [16, 64, 32, 384], P('data', 'sp')
- cotangent: bfloat16 [16, 64, 32, 384], P('data', 'sp')
- ln_params: bfloat16 [2, 4, 384], replicated
- w_qkv: bfloat16 [2, 384, 1152], replicated
- w_out: bfloat16 [2, 6, 64, 384], replicated
- w_up: bfloat16 [2, 384, 1536], replicated
- w_down: bfloat16 [2, 1536, 384], replicated
Outputs:
- output 1: bfloat16 [16, 64, 32, 384], P('data', 'sp')
- output 2: bfloat16 [16, 64, 32, 384], P('data', 'sp')
- output 3: float32 [2, 4, 384], P('data')
- output 4: float32 [2, 384, 1152], P('data')
- output 5: float32 [2, 6, 64, 384], P('data')
- output 6: float32 [2, 384, 1536], P('data')
- output 7: float32 [2, 1536, 384], P('data')
All inputs are finite; a program needn't handle non-finite values.
Results may differ from the reference program's by a relative error of at most 0.02.
Values are sent between devices in bfloat16 or wider.
A program may use at most 1 GiB of HBM per device.

```python
import jax
import jax.numpy as jnp
from jax import lax

VIDEOS = 16
FRAMES = 64
PATCHES = 32
MODEL_WIDTH = 384
NUM_HEADS = 6
HEAD_DIM = MODEL_WIDTH // NUM_HEADS


def setup_inputs(seed: int = 0, part: int = 0) -> dict:
    part_key = jax.random.fold_in(jax.random.key(seed), part)
    key_x, key_cot = jax.random.split(part_key)
    key_ln, key_qkv, key_out, key_up, key_down = jax.random.split(jax.random.key(seed + 1), 5)
    act_shape = (VIDEOS, FRAMES, PATCHES, MODEL_WIDTH)
    ln_base = jnp.array([1.0, 0.0, 1.0, 0.0], dtype=jnp.float32)[None, :, None]
    ln_noise = jax.random.normal(key_ln, (2, 4, MODEL_WIDTH), jnp.float32)
    qkv_draw = jax.random.normal(key_qkv, (2, MODEL_WIDTH, 3 * MODEL_WIDTH), jnp.float32)
    out_draw = jax.random.normal(key_out, (2, NUM_HEADS, HEAD_DIM, MODEL_WIDTH), jnp.float32)
    up_draw = jax.random.normal(key_up, (2, MODEL_WIDTH, 4 * MODEL_WIDTH), jnp.float32)
    down_draw = jax.random.normal(key_down, (2, 4 * MODEL_WIDTH, MODEL_WIDTH), jnp.float32)
    return {
        'latents': jax.random.normal(key_x, act_shape, jnp.float32).astype(jnp.bfloat16),
        'cotangent': jax.random.normal(key_cot, act_shape, jnp.float32).astype(jnp.bfloat16),
        'ln_params': (ln_base + 0.25 * ln_noise).astype(jnp.bfloat16),
        'w_qkv': (1.25 * MODEL_WIDTH ** -0.5 * qkv_draw).astype(jnp.bfloat16),
        'w_out': (MODEL_WIDTH ** -0.5 * out_draw).astype(jnp.bfloat16),
        'w_up': (MODEL_WIDTH ** -0.5 * up_draw).astype(jnp.bfloat16),
        'w_down': ((4 * MODEL_WIDTH) ** -0.5 * down_draw).astype(jnp.bfloat16),
    }


def layer_norm(resid32, ln_gain, ln_shift):
    row_mean = jnp.mean(resid32, axis=-1, keepdims=True)
    centered = resid32 - row_mean
    variance = jnp.mean(centered * centered, axis=-1, keepdims=True)
    return (centered * lax.rsqrt(variance + 1e-6) * ln_gain + ln_shift).astype(jnp.bfloat16)


def attend_group(seq_group):
    queries = seq_group[:, :, 0].astype(jnp.float32)
    keys_all = seq_group[:, :, 1].astype(jnp.float32)
    values_all = seq_group[:, :, 2].astype(jnp.float32)
    scores = jnp.einsum('nlhe,nmhe->nhlm', queries, keys_all) * HEAD_DIM ** -0.5
    attn_probs = jax.nn.softmax(scores, axis=-1).astype(jnp.bfloat16)
    return jnp.einsum('nhlm,nmhe->nlhe', attn_probs.astype(jnp.float32), values_all).astype(jnp.bfloat16)


def attention(qkv_heads, lead_axis):
    lead_first = jnp.moveaxis(qkv_heads, lead_axis, 0)
    attended = lax.map(jax.checkpoint(attend_group), lead_first)
    return jnp.moveaxis(attended, 0, lead_axis).reshape(VIDEOS, FRAMES, PATCHES, MODEL_WIDTH)


def dit_block(block_in, ln_f32, w_qkv, w_out, w_up, w_down, lead_axis):
    block_in32 = block_in.astype(jnp.float32)
    a_in = layer_norm(block_in32, ln_f32[0], ln_f32[1])
    qkv_heads = jnp.einsum('btsd,de->btse', a_in.astype(jnp.float32), w_qkv).astype(jnp.bfloat16)
    qkv_heads = qkv_heads.reshape(VIDEOS, FRAMES, PATCHES, 3, NUM_HEADS, HEAD_DIM)
    attn_out = attention(qkv_heads, lead_axis)
    attn_proj = jnp.einsum('btsd,de->btse', attn_out.astype(jnp.float32), w_out.reshape(MODEL_WIDTH, MODEL_WIDTH))
    hid32 = (block_in32 + attn_proj).astype(jnp.bfloat16).astype(jnp.float32)
    m_in = layer_norm(hid32, ln_f32[2], ln_f32[3])
    up_proj = jnp.einsum('btsd,de->btse', m_in.astype(jnp.float32), w_up)
    act_out = jax.nn.gelu(up_proj, approximate=True).astype(jnp.bfloat16)
    mlp_down = jnp.einsum('btse,ed->btsd', act_out.astype(jnp.float32), w_down)
    return (hid32 + mlp_down).astype(jnp.bfloat16)


def reference(latents, cotangent, ln_params, w_qkv, w_out, w_up, w_down):
    weights32 = [weight.astype(jnp.float32) for weight in (ln_params, w_qkv, w_out, w_up, w_down)]

    def forward(block_in, ln_f32, qkv_f32, out_f32, up_f32, down_f32):
        mid_act = dit_block(block_in, ln_f32[0], qkv_f32[0], out_f32[0], up_f32[0], down_f32[0], 1)
        return dit_block(mid_act, ln_f32[1], qkv_f32[1], out_f32[1], up_f32[1], down_f32[1], 2)

    y_out, pullback = jax.vjp(forward, latents, *weights32)
    grads_all = pullback(cotangent)
    return (y_out, grads_all[0], grads_all[1], grads_all[2], grads_all[3], grads_all[4], grads_all[5])
```

```python
import functools

import jax
import jax.numpy as jnp
import numpy as np
from jax import lax
from jax.experimental import pallas as pl
from jax.experimental.pallas import tpu as pltpu
from jax.sharding import PartitionSpec as P

BF16 = jnp.bfloat16
F32 = jnp.float32
N_DEV = 8
WIDTH = 384
HIDDEN = 4 * WIDTH
QKV = 3 * WIDTH
VIDEOS = 16
HALF = 8
ROWS = 256
NV = 2
STEP_ROWS = ROWS * NV
GROUP = 128
PAIRS = 3
SCALE = 0.125
LOG2E = 1.4426950408889634
GELU_C = 0.7978845608028654
GELU_C3 = GELU_C * 0.044715
VMEM_LIMIT = 62 * 1024 * 1024


def dot_nn(a, b):
    return lax.dot_general(a, b, (((1,), (0,)), ((), ())), preferred_element_type=F32)


def dot_nt(a, b):
    return lax.dot_general(a, b, (((1,), (1,)), ((), ())), preferred_element_type=F32)


def dot_tn(a, b):
    return lax.dot_general(a, b, (((0,), (0,)), ((), ())), preferred_element_type=F32)


def norm_stats(x32):
    centered = x32 - jnp.mean(x32, axis=-1, keepdims=True)
    inv_std = lax.rsqrt(jnp.mean(centered * centered, axis=-1, keepdims=True) + 1e-6)
    return centered * inv_std, inv_std


def norm_back(d_out32, normed, inv_std, gain):
    d_gain = jnp.sum(d_out32 * normed, axis=0, keepdims=True)
    d_shift = jnp.sum(d_out32, axis=0, keepdims=True)
    d_norm = d_out32 * gain
    d_center = d_norm - jnp.mean(d_norm, axis=-1, keepdims=True)
    d_in = inv_std * (d_center - normed * jnp.mean(d_norm * normed, axis=-1, keepdims=True))
    return d_in, d_gain, d_shift


def gelu_parts(x):
    x2 = x * x
    t = jnp.tanh(x * (GELU_C + GELU_C3 * x2))
    half = 0.5 + 0.5 * t
    slope = half + (x * (0.5 - 0.5 * (t * t))) * (GELU_C + (3.0 * GELU_C3) * x2)
    return x * half, slope


def gelu_value(x):
    t = jnp.tanh(x * (GELU_C + GELU_C3 * (x * x)))
    return x * (0.5 + 0.5 * t)


def lane_masks():
    lane = lax.broadcasted_iota(jnp.int32, (1, GROUP), 1)
    low = (lane < GROUP // 2)
    m_low = jnp.where(low, 1.0, 0.0).astype(BF16)
    m_high = jnp.where(low, 0.0, 1.0).astype(BF16)
    return low, m_low, m_high


def split_heads(k, m_low, m_high):
    return jnp.concatenate([k * m_low, k * m_high], axis=0)


GROUPS = STEP_ROWS // GROUP
BLOCKS = [(g, pair) for g in range(GROUPS) for pair in range(PAIRS)]


def rows_of(g):
    return pl.ds(g * GROUP, GROUP)


def part(kind, pair):
    return pl.ds(kind * WIDTH + pair * GROUP, GROUP)


def both(pair):
    return pl.ds(pair * 2 * GROUP, 2 * GROUP)


def attend(qkv_ref, bias_ref, p_ref, o_ref, s_ref):
    low, m_low, m_high = lane_masks()
    for g, pair in BLOCKS:
        k2 = split_heads(qkv_ref[rows_of(g), part(1, pair)], m_low, m_high)
        s_ref[rows_of(g), both(pair)] = dot_nt(qkv_ref[rows_of(g), part(0, pair)], k2) * (SCALE * LOG2E) + bias_ref[...]
    for g, pair in BLOCKS:
        s = s_ref[rows_of(g), both(pair)]
        probs = []
        for h in range(2):
            s_h = s[:, h * GROUP:(h + 1) * GROUP]
            e_h = jnp.exp2(s_h - jnp.max(s_h, axis=-1, keepdims=True))
            probs.append(e_h * (1.0 / jnp.sum(e_h, axis=-1, keepdims=True)))
        p_ref[rows_of(g), both(pair)] = jnp.concatenate(probs, axis=1).astype(BF16)
    for g, pair in BLOCKS:
        v2 = split_heads(qkv_ref[rows_of(g), part(2, pair)], m_low, m_high)
        o_ref[rows_of(g), part(0, pair)] = dot_nn(p_ref[rows_of(g), both(pair)], v2).astype(BF16)


def attend_back(qkv_ref, p_ref, do_ref, dqkv_ref, dp_ref):
    low, m_low, m_high = lane_masks()
    for g, pair in BLOCKS:
        do = do_ref[rows_of(g), part(0, pair)]
        v2 = split_heads(qkv_ref[rows_of(g), part(2, pair)], m_low, m_high)
        dp_ref[rows_of(g), both(pair)] = dot_nt(do, v2).astype(BF16)
        dv = dot_tn(p_ref[rows_of(g), both(pair)], do)
        dqkv_ref[rows_of(g), part(2, pair)] = jnp.where(low, dv[:GROUP], dv[GROUP:]).astype(BF16)
    for g, pair in BLOCKS:
        p32 = p_ref[rows_of(g), both(pair)].astype(F32)
        t = dp_ref[rows_of(g), both(pair)].astype(F32) * p32
        ds = []
        for h in range(2):
            half = slice(h * GROUP, (h + 1) * GROUP)
            ds.append(t[:, half] - p32[:, half] * jnp.sum(t[:, half], axis=-1, keepdims=True))
        dp_ref[rows_of(g), both(pair)] = jnp.concatenate(ds, axis=1).astype(BF16)
    for g, pair in BLOCKS:
        ds = dp_ref[rows_of(g), both(pair)]
        k2 = split_heads(qkv_ref[rows_of(g), part(1, pair)], m_low, m_high)
        dqkv_ref[rows_of(g), part(0, pair)] = (dot_nn(ds, k2) * SCALE).astype(BF16)
        dk = dot_tn(ds, qkv_ref[rows_of(g), part(0, pair)])
        dqkv_ref[rows_of(g), part(1, pair)] = (jnp.where(low, dk[:GROUP], dk[GROUP:]) * SCALE).astype(BF16)


CHUNK = 512
CHUNKS = HIDDEN // CHUNK


def cut(c):
    return pl.ds(c * CHUNK, CHUNK)


def gains(ln_ref):
    ln = ln_ref[...].astype(F32)
    return [ln[r:r + 1, :] for r in range(4)]


def spatial_forward_kernel(n_alias, *refs):
    x_ref, dy_ref, ln_ref, wqkv_ref, wout_ref, wup_ref, wdown_ref, bias_ref, perm_ref = refs[:9]
    out_ref, h_ref, o_ref, qkv_ref, p_ref, act_ref, s_ref = refs[9 + n_alias:]
    gain1, shift1, gain2, shift2 = gains(ln_ref)
    normed, _ = norm_stats(x_ref[...].astype(F32))
    a_in = (normed * gain1 + shift1).astype(BF16)
    for c in range(3):
        cols = pl.ds(c * WIDTH, WIDTH)
        qkv_ref[:, cols] = dot_nn(a_in, wqkv_ref[:, cols]).astype(BF16)
    attend(qkv_ref, bias_ref, p_ref, o_ref, s_ref)
    h_ref[...] = (x_ref[...].astype(F32) + dot_nn(o_ref[...], wout_ref[...])).astype(BF16)
    normed, _ = norm_stats(h_ref[...].astype(F32))
    m_in = (normed * gain2 + shift2).astype(BF16)
    for c in range(CHUNKS):
        act_ref[:, cut(c)] = gelu_value(dot_nn(m_in, wup_ref[:, cut(c)])).astype(BF16)
    out = (h_ref[...].astype(F32) + dot_nn(act_ref[...], wdown_ref[...])).astype(BF16)
    for v in range(NV):
        moved = dot_nn(perm_ref[...], out[v * ROWS:(v + 1) * ROWS]).astype(BF16)
        for d in range(N_DEV):
            out_ref[d, 0, v] = moved[d * 32:(d + 1) * 32]
        moved = dot_nn(perm_ref[...], dy_ref[pl.ds(v * ROWS, ROWS), :]).astype(BF16)
        for d in range(N_DEV):
            out_ref[d, 1, v] = moved[d * 32:(d + 1) * 32]


def add_blocks(sum_ref, first, product):
    for c in range(product.shape[1] // WIDTH):
        rows = pl.ds(first + c * WIDTH, WIDTH)
        sum_ref[rows, :] += product[:, c * WIDTH:(c + 1) * WIDTH]


def tail_backward(dv_ref, o_ref, m_ref, normed, inv_std, gain2, gp_ref, act_ref, dup_ref, do_ref,
                  wout_ref, wup_ref, wdown_ref, sum_ref):
    add_blocks(sum_ref, ROW_DOWN, dot_tn(dv_ref[...], act_ref[...]))
    for c in range(CHUNKS):
        d_act = dot_nt(dv_ref[...], wdown_ref[cut(c), :]).astype(BF16).astype(F32)
        dup_ref[:, cut(c)] = (d_act * gp_ref[:, cut(c)]).astype(BF16)
    add_blocks(sum_ref, ROW_UP, dot_tn(m_ref[...], dup_ref[...]))
    d_m = dot_nt(dup_ref[...], wup_ref[...]).astype(BF16).astype(F32)
    d_h, g_gain, g_shift = norm_back(d_m, normed, inv_std, gain2)
    dv_ref[...] = (d_h + dv_ref[...].astype(F32)).astype(BF16)
    add_blocks(sum_ref, ROW_OUT, dot_tn(o_ref[...], dv_ref[...]))
    do_ref[...] = dot_nt(dv_ref[...], wout_ref[...]).astype(BF16)
    return g_gain, g_shift


def qkv_backward(u32, a_ref, dh_ref, dqkv_ref, gain1, wqkv_ref, sum_ref):
    normed, inv_std = norm_stats(u32)
    add_blocks(sum_ref, ROW_QKV, dot_tn(a_ref[...], dqkv_ref[...]))
    d_a = dot_nt(dqkv_ref[...], wqkv_ref[...]).astype(BF16).astype(F32)
    d_in, g_gain, g_shift = norm_back(d_a, normed, inv_std, gain1)
    return (d_in + dh_ref[...].astype(F32)).astype(BF16), g_gain, g_shift


def up_forward(h32, gain2, shift2, m_ref, wup_ref, act_ref, gp_ref):
    normed, inv_std = norm_stats(h32)
    m_ref[...] = (normed * gain2 + shift2).astype(BF16)
    for c in range(CHUNKS):
        act, slope = gelu_parts(dot_nn(m_ref[...], wup_ref[:, cut(c)]))
        act_ref[:, cut(c)] = act.astype(BF16)
        gp_ref[:, cut(c)] = slope
    return normed, inv_std


def add_ln_sums(ref, first, sums):
    for r, g in enumerate(sums):
        ref[first + r:first + r + 1, :] += g


def temporal_kernel(n_sums, *refs):
    act_in_ref, ln_ref, wqkv_ref, wout_ref, wup_ref, wdown_ref, bias_ref = refs[:7]
    sums_in = refs[7:7 + n_sums]
    (out_ref, sum_ref, u_ref, dv_ref, a_ref, qkv_ref, p_ref, o_ref, m_ref, act_ref,
     dup_ref, do_ref, dqkv_ref, dp_ref, gp_ref, s_ref) = refs[7 + n_sums:]

    @pl.when(pl.program_id(0) == 0)
    def _():
        sum_ref[...] = sums_in[0][...] if n_sums else jnp.zeros_like(sum_ref)

    gain1, shift1, gain2, shift2 = gains(ln_ref)
    places = [(v, g, s) for v in range(NV) for g in range(2) for s in range(N_DEV)]
    for v, g, s in places:
        dst = pl.ds(v * ROWS + g * GROUP + s * 16, 16)
        u_ref[dst, :] = act_in_ref[s, 0, v, pl.ds(g * 16, 16), :]
        dv_ref[dst, :] = act_in_ref[s, 1, v, pl.ds(g * 16, 16), :]
    normed1, _ = norm_stats(u_ref[...].astype(F32))
    a_ref[...] = (normed1 * gain1 + shift1).astype(BF16)
    for c in range(3):
        cols = pl.ds(c * WIDTH, WIDTH)
        qkv_ref[:, cols] = dot_nn(a_ref[...], wqkv_ref[:, cols]).astype(BF16)
    attend(qkv_ref, bias_ref, p_ref, o_ref, s_ref)
    h = (u_ref[...].astype(F32) + dot_nn(o_ref[...], wout_ref[...])).astype(BF16)
    h32 = h.astype(F32)
    normed, inv_std = up_forward(h32, gain2, shift2, m_ref, wup_ref, act_ref, gp_ref)
    out = (h32 + dot_nn(act_ref[...], wdown_ref[...])).astype(BF16)
    for v, g, s in places:
        src = v * ROWS + g * GROUP + s * 16
        out_ref[s, 0, v, pl.ds(g * 16, 16), :] = out[src:src + 16]
    g_gain2, g_shift2 = tail_backward(dv_ref, o_ref, m_ref, normed, inv_std, gain2, gp_ref, act_ref, dup_ref, do_ref,
                                      wout_ref, wup_ref, wdown_ref, sum_ref)
    attend_back(qkv_ref, p_ref, do_ref, dqkv_ref, dp_ref)
    d_in, g_gain1, g_shift1 = qkv_backward(u_ref[...].astype(F32), a_ref, dv_ref, dqkv_ref, gain1, wqkv_ref, sum_ref)
    add_ln_sums(sum_ref, SUM_ROWS, (g_gain1, g_shift1, g_gain2, g_shift2))
    for v, g, s in places:
        src = v * ROWS + g * GROUP + s * 16
        out_ref[s, 1, v, pl.ds(g * 16, 16), :] = d_in[src:src + 16]


def position():
    me = lax.axis_index('sp')
    y, x, c = me // 4, (me // 2) % 2, me % 2
    return me, y, x, c, 4 * y + 2 * x + 1 - c, 4 * y + 2 * (1 - x) + c, 4 * (1 - y) + 2 * x + c


def span(k, idx, n):
    return pl.ds(pl.multiple_of(k * LAP_ROWS + idx * BLOCK, 16), n * BLOCK)


def slot(k, idx, n):
    return pl.ds((k * SLOTS + idx) * BLOCK, n * BLOCK)


def reduce_copies(phase, k, w_ref, r_ref, sems):
    _, y, x, c, partner, xn, yn = position()
    own0, own1 = c * 8 + x * 2, c * 8 + 4 + y * 2
    moves = (
        [((1 - c) * 8, 8, 0, partner)],
        [(c * 8 + (1 - x) * 2, 2, 8, xn), (c * 8 + 4 + (1 - y) * 2, 2, 10, yn)],
        [(own0 + 1 - y, 1, 12, yn), (own1 + 1 - x, 1, 13, xn)],
        [(own0 + y, 1, None, yn), (own1 + x, 1, None, xn)],
        [(own0, 2, None, xn), (own1, 2, None, yn)],
        [(c * 8, 8, None, partner)],
    )[phase]
    copies = []
    for j, (idx, n, place, device) in enumerate(moves):
        src = w_ref.at[span(k, idx, n), :]
        dst = src if place is None else r_ref.at[slot(k, place, n), :]
        copies.append(pltpu.make_async_remote_copy(
            src_ref=src, dst_ref=dst, send_sem=sems.at[0, phase, k, j], recv_sem=sems.at[1, phase, k, j],
            device_id={'sp': device}, device_id_type=pl.DeviceIdType.MESH))
    return copies


def reduce_peers(phase):
    _, _, _, _, partner, xn, yn = position()
    return ([partner], [xn, yn], [yn, xn])[phase]


def reduce_start(phase, k, w_ref, r_ref, sems, credits):
    copies = reduce_copies(phase, k, w_ref, r_ref, sems)
    for j, copy in enumerate(copies):
        if phase >= 3:
            pl.semaphore_wait(credits.at[5 - phase, k, j], 1)
        copy.start()


def reduce_finish(phase, k, w_ref, r_ref, sems, credits):
    for j, copy in enumerate(reduce_copies(phase, k, w_ref, r_ref, sems)):
        copy.wait()
        if phase < 3:
            pl.semaphore_signal(credits.at[phase, k, j], inc=1, device_id={'sp': reduce_peers(phase)[j]},
                                device_id_type=pl.DeviceIdType.MESH)
    _, y, x, c, _, _, _ = position()
    own0, own1 = c * 8 + x * 2, c * 8 + 4 + y * 2
    adds = ([(c * 8, 8, 0)], [(own0, 2, 8), (own1, 2, 10)], [(own0 + y, 1, 12), (own1 + x, 1, 13)], (), (), ())[phase]
    for idx, n, place in adds:
        def body(i, carry):
            w_rows = pl.ds(pl.multiple_of(k * LAP_ROWS + (idx + i) * BLOCK, 16), BLOCK)
            r_rows = pl.ds(pl.multiple_of((k * SLOTS + place + i) * BLOCK, 16), BLOCK)
            w_ref[w_rows, :] += r_ref[r_rows, :]
            return carry
        lax.fori_loop(0, n, body, 0)


def enter():
    me = lax.axis_index('sp')
    barrier = pltpu.get_barrier_semaphore()
    for d in range(1, N_DEV):
        pl.semaphore_signal(barrier, inc=1, device_id={'sp': lax.rem(me + d, N_DEV)},
                            device_id_type=pl.DeviceIdType.MESH)
    pl.semaphore_wait(barrier, N_DEV - 1)


def ln_copies(ln_ref, sems):
    me = lax.axis_index('sp')
    return [pltpu.make_async_remote_copy(
        src_ref=ln_ref.at[me], dst_ref=ln_ref.at[me], send_sem=sems.at[0, d], recv_sem=sems.at[1, d],
        device_id={'sp': lax.rem(me + d, N_DEV)}, device_id_type=pl.DeviceIdType.MESH) for d in range(1, N_DEV)]


def spatial_backward_kernel(*refs):
    (back_ref, x_ref, h_ref, o_ref, qkv_ref, p_ref,
     ln_ref, wqkv_ref, wout_ref, wup_ref, wdown_ref, perm_ref, gt_ref) = refs[:13]
    (y_ref, dx_ref, rt_ref, rs_ref, lnsum_ref, dv_ref, a_ref, m_ref, act_ref, dup_ref, do_ref, dqkv_ref, dp_ref, gp_ref,
     sum_ref, t_ref, rb_s_ref, rb_t_ref, ln_s_ref, ln_all_ref, sems_s, sems_t, credits_s, credits_t,
     sems_ln, sems_io) = refs[13:]
    step, last = pl.program_id(0), pl.num_programs(0) - 1
    me = lax.axis_index('sp')
    load_t = pltpu.make_async_copy(gt_ref.at[pl.ds(0, SUM_ROWS), :], t_ref, sems_io.at[0])
    load_ln = pltpu.make_async_copy(gt_ref.at[pl.ds(SUM_ROWS, 8), :], ln_all_ref.at[me, pl.ds(0, 8), :], sems_io.at[1])
    args_t, args_s = (t_ref, rb_t_ref, sems_t, credits_t), (sum_ref, rb_s_ref, sems_s, credits_s)

    @pl.when(step == 0)
    def _():
        enter()
        load_t.start()
        load_ln.start()
        sum_ref[...] = jnp.zeros_like(sum_ref)
        ln_s_ref[...] = jnp.zeros_like(ln_s_ref)

    @pl.when(step == 1)
    def _():
        load_t.wait()
        load_ln.wait()
        for k in range(LAPS):
            reduce_start(0, k, *args_t)

    for phase, at in enumerate(T_FINISH):
        @pl.when(step == at)
        def _(phase=phase):
            for k in range(LAPS):
                reduce_finish(phase, k, *args_t)
                reduce_start(phase + 1, k, *args_t)

    gain1, shift1, gain2, shift2 = gains(ln_ref)
    for v in range(NV):
        rows = pl.ds(v * ROWS, ROWS)
        dv_ref[rows, :] = dot_tn(perm_ref[...], back_ref[:, 1, v].reshape(ROWS, WIDTH)).astype(BF16)
        y_ref[rows, :] = dot_tn(perm_ref[...], back_ref[:, 0, v].reshape(ROWS, WIDTH)).astype(BF16)
    normed1, _ = norm_stats(x_ref[...].astype(F32))
    a_ref[...] = (normed1 * gain1 + shift1).astype(BF16)
    normed, inv_std = up_forward(h_ref[...].astype(F32), gain2, shift2, m_ref, wup_ref, act_ref, gp_ref)
    g_gain2, g_shift2 = tail_backward(dv_ref, o_ref, m_ref, normed, inv_std, gain2, gp_ref, act_ref, dup_ref, do_ref,
                                      wout_ref, wup_ref, wdown_ref, sum_ref)
    attend_back(qkv_ref, p_ref, do_ref, dqkv_ref, dp_ref)
    d_in, g_gain1, g_shift1 = qkv_backward(x_ref[...].astype(F32), a_ref, dv_ref, dqkv_ref, gain1, wqkv_ref, sum_ref)
    add_ln_sums(ln_s_ref, 0, (g_gain1, g_shift1, g_gain2, g_shift2))
    dx_ref[...] = d_in

    @pl.when(step == last)
    def _():
        ln_all_ref[me, pl.ds(8, 8), :] = ln_s_ref[...]
        for copy in ln_copies(ln_all_ref, sems_ln):
            copy.start()
        for k in range(LAPS):
            reduce_start(0, k, *args_s)
        for k in range(LAPS):
            reduce_finish(4, k, *args_t)
            reduce_start(5, k, *args_t)
        for phase in range(5):
            for k in range(LAPS):
                reduce_finish(phase, k, *args_s)
                reduce_start(phase + 1, k, *args_s)
            if phase == 0:
                for k in range(LAPS):
                    reduce_finish(5, k, *args_t)
                pltpu.make_async_copy(t_ref, rt_ref, sems_io.at[0]).start()
            if phase == 1:
                for copy in ln_copies(ln_all_ref, sems_ln):
                    copy.wait()
                total = ln_all_ref[0]
                for d in range(1, N_DEV):
                    total += ln_all_ref[d]
                lnsum_ref[...] = total
        outs = []
        for k in range(LAPS):
            reduce_finish(5, k, *args_s)
            lap = pl.ds(k * LAP_ROWS, LAP_ROWS)
            outs.append(pltpu.make_async_copy(sum_ref.at[lap, :], rs_ref.at[lap, :], sems_io.at[1 + k]))
            outs[-1].start()
        pltpu.make_async_copy(t_ref, rt_ref, sems_io.at[0]).wait()
        for copy in outs:
            copy.wait()


def assemble_kernel(s_ref, t_ref, ln_ref, qkv_ref, out_ref, up_ref, down_ref, gln_ref):
    block, part_id = pl.program_id(0), pl.program_id(1)
    moved = jnp.where(block == 0, s_ref[...], t_ref[...])

    @pl.when(part_id < 3)
    def _():
        qkv_ref[...] = moved

    @pl.when(part_id == 3)
    def _():
        out_ref[...] = moved
        gln_ref[...] = jnp.where(block == 0, ln_ref[8:12, :], ln_ref[0:4, :])

    @pl.when((part_id >= 4) & (part_id < 8))
    def _():
        up_ref[...] = moved

    @pl.when(part_id >= 8)
    def _():
        down_ref[...] = moved.T


def full(shape):
    return pl.BlockSpec(shape, lambda i: (0,) * len(shape), pipeline_mode=pl.Buffered(1))


def weight_specs(block):
    shapes = [(4, WIDTH), (WIDTH, QKV), (WIDTH, WIDTH), (WIDTH, HIDDEN), (HIDDEN, WIDTH)]
    return [pl.BlockSpec((None,) + s, lambda i: (block, 0, 0), pipeline_mode=pl.Buffered(1)) for s in shapes]


def rows_spec(width, first=0):
    return pl.BlockSpec((STEP_ROWS, width), lambda i: (i + first, 0))


def pair_spec():
    return pl.BlockSpec((N_DEV, 2, NV, 32, WIDTH), lambda i: (0, 0, i, 0, 0))


ANY = pl.BlockSpec(memory_space=pl.ANY)


def params():
    return pltpu.CompilerParams(dimension_semantics=("arbitrary",), vmem_limit_bytes=VMEM_LIMIT)


def cost(us, mib):
    return pl.CostEstimate(flops=int(us * 9e8), bytes_accessed=int(mib * 2 ** 20), transcendentals=0)


def sds(shape, dtype):
    return jax.ShapeDtypeStruct(shape, dtype)


def vm(width, dtype=BF16):
    return pltpu.VMEM((STEP_ROWS, width), dtype)


TOKENS = VIDEOS * ROWS
PROBS = 6 * GROUP
EXCHANGE = (N_DEV, 2, HALF, 32, WIDTH)
ROW_QKV, ROW_OUT, ROW_UP, ROW_DOWN = 0, 3 * WIDTH, 4 * WIDTH, 8 * WIDTH
SUM_ROWS = 12 * WIDTH
LAPS = 2
LAP_ROWS = SUM_ROWS // LAPS
BLOCK = LAP_ROWS // 16
SLOTS = 14
T_FINISH = (2, 4, 5, 6)


def spatial_forward_call(half, x, dy, weights, bias, perm, saved):
    first = half * (HALF // NV)
    widths = (WIDTH, WIDTH, QKV, PROBS)
    n_in = 9
    return pl.pallas_call(
        functools.partial(spatial_forward_kernel, len(saved)), grid=(HALF // NV,), name="spatial_fwd",
        in_specs=[rows_spec(WIDTH, first)] * 2 + weight_specs(0) + [full((GROUP, 2 * GROUP)), full((ROWS, ROWS))]
        + [ANY] * len(saved),
        out_specs=[pair_spec()] + [rows_spec(w, first) for w in widths],
        out_shape=[sds(EXCHANGE, BF16)] + [sds((TOKENS, w), BF16) for w in widths],
        scratch_shapes=[vm(HIDDEN), vm(PROBS, F32)],
        input_output_aliases={n_in + i: 1 + i for i in range(len(saved))},
        compiler_params=params(), cost_estimate=cost(25, 16),
    )(x, dy, *weights, bias, perm, *saved)


def temporal_call(acts, weights, bias, sums):
    n_in = 7
    return pl.pallas_call(
        functools.partial(temporal_kernel, len(sums)), grid=(HALF // NV,), name="temporal",
        in_specs=[pair_spec()] + weight_specs(1) + [full((GROUP, 2 * GROUP))] + [full((SUM_ROWS + 8, WIDTH))] * len(sums),
        out_specs=[pair_spec(), full((SUM_ROWS + 8, WIDTH))],
        out_shape=[sds(EXCHANGE, BF16), sds((SUM_ROWS + 8, WIDTH), F32)],
        scratch_shapes=[vm(w) for w in (WIDTH, WIDTH, WIDTH, QKV, PROBS, WIDTH, WIDTH, HIDDEN, HIDDEN, WIDTH, QKV, PROBS)]
        + [vm(HIDDEN, F32), vm(PROBS, F32)],
        input_output_aliases={n_in + i: 1 + i for i in range(len(sums))},
        compiler_params=params(), cost_estimate=cost(60, 20),
    )(acts, *weights, bias, *sums)


def spatial_backward_call(back, x, saved, weights, perm, sum_t):
    return pl.pallas_call(
        spatial_backward_kernel, grid=(VIDEOS // NV,), name="spatial_bwd",
        in_specs=[pl.BlockSpec((N_DEV, 2, NV, 32, WIDTH), lambda i: (0, 0, i, 0, 0))]
        + [rows_spec(w) for w in (WIDTH, WIDTH, WIDTH, QKV, PROBS)] + weight_specs(0) + [full((ROWS, ROWS)), ANY],
        out_specs=[rows_spec(WIDTH)] * 2 + [ANY, ANY, full((16, WIDTH))],
        out_shape=[sds((TOKENS, WIDTH), BF16)] * 2 + [sds((SUM_ROWS, WIDTH), F32)] * 2 + [sds((16, WIDTH), F32)],
        scratch_shapes=[vm(w) for w in (WIDTH, WIDTH, WIDTH, HIDDEN, HIDDEN, WIDTH, QKV, PROBS)] + [vm(HIDDEN, F32)]
        + [pltpu.VMEM((SUM_ROWS, WIDTH), F32)] * 2 + [pltpu.VMEM((LAPS * SLOTS * BLOCK, WIDTH), F32)] * 2
        + [pltpu.VMEM((8, WIDTH), F32), pltpu.VMEM((N_DEV, 16, WIDTH), F32)]
        + [pltpu.SemaphoreType.DMA((2, 6, LAPS, 2))] * 2 + [pltpu.SemaphoreType.REGULAR((3, LAPS, 2))] * 2
        + [pltpu.SemaphoreType.DMA((2, N_DEV)), pltpu.SemaphoreType.DMA((4,))],
        compiler_params=pltpu.CompilerParams(dimension_semantics=("arbitrary",), vmem_limit_bytes=VMEM_LIMIT,
                                             collective_id=1, has_side_effects=True),
        cost_estimate=cost(160, 60),
    )(back, x, *saved, *weights, perm, sum_t)


def assemble_call(sum_s, sum_t, ln_sums):
    def block(clip):
        return lambda b, j: (b,) + clip(j)
    grads = [(2, WIDTH, QKV), (2, WIDTH, WIDTH), (2, WIDTH, HIDDEN), (2, HIDDEN, WIDTH), (2, 4, WIDTH)]
    maps = [lambda j: (0, jnp.minimum(j, 2)), lambda j: (0, 0), lambda j: (0, jnp.clip(j - 4, 0, 3)),
            lambda j: (jnp.clip(j - 8, 0, 3), 0)]
    return pl.pallas_call(
        assemble_kernel, grid=(2, 12), name="assemble",
        in_specs=[pl.BlockSpec((WIDTH, WIDTH), lambda b, j: (jnp.where(b == 0, j, 11), 0)),
                  pl.BlockSpec((WIDTH, WIDTH), lambda b, j: (jnp.where(b == 0, 0, j), 0)),
                  pl.BlockSpec((16, WIDTH), lambda b, j: (0, 0))],
        out_specs=[pl.BlockSpec((None, WIDTH, WIDTH), block(m)) for m in maps]
        + [pl.BlockSpec((None, 4, WIDTH), lambda b, j: (b, 0, 0))],
        out_shape=[sds(g, F32) for g in grads],
        compiler_params=pltpu.CompilerParams(dimension_semantics=("arbitrary", "arbitrary"), vmem_limit_bytes=VMEM_LIMIT),
        cost_estimate=cost(10, 28),
    )(sum_s, sum_t, ln_sums)


def constants():
    row = np.arange(ROWS)
    dev, patch, frame = row // 32, (row // 8) % 4, row % 8
    perm = np.zeros((ROWS, ROWS), np.float32)
    perm[row, frame * 32 + dev * 4 + patch] = 1.0
    r = np.arange(GROUP)
    frame_of = r // 32
    patch_of = (r // 8) % 2
    bias_s = np.where(frame_of[:, None] == frame_of[None], 0.0, -np.inf).astype(np.float32)
    bias_t = np.where(patch_of[:, None] == patch_of[None], 0.0, -np.inf).astype(np.float32)
    return perm, np.concatenate([bias_s] * 2, 1), np.concatenate([bias_t] * 2, 1)


def swap(arr):
    return lax.all_to_all(arr, 'sp', 0, 0, tiled=True)


def device_step(latents, cotangent, ln_params, w_qkv, w_out, w_up, w_down):
    perm, bias_s, bias_t = constants()
    perm = jnp.asarray(perm, BF16)
    bias_s, bias_t = jnp.asarray(bias_s), jnp.asarray(bias_t)
    weights = (ln_params, w_qkv, w_out.reshape(2, WIDTH, WIDTH), w_up, w_down)
    x = latents.reshape(TOKENS, WIDTH)
    dy = cotangent.reshape(TOKENS, WIDTH)

    act_a, *saved = spatial_forward_call(0, x, dy, weights, bias_s, perm, ())
    act_a = swap(act_a)
    act_b, *saved = spatial_forward_call(1, x, dy, weights, bias_s, perm, saved)
    act_b = swap(act_b)
    back_a, sum_t = temporal_call(act_a, weights, bias_t, ())
    back_a = swap(back_a)
    back_b, sum_t = temporal_call(act_b, weights, bias_t, (sum_t,))
    back_b = swap(back_b)
    back = jnp.concatenate([back_a, back_b], axis=2)
    y, dx, sum_t, sum_s, ln_sums = spatial_backward_call(back, x, saved, weights, perm, sum_t)
    g_qkv, g_out, g_up, g_down, g_ln = assemble_call(sum_s, sum_t, ln_sums)
    g_out = g_out.reshape(2, 6, 64, WIDTH)
    shape = latents.shape
    return y.reshape(shape), dx.reshape(shape), g_ln, g_qkv, g_out, g_up, g_down


def solution(mesh):
    act_spec = P('data', 'sp', None, None)
    replicated = P()
    part_spec = P('data')
    return jax.shard_map(device_step, mesh=mesh,
                         in_specs=(act_spec, act_spec, replicated, replicated, replicated, replicated, replicated),
                         out_specs=(act_spec, act_spec, part_spec, part_spec, part_spec, part_spec, part_spec),
                         check_vma=False)
```

```python
import functools

import jax
import jax.numpy as jnp
import numpy as np
from jax import lax
from jax.experimental import pallas as pl
from jax.experimental.pallas import tpu as pltpu
from jax.sharding import PartitionSpec as P

BF16 = jnp.bfloat16
F32 = jnp.float32
N_DEV = 8
WIDTH = 384
HIDDEN = 4 * WIDTH
QKV = 3 * WIDTH
VIDEOS = 16
ROWS = 256
NV = 2
STEP_ROWS = ROWS * NV
GROUP = 128
PAIRS = 3
SCALE = 0.125
LOG2E = 1.4426950408889634
STEPS = VIDEOS // NV
GELU_C = 0.7978845608028654
GELU_C3 = GELU_C * 0.044715
VMEM_LIMIT = 62 * 1024 * 1024


def dot_nn(a, b):
    return lax.dot_general(a, b, (((1,), (0,)), ((), ())), preferred_element_type=F32)


def dot_nt(a, b):
    return lax.dot_general(a, b, (((1,), (1,)), ((), ())), preferred_element_type=F32)


def dot_tn(a, b):
    return lax.dot_general(a, b, (((0,), (0,)), ((), ())), preferred_element_type=F32)


def norm_stats(x32):
    centered = x32 - jnp.mean(x32, axis=-1, keepdims=True)
    inv_std = lax.rsqrt(jnp.mean(centered * centered, axis=-1, keepdims=True) + 1e-6)
    return centered * inv_std, inv_std


def norm_back(d_out32, normed, inv_std, gain):
    d_gain = jnp.sum(d_out32 * normed, axis=0, keepdims=True)
    d_shift = jnp.sum(d_out32, axis=0, keepdims=True)
    d_norm = d_out32 * gain
    d_center = d_norm - jnp.mean(d_norm, axis=-1, keepdims=True)
    d_in = inv_std * (d_center - normed * jnp.mean(d_norm * normed, axis=-1, keepdims=True))
    return d_in, d_gain, d_shift


def gelu_parts(x):
    x2 = x * x
    t = jnp.tanh(x * (GELU_C + GELU_C3 * x2))
    half = 0.5 + 0.5 * t
    slope = half + (x * (0.5 - 0.5 * (t * t))) * (GELU_C + (3.0 * GELU_C3) * x2)
    return x * half, slope


def gelu_value(x):
    t = jnp.tanh(x * (GELU_C + GELU_C3 * (x * x)))
    return x * (0.5 + 0.5 * t)


def lane_masks():
    lane = lax.broadcasted_iota(jnp.int32, (1, GROUP), 1)
    low = (lane < GROUP // 2)
    m_low = jnp.where(low, 1.0, 0.0).astype(BF16)
    m_high = jnp.where(low, 0.0, 1.0).astype(BF16)
    return low, m_low, m_high


def split_heads(k, m_low, m_high):
    return jnp.concatenate([k * m_low, k * m_high], axis=0)


GROUPS = STEP_ROWS // GROUP
BLOCKS = [(g, pair) for g in range(GROUPS) for pair in range(PAIRS)]


def rows_of(g):
    return pl.ds(g * GROUP, GROUP)


def part(kind, pair):
    return pl.ds(kind * WIDTH + pair * GROUP, GROUP)


def both(pair):
    return pl.ds(pair * 2 * GROUP, 2 * GROUP)


def attend(qkv_ref, bias_ref, p_ref, o_ref, s_ref):
    low, m_low, m_high = lane_masks()
    for g, pair in BLOCKS:
        k2 = split_heads(qkv_ref[rows_of(g), part(1, pair)], m_low, m_high)
        s_ref[rows_of(g), both(pair)] = dot_nt(qkv_ref[rows_of(g), part(0, pair)], k2) * (SCALE * LOG2E) + bias_ref[...]
    for g, pair in BLOCKS:
        s = s_ref[rows_of(g), both(pair)]
        probs = []
        for h in range(2):
            s_h = s[:, h * GROUP:(h + 1) * GROUP]
            e_h = jnp.exp2(s_h - jnp.max(s_h, axis=-1, keepdims=True))
            probs.append(e_h * (1.0 / jnp.sum(e_h, axis=-1, keepdims=True)))
        p_ref[rows_of(g), both(pair)] = jnp.concatenate(probs, axis=1).astype(BF16)
    for g, pair in BLOCKS:
        v2 = split_heads(qkv_ref[rows_of(g), part(2, pair)], m_low, m_high)
        o_ref[rows_of(g), part(0, pair)] = dot_nn(p_ref[rows_of(g), both(pair)], v2).astype(BF16)


def attend_back(qkv_ref, p_ref, do_ref, dqkv_ref, dp_ref):
    low, m_low, m_high = lane_masks()
    for g, pair in BLOCKS:
        do = do_ref[rows_of(g), part(0, pair)]
        v2 = split_heads(qkv_ref[rows_of(g), part(2, pair)], m_low, m_high)
        dp_ref[rows_of(g), both(pair)] = dot_nt(do, v2).astype(BF16)
        dv = dot_tn(p_ref[rows_of(g), both(pair)], do)
        dqkv_ref[rows_of(g), part(2, pair)] = jnp.where(low, dv[:GROUP], dv[GROUP:]).astype(BF16)
    for g, pair in BLOCKS:
        p32 = p_ref[rows_of(g), both(pair)].astype(F32)
        t = dp_ref[rows_of(g), both(pair)].astype(F32) * p32
        ds = []
        for h in range(2):
            half = slice(h * GROUP, (h + 1) * GROUP)
            ds.append(t[:, half] - p32[:, half] * jnp.sum(t[:, half], axis=-1, keepdims=True))
        dp_ref[rows_of(g), both(pair)] = jnp.concatenate(ds, axis=1).astype(BF16)
    for g, pair in BLOCKS:
        ds = dp_ref[rows_of(g), both(pair)]
        k2 = split_heads(qkv_ref[rows_of(g), part(1, pair)], m_low, m_high)
        dqkv_ref[rows_of(g), part(0, pair)] = (dot_nn(ds, k2) * SCALE).astype(BF16)
        dk = dot_tn(ds, qkv_ref[rows_of(g), part(0, pair)])
        dqkv_ref[rows_of(g), part(1, pair)] = (jnp.where(low, dk[:GROUP], dk[GROUP:]) * SCALE).astype(BF16)


CHUNK = 512
CHUNKS = HIDDEN // CHUNK


def cut(c):
    return pl.ds(c * CHUNK, CHUNK)


def gains(ln_ref):
    ln = ln_ref[...].astype(F32)
    return [ln[r:r + 1, :] for r in range(4)]


def position():
    me = lax.axis_index('sp')
    y, x, c = me // 4, (me // 2) % 2, me % 2
    return me, y, x, c, 4 * y + 2 * x + 1 - c, 4 * y + 2 * (1 - x) + c, 4 * (1 - y) + 2 * x + c


def peer(d):
    return lax.rem(lax.axis_index('sp') + d, N_DEV)


def enter():
    barrier = pltpu.get_barrier_semaphore()
    for d in range(1, N_DEV):
        pl.semaphore_signal(barrier, inc=1, device_id={'sp': peer(d)}, device_id_type=pl.DeviceIdType.MESH)
    pl.semaphore_wait(barrier, N_DEV - 1)


def remote(src, dst, send_sem, recv_sem, device):
    return pltpu.make_async_remote_copy(src_ref=src, dst_ref=dst, send_sem=send_sem, recv_sem=recv_sem,
                                        device_id={'sp': device}, device_id_type=pl.DeviceIdType.MESH)


def videos_of(i):
    return pl.ds(i * NV, NV)


class Exchange:
    def __init__(self, stage, landing, sems):
        self.stage, self.landing, (self.send, self.recv, self.own) = stage, landing, sems

    def copies(self, i):
        me, slot = lax.axis_index('sp'), i % 2
        return [remote(self.stage.at[slot, peer(d)], self.landing(me, i), self.send.at[slot, d], self.recv.at[i, d], peer(d))
                for d in range(1, N_DEV)]

    def local(self, i):
        me, slot = lax.axis_index('sp'), i % 2
        return pltpu.make_async_copy(self.stage.at[slot, me], self.landing(me, i), self.own.at[slot])

    def start(self, i):
        for copy in self.copies(i):
            copy.start()
        self.local(i).start()

    def wait_sent(self, i):
        for copy in self.copies(i):
            copy.wait_send()
        self.local(i).wait()

    def wait_received(self, i):
        slot = i % 2
        for d in range(1, N_DEV):
            remote(self.stage.at[slot, 0], self.landing(peer(N_DEV - d), i), self.send.at[slot, d], self.recv.at[i, d],
                   peer(d)).wait_recv()

    def free_slot(self, i):
        @pl.when(i >= 2)
        def _():
            self.wait_sent(i - 2)

    def finish(self, n):
        self.wait_sent(n - 2)
        self.wait_sent(n - 1)

        def body(i, carry):
            self.wait_received(i)
            return carry
        lax.fori_loop(0, n, body, 0)


EXCHANGE_SEMS = [pltpu.SemaphoreType.DMA((2, N_DEV)), pltpu.SemaphoreType.DMA((STEPS, N_DEV)),
                 pltpu.SemaphoreType.DMA((2,))]


def spatial_forward_kernel(x_ref, dy_ref, ln_ref, wqkv_ref, wout_ref, wup_ref, wdown_ref, bias_ref, perm_ref,
                           mid_ref, dyp_ref, h_ref, o_ref, qkv_ref, p_ref, act_ref, s_ref, stage_ref, *sems):
    step = pl.program_id(0)
    exchange = Exchange(stage_ref, lambda src, i: mid_ref.at[src, videos_of(i)], sems)

    @pl.when(step == 0)
    def _():
        enter()

    for v in range(NV):
        moved = dot_nn(perm_ref[...], dy_ref[pl.ds(v * ROWS, ROWS), :]).astype(BF16)
        for d in range(N_DEV):
            dyp_ref[d, v] = moved[d * 32:(d + 1) * 32]
    gain1, shift1, gain2, shift2 = gains(ln_ref)
    normed, _ = norm_stats(x_ref[...].astype(F32))
    a_in = (normed * gain1 + shift1).astype(BF16)
    for c in range(3):
        cols = pl.ds(c * WIDTH, WIDTH)
        qkv_ref[:, cols] = dot_nn(a_in, wqkv_ref[:, cols]).astype(BF16)
    attend(qkv_ref, bias_ref, p_ref, o_ref, s_ref)
    h_ref[...] = (x_ref[...].astype(F32) + dot_nn(o_ref[...], wout_ref[...])).astype(BF16)
    normed, _ = norm_stats(h_ref[...].astype(F32))
    m_in = (normed * gain2 + shift2).astype(BF16)
    for c in range(CHUNKS):
        act_ref[:, cut(c)] = gelu_value(dot_nn(m_in, wup_ref[:, cut(c)])).astype(BF16)
    out = (h_ref[...].astype(F32) + dot_nn(act_ref[...], wdown_ref[...])).astype(BF16)
    exchange.free_slot(step)
    for v in range(NV):
        moved = dot_nn(perm_ref[...], out[v * ROWS:(v + 1) * ROWS]).astype(BF16)
        for d in range(N_DEV):
            stage_ref[step % 2, d, v] = moved[d * 32:(d + 1) * 32]
    exchange.start(step)

    @pl.when(step == STEPS - 1)
    def _():
        exchange.finish(STEPS)


def add_blocks(sum_ref, first, product):
    for c in range(product.shape[1] // WIDTH):
        rows = pl.ds(first + c * WIDTH, WIDTH)
        sum_ref[rows, :] += product[:, c * WIDTH:(c + 1) * WIDTH]


def tail_backward(dv_ref, o_ref, m_ref, normed, inv_std, gain2, gp_ref, act_ref, dup_ref, do_ref,
                  wout_ref, wup_ref, wdown_ref, sum_ref):
    add_blocks(sum_ref, ROW_DOWN, dot_tn(dv_ref[...], act_ref[...]))
    for c in range(CHUNKS):
        d_act = dot_nt(dv_ref[...], wdown_ref[cut(c), :]).astype(BF16).astype(F32)
        dup_ref[:, cut(c)] = (d_act * gp_ref[:, cut(c)]).astype(BF16)
    add_blocks(sum_ref, ROW_UP, dot_tn(m_ref[...], dup_ref[...]))
    d_m = dot_nt(dup_ref[...], wup_ref[...]).astype(BF16).astype(F32)
    d_h, g_gain, g_shift = norm_back(d_m, normed, inv_std, gain2)
    dv_ref[...] = (d_h + dv_ref[...].astype(F32)).astype(BF16)
    add_blocks(sum_ref, ROW_OUT, dot_tn(o_ref[...], dv_ref[...]))
    do_ref[...] = dot_nt(dv_ref[...], wout_ref[...]).astype(BF16)
    return g_gain, g_shift


def qkv_backward(u32, a_ref, dh_ref, dqkv_ref, gain1, wqkv_ref, sum_ref):
    normed, inv_std = norm_stats(u32)
    add_blocks(sum_ref, ROW_QKV, dot_tn(a_ref[...], dqkv_ref[...]))
    d_a = dot_nt(dqkv_ref[...], wqkv_ref[...]).astype(BF16).astype(F32)
    d_in, g_gain, g_shift = norm_back(d_a, normed, inv_std, gain1)
    return (d_in + dh_ref[...].astype(F32)).astype(BF16), g_gain, g_shift


def up_forward(h32, gain2, shift2, m_ref, wup_ref, act_ref, gp_ref):
    normed, inv_std = norm_stats(h32)
    m_ref[...] = (normed * gain2 + shift2).astype(BF16)
    for c in range(CHUNKS):
        act, slope = gelu_parts(dot_nn(m_ref[...], wup_ref[:, cut(c)]))
        act_ref[:, cut(c)] = act.astype(BF16)
        gp_ref[:, cut(c)] = slope
    return normed, inv_std


def add_ln_sums(ref, first, sums):
    for r, g in enumerate(sums):
        ref[first + r:first + r + 1, :] += g


def temporal_kernel(mid_ref, dyp_ref, ln_ref, wqkv_ref, wout_ref, wup_ref, wdown_ref, bias_ref,
                    back_ref, sum_ref, u_ref, dv_ref, a_ref, qkv_ref, p_ref, o_ref, m_ref, act_ref,
                    dup_ref, do_ref, dqkv_ref, dp_ref, gp_ref, s_ref, dy_ref, y_stage, dm_stage, *sems):
    step = pl.program_id(0)
    me = lax.axis_index('sp')
    send_y = Exchange(y_stage, lambda src, i: back_ref.at[src, 0, videos_of(i)], sems[0:3])
    send_dm = Exchange(dm_stage, lambda src, i: back_ref.at[src, 1, videos_of(i)], sems[3:6])
    dy_send, dy_recv, dy_own = sems[6:]

    def dy_copy(i, d):
        return remote(dyp_ref.at[peer(d), videos_of(i)], dy_ref.at[me, videos_of(i)], dy_send.at[i, d], dy_recv.at[i, d],
                      peer(d))

    dy_local = pltpu.make_async_copy(dyp_ref.at[me], dy_ref.at[me], dy_own)

    @pl.when(step == 0)
    def _():
        enter()
        dy_local.start()
        for i in range(STEPS):
            for d in range(1, N_DEV):
                dy_copy(i, d).start()
        sum_ref[...] = jnp.zeros_like(sum_ref)

    gain1, shift1, gain2, shift2 = gains(ln_ref)
    places = [(v, g, s) for v in range(NV) for g in range(2) for s in range(N_DEV)]
    for v, g, s in places:
        u_ref[pl.ds(v * ROWS + g * GROUP + s * 16, 16), :] = mid_ref[s, v, pl.ds(g * 16, 16), :]
    normed1, _ = norm_stats(u_ref[...].astype(F32))
    a_ref[...] = (normed1 * gain1 + shift1).astype(BF16)
    for c in range(3):
        cols = pl.ds(c * WIDTH, WIDTH)
        qkv_ref[:, cols] = dot_nn(a_ref[...], wqkv_ref[:, cols]).astype(BF16)
    attend(qkv_ref, bias_ref, p_ref, o_ref, s_ref)
    h = (u_ref[...].astype(F32) + dot_nn(o_ref[...], wout_ref[...])).astype(BF16)
    h32 = h.astype(F32)
    normed, inv_std = up_forward(h32, gain2, shift2, m_ref, wup_ref, act_ref, gp_ref)
    out = (h32 + dot_nn(act_ref[...], wdown_ref[...])).astype(BF16)
    send_y.free_slot(step)
    for v, g, s in places:
        src = v * ROWS + g * GROUP + s * 16
        y_stage[step % 2, s, v, pl.ds(g * 16, 16), :] = out[src:src + 16]

    @pl.when(step == 0)
    def _():
        dy_local.wait()

    for d in range(1, N_DEV):
        remote(dyp_ref.at[0, videos_of(step)], dy_ref.at[peer(N_DEV - d), videos_of(step)], dy_send.at[step, d],
               dy_recv.at[step, d], peer(d)).wait_recv()
    for v, g, s in places:
        dv_ref[pl.ds(v * ROWS + g * GROUP + s * 16, 16), :] = dy_ref[s, step * NV + v, pl.ds(g * 16, 16), :]
    send_y.start(step)
    g_gain2, g_shift2 = tail_backward(dv_ref, o_ref, m_ref, normed, inv_std, gain2, gp_ref, act_ref, dup_ref, do_ref,
                                      wout_ref, wup_ref, wdown_ref, sum_ref)
    attend_back(qkv_ref, p_ref, do_ref, dqkv_ref, dp_ref)
    d_in, g_gain1, g_shift1 = qkv_backward(u_ref[...].astype(F32), a_ref, dv_ref, dqkv_ref, gain1, wqkv_ref, sum_ref)
    add_ln_sums(sum_ref, SUM_ROWS, (g_gain1, g_shift1, g_gain2, g_shift2))
    send_dm.free_slot(step)
    for v, g, s in places:
        src = v * ROWS + g * GROUP + s * 16
        dm_stage[step % 2, s, v, pl.ds(g * 16, 16), :] = d_in[src:src + 16]
    send_dm.start(step)

    @pl.when(step == STEPS - 1)
    def _():
        for i in range(STEPS):
            for d in range(1, N_DEV):
                dy_copy(i, d).wait_send()
        send_y.finish(STEPS)
        send_dm.finish(STEPS)


def span(k, idx, n):
    return pl.ds(pl.multiple_of(k * LAP_ROWS + idx * BLOCK, 16), n * BLOCK)


def slot(k, idx, n):
    return pl.ds((k * SLOTS + idx) * BLOCK, n * BLOCK)


def reduce_copies(phase, k, w_ref, r_ref, sems):
    _, y, x, c, partner, xn, yn = position()
    own0, own1 = c * 8 + x * 2, c * 8 + 4 + y * 2
    moves = (
        [((1 - c) * 8, 8, 0, partner)],
        [(c * 8 + (1 - x) * 2, 2, 8, xn), (c * 8 + 4 + (1 - y) * 2, 2, 10, yn)],
        [(own0 + 1 - y, 1, 12, yn), (own1 + 1 - x, 1, 13, xn)],
        [(own0 + y, 1, None, yn), (own1 + x, 1, None, xn)],
        [(own0, 2, None, xn), (own1, 2, None, yn)],
        [(c * 8, 8, None, partner)],
    )[phase]
    copies = []
    for j, (idx, n, place, device) in enumerate(moves):
        src = w_ref.at[span(k, idx, n), :]
        dst = src if place is None else r_ref.at[slot(k, place, n), :]
        copies.append(pltpu.make_async_remote_copy(
            src_ref=src, dst_ref=dst, send_sem=sems.at[0, phase, k, j], recv_sem=sems.at[1, phase, k, j],
            device_id={'sp': device}, device_id_type=pl.DeviceIdType.MESH))
    return copies


def reduce_peers(phase):
    _, _, _, _, partner, xn, yn = position()
    return ([partner], [xn, yn], [yn, xn])[phase]


def reduce_start(phase, k, w_ref, r_ref, sems, credits):
    copies = reduce_copies(phase, k, w_ref, r_ref, sems)
    for j, copy in enumerate(copies):
        if phase >= 3:
            pl.semaphore_wait(credits.at[5 - phase, k, j], 1)
        copy.start()


def reduce_finish(phase, k, w_ref, r_ref, sems, credits):
    for j, copy in enumerate(reduce_copies(phase, k, w_ref, r_ref, sems)):
        copy.wait()
        if phase < 3:
            pl.semaphore_signal(credits.at[phase, k, j], inc=1, device_id={'sp': reduce_peers(phase)[j]},
                                device_id_type=pl.DeviceIdType.MESH)
    _, y, x, c, _, _, _ = position()
    own0, own1 = c * 8 + x * 2, c * 8 + 4 + y * 2
    adds = ([(c * 8, 8, 0)], [(own0, 2, 8), (own1, 2, 10)], [(own0 + y, 1, 12), (own1 + x, 1, 13)], (), (), ())[phase]
    for idx, n, place in adds:
        def body(i, carry):
            w_rows = pl.ds(pl.multiple_of(k * LAP_ROWS + (idx + i) * BLOCK, 16), BLOCK)
            r_rows = pl.ds(pl.multiple_of((k * SLOTS + place + i) * BLOCK, 16), BLOCK)
            w_ref[w_rows, :] += r_ref[r_rows, :]
            return carry
        lax.fori_loop(0, n, body, 0)


def ln_copies(ln_ref, sems):
    me = lax.axis_index('sp')
    return [pltpu.make_async_remote_copy(
        src_ref=ln_ref.at[me], dst_ref=ln_ref.at[me], send_sem=sems.at[0, d], recv_sem=sems.at[1, d],
        device_id={'sp': lax.rem(me + d, N_DEV)}, device_id_type=pl.DeviceIdType.MESH) for d in range(1, N_DEV)]


def spatial_backward_kernel(*refs):
    (back_ref, x_ref, h_ref, o_ref, qkv_ref, p_ref,
     ln_ref, wqkv_ref, wout_ref, wup_ref, wdown_ref, perm_ref, gt_ref) = refs[:13]
    (y_ref, dx_ref, rt_ref, rs_ref, lnsum_ref, dv_ref, a_ref, m_ref, act_ref, dup_ref, do_ref, dqkv_ref, dp_ref, gp_ref,
     sum_ref, t_ref, rb_s_ref, rb_t_ref, ln_s_ref, ln_all_ref, sems_s, sems_t, credits_s, credits_t,
     sems_ln, sems_io) = refs[13:]
    step, last = pl.program_id(0), pl.num_programs(0) - 1
    me = lax.axis_index('sp')
    load_t = pltpu.make_async_copy(gt_ref.at[pl.ds(0, SUM_ROWS), :], t_ref, sems_io.at[0])
    load_ln = pltpu.make_async_copy(gt_ref.at[pl.ds(SUM_ROWS, 8), :], ln_all_ref.at[me, pl.ds(0, 8), :], sems_io.at[1])
    args_t, args_s = (t_ref, rb_t_ref, sems_t, credits_t), (sum_ref, rb_s_ref, sems_s, credits_s)

    @pl.when(step == 0)
    def _():
        enter()
        load_t.start()
        load_ln.start()
        sum_ref[...] = jnp.zeros_like(sum_ref)
        ln_s_ref[...] = jnp.zeros_like(ln_s_ref)

    @pl.when(step == 1)
    def _():
        load_t.wait()
        load_ln.wait()
        for k in range(LAPS):
            reduce_start(0, k, *args_t)

    for phase, at in enumerate(T_FINISH):
        @pl.when(step == at)
        def _(phase=phase):
            for k in range(LAPS):
                reduce_finish(phase, k, *args_t)
                reduce_start(phase + 1, k, *args_t)

    gain1, shift1, gain2, shift2 = gains(ln_ref)
    for v in range(NV):
        rows = pl.ds(v * ROWS, ROWS)
        dv_ref[rows, :] = dot_tn(perm_ref[...], back_ref[:, 1, v].reshape(ROWS, WIDTH)).astype(BF16)
        y_ref[rows, :] = dot_tn(perm_ref[...], back_ref[:, 0, v].reshape(ROWS, WIDTH)).astype(BF16)
    normed1, _ = norm_stats(x_ref[...].astype(F32))
    a_ref[...] = (normed1 * gain1 + shift1).astype(BF16)
    normed, inv_std = up_forward(h_ref[...].astype(F32), gain2, shift2, m_ref, wup_ref, act_ref, gp_ref)
    g_gain2, g_shift2 = tail_backward(dv_ref, o_ref, m_ref, normed, inv_std, gain2, gp_ref, act_ref, dup_ref, do_ref,
                                      wout_ref, wup_ref, wdown_ref, sum_ref)
    attend_back(qkv_ref, p_ref, do_ref, dqkv_ref, dp_ref)
    d_in, g_gain1, g_shift1 = qkv_backward(x_ref[...].astype(F32), a_ref, dv_ref, dqkv_ref, gain1, wqkv_ref, sum_ref)
    add_ln_sums(ln_s_ref, 0, (g_gain1, g_shift1, g_gain2, g_shift2))
    dx_ref[...] = d_in

    @pl.when(step == last)
    def _():
        ln_all_ref[me, pl.ds(8, 8), :] = ln_s_ref[...]
        for copy in ln_copies(ln_all_ref, sems_ln):
            copy.start()
        for k in range(LAPS):
            reduce_start(0, k, *args_s)
        for k in range(LAPS):
            reduce_finish(4, k, *args_t)
            reduce_start(5, k, *args_t)
        for phase in range(5):
            for k in range(LAPS):
                reduce_finish(phase, k, *args_s)
                reduce_start(phase + 1, k, *args_s)
            if phase == 0:
                for k in range(LAPS):
                    reduce_finish(5, k, *args_t)
                pltpu.make_async_copy(t_ref, rt_ref, sems_io.at[0]).start()
            if phase == 1:
                for copy in ln_copies(ln_all_ref, sems_ln):
                    copy.wait()
                total = ln_all_ref[0]
                for d in range(1, N_DEV):
                    total += ln_all_ref[d]
                lnsum_ref[...] = total
        outs = []
        for k in range(LAPS):
            reduce_finish(5, k, *args_s)
            lap = pl.ds(k * LAP_ROWS, LAP_ROWS)
            outs.append(pltpu.make_async_copy(sum_ref.at[lap, :], rs_ref.at[lap, :], sems_io.at[1 + k]))
            outs[-1].start()
        pltpu.make_async_copy(t_ref, rt_ref, sems_io.at[0]).wait()
        for copy in outs:
            copy.wait()


def assemble_kernel(s_ref, t_ref, ln_ref, qkv_ref, out_ref, up_ref, down_ref, gln_ref):
    third = pl.program_id(1)

    def place(src_ref, ln_row):
        @pl.when(third == 0)
        def _():
            for c in range(3):
                qkv_ref[:, pl.ds(c * WIDTH, WIDTH)] = src_ref[pl.ds(c * WIDTH, WIDTH), :]
            out_ref[...] = src_ref[pl.ds(3 * WIDTH, WIDTH), :]
            gln_ref[...] = ln_ref[ln_row:ln_row + 4, :]

        @pl.when(third == 1)
        def _():
            for c in range(4):
                up_ref[:, pl.ds(c * WIDTH, WIDTH)] = src_ref[pl.ds(c * WIDTH, WIDTH), :]

        @pl.when(third == 2)
        def _():
            for c in range(4):
                down_ref[pl.ds(c * WIDTH, WIDTH), :] = src_ref[pl.ds(c * WIDTH, WIDTH), :].T

    @pl.when(pl.program_id(0) == 0)
    def _():
        place(t_ref, 0)

    @pl.when(pl.program_id(0) == 1)
    def _():
        place(s_ref, 8)


def full(shape):
    return pl.BlockSpec(shape, lambda i: (0,) * len(shape), pipeline_mode=pl.Buffered(1))


def weight_specs(block):
    shapes = [(4, WIDTH), (WIDTH, QKV), (WIDTH, WIDTH), (WIDTH, HIDDEN), (HIDDEN, WIDTH)]
    return [pl.BlockSpec((None,) + s, lambda i: (block, 0, 0), pipeline_mode=pl.Buffered(1)) for s in shapes]


def rows_spec(width):
    return pl.BlockSpec((STEP_ROWS, width), lambda i: (i, 0))


def swap_spec():
    return pl.BlockSpec((N_DEV, NV, 32, WIDTH), lambda i: (0, i, 0, 0))


ANY = pl.BlockSpec(memory_space=pl.ANY)


def params(collective_id):
    return pltpu.CompilerParams(dimension_semantics=("arbitrary",), vmem_limit_bytes=VMEM_LIMIT,
                                collective_id=collective_id, has_side_effects=True)


def cost(us, mib):
    return pl.CostEstimate(flops=int(us * 9e8), bytes_accessed=int(mib * 2 ** 20), transcendentals=0)


def sds(shape, dtype):
    return jax.ShapeDtypeStruct(shape, dtype)


def vm(width, dtype=BF16):
    return pltpu.VMEM((STEP_ROWS, width), dtype)


TOKENS = VIDEOS * ROWS
PROBS = 6 * GROUP
SWAP = (N_DEV, VIDEOS, 32, WIDTH)
ROW_QKV, ROW_OUT, ROW_UP, ROW_DOWN = 0, 3 * WIDTH, 4 * WIDTH, 8 * WIDTH
SUM_ROWS = 12 * WIDTH
LAPS = 2
LAP_ROWS = SUM_ROWS // LAPS
BLOCK = LAP_ROWS // 16
SLOTS = 14
T_FINISH = (2, 4, 5, 6)


def spatial_forward_call(x, dy, weights, bias, perm):
    widths = (WIDTH, WIDTH, QKV, PROBS)
    return pl.pallas_call(
        spatial_forward_kernel, grid=(STEPS,), name="spatial_fwd",
        in_specs=[rows_spec(WIDTH)] * 2 + weight_specs(0) + [full((GROUP, 2 * GROUP)), full((ROWS, ROWS))],
        out_specs=[ANY, swap_spec()] + [rows_spec(w) for w in widths],
        out_shape=[sds(SWAP, BF16)] * 2 + [sds((TOKENS, w), BF16) for w in widths],
        scratch_shapes=[vm(HIDDEN), vm(PROBS, F32), pltpu.VMEM((2, N_DEV, NV, 32, WIDTH), BF16)] + EXCHANGE_SEMS,
        compiler_params=params(1), cost_estimate=cost(50, 40),
    )(x, dy, *weights, bias, perm)


def temporal_call(mid, dyp, weights, bias):
    return pl.pallas_call(
        temporal_kernel, grid=(STEPS,), name="temporal",
        in_specs=[swap_spec(), ANY] + weight_specs(1) + [full((GROUP, 2 * GROUP))],
        out_specs=[ANY, full((SUM_ROWS + 8, WIDTH))],
        out_shape=[sds((N_DEV, 2) + SWAP[1:], BF16), sds((SUM_ROWS + 8, WIDTH), F32)],
        scratch_shapes=[vm(w) for w in (WIDTH, WIDTH, WIDTH, QKV, PROBS, WIDTH, WIDTH, HIDDEN, HIDDEN, WIDTH, QKV, PROBS)]
        + [vm(HIDDEN, F32), vm(PROBS, F32), pltpu.VMEM(SWAP, BF16)]
        + [pltpu.VMEM((2, N_DEV, NV, 32, WIDTH), BF16)] * 2 + EXCHANGE_SEMS * 2
        + [pltpu.SemaphoreType.DMA((STEPS, N_DEV))] * 2 + [pltpu.SemaphoreType.DMA],
        compiler_params=params(2), cost_estimate=cost(110, 20),
    )(mid, dyp, *weights, bias)


def spatial_backward_call(back, x, saved, weights, perm, sum_t):
    return pl.pallas_call(
        spatial_backward_kernel, grid=(VIDEOS // NV,), name="spatial_bwd",
        in_specs=[pl.BlockSpec((N_DEV, 2, NV, 32, WIDTH), lambda i: (0, 0, i, 0, 0))]
        + [rows_spec(w) for w in (WIDTH, WIDTH, WIDTH, QKV, PROBS)] + weight_specs(0) + [full((ROWS, ROWS)), ANY],
        out_specs=[rows_spec(WIDTH)] * 2 + [ANY, ANY, full((16, WIDTH))],
        out_shape=[sds((TOKENS, WIDTH), BF16)] * 2 + [sds((SUM_ROWS, WIDTH), F32)] * 2 + [sds((16, WIDTH), F32)],
        scratch_shapes=[vm(w) for w in (WIDTH, WIDTH, WIDTH, HIDDEN, HIDDEN, WIDTH, QKV, PROBS)] + [vm(HIDDEN, F32)]
        + [pltpu.VMEM((SUM_ROWS, WIDTH), F32)] * 2 + [pltpu.VMEM((LAPS * SLOTS * BLOCK, WIDTH), F32)] * 2
        + [pltpu.VMEM((8, WIDTH), F32), pltpu.VMEM((N_DEV, 16, WIDTH), F32)]
        + [pltpu.SemaphoreType.DMA((2, 6, LAPS, 2))] * 2 + [pltpu.SemaphoreType.REGULAR((3, LAPS, 2))] * 2
        + [pltpu.SemaphoreType.DMA((2, N_DEV)), pltpu.SemaphoreType.DMA((4,))],
        compiler_params=params(3), cost_estimate=cost(160, 60),
    )(back, x, *saved, *weights, perm, sum_t)


def assemble_call(sum_s, sum_t, ln_sums):
    grads = [(2, WIDTH, QKV), (2, WIDTH, WIDTH), (2, WIDTH, HIDDEN), (2, HIDDEN, WIDTH), (2, 4, WIDTH)]
    return pl.pallas_call(
        assemble_kernel, grid=(2, 3), name="assemble",
        in_specs=[pl.BlockSpec((4 * WIDTH, WIDTH), lambda b, j: (jnp.where(b == 1, j, 0), 0)),
                  pl.BlockSpec((4 * WIDTH, WIDTH), lambda b, j: (jnp.where(b == 0, j, 2), 0)),
                  pl.BlockSpec((16, WIDTH), lambda b, j: (0, 0))],
        out_specs=[pl.BlockSpec((None,) + g[1:], lambda b, j: (1 - b, 0, 0)) for g in grads],
        out_shape=[sds(g, F32) for g in grads],
        compiler_params=pltpu.CompilerParams(dimension_semantics=("arbitrary", "arbitrary"), vmem_limit_bytes=VMEM_LIMIT),
        cost_estimate=cost(10, 28),
    )(sum_s, sum_t, ln_sums)


def constants():
    row = np.arange(ROWS)
    dev, patch, frame = row // 32, (row // 8) % 4, row % 8
    perm = np.zeros((ROWS, ROWS), np.float32)
    perm[row, frame * 32 + dev * 4 + patch] = 1.0
    r = np.arange(GROUP)
    frame_of = r // 32
    patch_of = (r // 8) % 2
    bias_s = np.where(frame_of[:, None] == frame_of[None], 0.0, -np.inf).astype(np.float32)
    bias_t = np.where(patch_of[:, None] == patch_of[None], 0.0, -np.inf).astype(np.float32)
    return perm, np.concatenate([bias_s] * 2, 1), np.concatenate([bias_t] * 2, 1)


def device_step(latents, cotangent, ln_params, w_qkv, w_out, w_up, w_down):
    perm, bias_s, bias_t = constants()
    perm = jnp.asarray(perm, BF16)
    bias_s, bias_t = jnp.asarray(bias_s), jnp.asarray(bias_t)
    weights = (ln_params, w_qkv, w_out.reshape(2, WIDTH, WIDTH), w_up, w_down)
    x = latents.reshape(TOKENS, WIDTH)
    dy = cotangent.reshape(TOKENS, WIDTH)

    mid, dyp, *saved = spatial_forward_call(x, dy, weights, bias_s, perm)
    back, sum_t = temporal_call(mid, dyp, weights, bias_t)
    y, dx, sum_t, sum_s, ln_sums = spatial_backward_call(back, x, saved, weights, perm, sum_t)
    g_qkv, g_out, g_up, g_down, g_ln = assemble_call(sum_s, sum_t, ln_sums)
    g_out = g_out.reshape(2, 6, 64, WIDTH)
    shape = latents.shape
    return y.reshape(shape), dx.reshape(shape), g_ln, g_qkv, g_out, g_up, g_down


def solution(mesh):
    act_spec = P('data', 'sp', None, None)
    replicated = P()
    part_spec = P('data')
    return jax.shard_map(device_step, mesh=mesh,
                         in_specs=(act_spec, act_spec, replicated, replicated, replicated, replicated, replicated),
                         out_specs=(act_spec, act_spec, part_spec, part_spec, part_spec, part_spec, part_spec),
                         check_vma=False)
```

```python
import functools

import jax
import jax.numpy as jnp
import numpy as np
from jax import lax
from jax.experimental import pallas as pl
from jax.experimental.pallas import tpu as pltpu
from jax.sharding import PartitionSpec as P

BF16 = jnp.bfloat16
F32 = jnp.float32
N_DEV = 8
WIDTH = 384
HIDDEN = 4 * WIDTH
QKV = 3 * WIDTH
VIDEOS = 16
ROWS = 256
NV = 2
STEP_ROWS = ROWS * NV
GROUP = 128
PAIRS = 3
SCALE = 0.125
LOG2E = 1.4426950408889634
STEPS = VIDEOS // NV
GELU_C = 0.7978845608028654
GELU_C3 = GELU_C * 0.044715
VMEM_LIMIT = 62 * 1024 * 1024


def dot_nn(a, b):
    return lax.dot_general(a, b, (((1,), (0,)), ((), ())), preferred_element_type=F32)


def dot_nt(a, b):
    return lax.dot_general(a, b, (((1,), (1,)), ((), ())), preferred_element_type=F32)


def dot_tn(a, b):
    return lax.dot_general(a, b, (((0,), (0,)), ((), ())), preferred_element_type=F32)


def norm_stats(x32):
    centered = x32 - jnp.mean(x32, axis=-1, keepdims=True)
    inv_std = lax.rsqrt(jnp.mean(centered * centered, axis=-1, keepdims=True) + 1e-6)
    return centered * inv_std, inv_std


def norm_back(d_out32, normed, inv_std, gain):
    d_gain = jnp.sum(d_out32 * normed, axis=0, keepdims=True)
    d_shift = jnp.sum(d_out32, axis=0, keepdims=True)
    d_norm = d_out32 * gain
    d_center = d_norm - jnp.mean(d_norm, axis=-1, keepdims=True)
    d_in = inv_std * (d_center - normed * jnp.mean(d_norm * normed, axis=-1, keepdims=True))
    return d_in, d_gain, d_shift


def gelu_parts(x):
    x2 = x * x
    t = jnp.tanh(x * (GELU_C + GELU_C3 * x2))
    half = 0.5 + 0.5 * t
    slope = half + (x * (0.5 - 0.5 * (t * t))) * (GELU_C + (3.0 * GELU_C3) * x2)
    return x * half, slope


def gelu_value(x):
    t = jnp.tanh(x * (GELU_C + GELU_C3 * (x * x)))
    return x * (0.5 + 0.5 * t)


def lane_masks():
    lane = lax.broadcasted_iota(jnp.int32, (1, GROUP), 1)
    low = (lane < GROUP // 2)
    m_low = jnp.where(low, 1.0, 0.0).astype(BF16)
    m_high = jnp.where(low, 0.0, 1.0).astype(BF16)
    return low, m_low, m_high


def split_heads(k, m_low, m_high):
    return jnp.concatenate([k * m_low, k * m_high], axis=0)


GROUPS = STEP_ROWS // GROUP
BLOCKS = [(g, pair) for g in range(GROUPS) for pair in range(PAIRS)]


def rows_of(g):
    return pl.ds(g * GROUP, GROUP)


def part(kind, pair):
    return pl.ds(kind * WIDTH + pair * GROUP, GROUP)


def both(pair):
    return pl.ds(pair * 2 * GROUP, 2 * GROUP)


def attend(qkv_ref, bias_ref, p_ref, o_ref, s_ref):
    low, m_low, m_high = lane_masks()
    for g, pair in BLOCKS:
        k2 = split_heads(qkv_ref[rows_of(g), part(1, pair)], m_low, m_high)
        s_ref[rows_of(g), both(pair)] = dot_nt(qkv_ref[rows_of(g), part(0, pair)], k2) * (SCALE * LOG2E) + bias_ref[...]
    for g, pair in BLOCKS:
        s = s_ref[rows_of(g), both(pair)]
        probs = []
        for h in range(2):
            s_h = s[:, h * GROUP:(h + 1) * GROUP]
            e_h = jnp.exp2(s_h - jnp.max(s_h, axis=-1, keepdims=True))
            probs.append(e_h * (1.0 / jnp.sum(e_h, axis=-1, keepdims=True)))
        p_ref[rows_of(g), both(pair)] = jnp.concatenate(probs, axis=1).astype(BF16)
    for g, pair in BLOCKS:
        v2 = split_heads(qkv_ref[rows_of(g), part(2, pair)], m_low, m_high)
        o_ref[rows_of(g), part(0, pair)] = dot_nn(p_ref[rows_of(g), both(pair)], v2).astype(BF16)


def attend_back(qkv_ref, p_ref, do_ref, dqkv_ref, dp_ref):
    low, m_low, m_high = lane_masks()
    for g, pair in BLOCKS:
        do = do_ref[rows_of(g), part(0, pair)]
        v2 = split_heads(qkv_ref[rows_of(g), part(2, pair)], m_low, m_high)
        dp_ref[rows_of(g), both(pair)] = dot_nt(do, v2).astype(BF16)
        dv = dot_tn(p_ref[rows_of(g), both(pair)], do)
        dqkv_ref[rows_of(g), part(2, pair)] = jnp.where(low, dv[:GROUP], dv[GROUP:]).astype(BF16)
    for g, pair in BLOCKS:
        p32 = p_ref[rows_of(g), both(pair)].astype(F32)
        t = dp_ref[rows_of(g), both(pair)].astype(F32) * p32
        ds = []
        for h in range(2):
            half = slice(h * GROUP, (h + 1) * GROUP)
            ds.append(t[:, half] - p32[:, half] * jnp.sum(t[:, half], axis=-1, keepdims=True))
        dp_ref[rows_of(g), both(pair)] = jnp.concatenate(ds, axis=1).astype(BF16)
    for g, pair in BLOCKS:
        ds = dp_ref[rows_of(g), both(pair)]
        k2 = split_heads(qkv_ref[rows_of(g), part(1, pair)], m_low, m_high)
        dqkv_ref[rows_of(g), part(0, pair)] = (dot_nn(ds, k2) * SCALE).astype(BF16)
        dk = dot_tn(ds, qkv_ref[rows_of(g), part(0, pair)])
        dqkv_ref[rows_of(g), part(1, pair)] = (jnp.where(low, dk[:GROUP], dk[GROUP:]) * SCALE).astype(BF16)


CHUNK = 512
CHUNKS = HIDDEN // CHUNK


def cut(c):
    return pl.ds(c * CHUNK, CHUNK)


def gains(ln_ref):
    ln = ln_ref[...].astype(F32)
    return [ln[r:r + 1, :] for r in range(4)]


def position():
    me = lax.axis_index('sp')
    y, x, c = me // 4, (me // 2) % 2, me % 2
    return me, y, x, c, 4 * y + 2 * x + 1 - c, 4 * y + 2 * (1 - x) + c, 4 * (1 - y) + 2 * x + c


def peer(d):
    return lax.rem(lax.axis_index('sp') + d, N_DEV)


def enter():
    barrier = pltpu.get_barrier_semaphore()
    for d in range(1, N_DEV):
        pl.semaphore_signal(barrier, inc=1, device_id={'sp': peer(d)}, device_id_type=pl.DeviceIdType.MESH)
    pl.semaphore_wait(barrier, N_DEV - 1)


def remote(src, dst, send_sem, recv_sem, device):
    return pltpu.make_async_remote_copy(src_ref=src, dst_ref=dst, send_sem=send_sem, recv_sem=recv_sem,
                                        device_id={'sp': device}, device_id_type=pl.DeviceIdType.MESH)


def videos_of(i):
    return pl.ds(i * NV, NV)


class Exchange:
    def __init__(self, stage, landing, sems):
        self.stage, self.landing, (self.send, self.recv, self.own) = stage, landing, sems

    def copies(self, i):
        me, slot = lax.axis_index('sp'), i % 2
        return [remote(self.stage.at[slot, peer(d)], self.landing(me, i), self.send.at[slot, d], self.recv.at[i, d], peer(d))
                for d in range(1, N_DEV)]

    def local(self, i):
        me, slot = lax.axis_index('sp'), i % 2
        return pltpu.make_async_copy(self.stage.at[slot, me], self.landing(me, i), self.own.at[slot])

    def start(self, i):
        for copy in self.copies(i):
            copy.start()
        self.local(i).start()

    def wait_sent(self, i):
        for copy in self.copies(i):
            copy.wait_send()
        self.local(i).wait()

    def wait_received(self, i):
        slot = i % 2
        for d in range(1, N_DEV):
            remote(self.stage.at[slot, 0], self.landing(peer(N_DEV - d), i), self.send.at[slot, d], self.recv.at[i, d],
                   peer(d)).wait_recv()

    def free_slot(self, i):
        @pl.when(i >= 2)
        def _():
            self.wait_sent(i - 2)

    def finish(self, n):
        self.wait_sent(n - 2)
        self.wait_sent(n - 1)

        def body(i, carry):
            self.wait_received(i)
            return carry
        lax.fori_loop(0, n, body, 0)


EXCHANGE_SEMS = [pltpu.SemaphoreType.DMA((2, N_DEV)), pltpu.SemaphoreType.DMA((STEPS, N_DEV)),
                 pltpu.SemaphoreType.DMA((2,))]


def spatial_forward_kernel(x_ref, dy_ref, ln_ref, wqkv_ref, wout_ref, wup_ref, wdown_ref, bias_ref, perm_ref,
                           mid_ref, dyp_ref, h_ref, o_ref, qkv_ref, p_ref, act_ref, s_ref, stage_ref, *sems):
    step = pl.program_id(0)
    exchange = Exchange(stage_ref, lambda src, i: mid_ref.at[src, videos_of(i)], sems)

    @pl.when(step == 0)
    def _():
        enter()

    for v in range(NV):
        moved = dot_nn(perm_ref[...], dy_ref[pl.ds(v * ROWS, ROWS), :]).astype(BF16)
        for d in range(N_DEV):
            dyp_ref[d, v] = moved[d * 32:(d + 1) * 32]
    gain1, shift1, gain2, shift2 = gains(ln_ref)
    normed, _ = norm_stats(x_ref[...].astype(F32))
    a_in = (normed * gain1 + shift1).astype(BF16)
    for c in range(3):
        cols = pl.ds(c * WIDTH, WIDTH)
        qkv_ref[:, cols] = dot_nn(a_in, wqkv_ref[:, cols]).astype(BF16)
    attend(qkv_ref, bias_ref, p_ref, o_ref, s_ref)
    h_ref[...] = (x_ref[...].astype(F32) + dot_nn(o_ref[...], wout_ref[...])).astype(BF16)
    normed, _ = norm_stats(h_ref[...].astype(F32))
    m_in = (normed * gain2 + shift2).astype(BF16)
    for c in range(CHUNKS):
        act_ref[:, cut(c)] = gelu_value(dot_nn(m_in, wup_ref[:, cut(c)])).astype(BF16)
    out = (h_ref[...].astype(F32) + dot_nn(act_ref[...], wdown_ref[...])).astype(BF16)
    exchange.free_slot(step)
    for v in range(NV):
        moved = dot_nn(perm_ref[...], out[v * ROWS:(v + 1) * ROWS]).astype(BF16)
        for d in range(N_DEV):
            stage_ref[step % 2, d, v] = moved[d * 32:(d + 1) * 32]
    exchange.start(step)

    @pl.when(step == STEPS - 1)
    def _():
        exchange.finish(STEPS)


def add_blocks(sum_ref, first, product):
    for c in range(product.shape[1] // WIDTH):
        rows = pl.ds(first + c * WIDTH, WIDTH)
        sum_ref[rows, :] += product[:, c * WIDTH:(c + 1) * WIDTH]


def tail_backward(dv_ref, o_ref, m_ref, normed, inv_std, gain2, gp_ref, act_ref, dup_ref, do_ref,
                  wout_ref, wup_ref, wdown_ref, sum_ref):
    add_blocks(sum_ref, ROW_DOWN, dot_tn(dv_ref[...], act_ref[...]))
    for c in range(CHUNKS):
        d_act = dot_nt(dv_ref[...], wdown_ref[cut(c), :]).astype(BF16).astype(F32)
        dup_ref[:, cut(c)] = (d_act * gp_ref[:, cut(c)]).astype(BF16)
    add_blocks(sum_ref, ROW_UP, dot_tn(m_ref[...], dup_ref[...]))
    d_m = dot_nt(dup_ref[...], wup_ref[...]).astype(BF16).astype(F32)
    d_h, g_gain, g_shift = norm_back(d_m, normed, inv_std, gain2)
    dv_ref[...] = (d_h + dv_ref[...].astype(F32)).astype(BF16)
    add_blocks(sum_ref, ROW_OUT, dot_tn(o_ref[...], dv_ref[...]))
    do_ref[...] = dot_nt(dv_ref[...], wout_ref[...]).astype(BF16)
    return g_gain, g_shift


def qkv_backward(u32, a_ref, dh_ref, dqkv_ref, gain1, wqkv_ref, sum_ref):
    normed, inv_std = norm_stats(u32)
    add_blocks(sum_ref, ROW_QKV, dot_tn(a_ref[...], dqkv_ref[...]))
    d_a = dot_nt(dqkv_ref[...], wqkv_ref[...]).astype(BF16).astype(F32)
    d_in, g_gain, g_shift = norm_back(d_a, normed, inv_std, gain1)
    return (d_in + dh_ref[...].astype(F32)).astype(BF16), g_gain, g_shift


def up_forward(h32, gain2, shift2, m_ref, wup_ref, act_ref, gp_ref):
    normed, inv_std = norm_stats(h32)
    m_ref[...] = (normed * gain2 + shift2).astype(BF16)
    for c in range(CHUNKS):
        act, slope = gelu_parts(dot_nn(m_ref[...], wup_ref[:, cut(c)]))
        act_ref[:, cut(c)] = act.astype(BF16)
        gp_ref[:, cut(c)] = slope
    return normed, inv_std


def add_ln_sums(ref, first, sums):
    for r, g in enumerate(sums):
        ref[first + r:first + r + 1, :] += g


def temporal_kernel(mid_ref, dyp_ref, ln_ref, wqkv_ref, wout_ref, wup_ref, wdown_ref, bias_ref,
                    back_ref, sum_ref, u_ref, dv_ref, a_ref, qkv_ref, p_ref, o_ref, m_ref, act_ref,
                    dup_ref, do_ref, dqkv_ref, dp_ref, gp_ref, s_ref, dy_ref, y_stage, dm_stage, *sems):
    step = pl.program_id(0)
    me = lax.axis_index('sp')
    send_y = Exchange(y_stage, lambda src, i: back_ref.at[src, 0, videos_of(i)], sems[0:3])
    send_dm = Exchange(dm_stage, lambda src, i: back_ref.at[src, 1, videos_of(i)], sems[3:6])
    dy_send, dy_recv, dy_own = sems[6:]

    def dy_copy(i, d):
        return remote(dyp_ref.at[peer(d), videos_of(i)], dy_ref.at[me, videos_of(i)], dy_send.at[i, d], dy_recv.at[i, d],
                      peer(d))

    dy_local = pltpu.make_async_copy(dyp_ref.at[me], dy_ref.at[me], dy_own)

    @pl.when(step == 0)
    def _():
        enter()
        dy_local.start()
        for i in range(STEPS):
            for d in range(1, N_DEV):
                dy_copy(i, d).start()
        sum_ref[...] = jnp.zeros_like(sum_ref)

    gain1, shift1, gain2, shift2 = gains(ln_ref)
    places = [(v, g, s) for v in range(NV) for g in range(2) for s in range(N_DEV)]
    for v, g, s in places:
        u_ref[pl.ds(v * ROWS + g * GROUP + s * 16, 16), :] = mid_ref[s, v, pl.ds(g * 16, 16), :]
    normed1, _ = norm_stats(u_ref[...].astype(F32))
    a_ref[...] = (normed1 * gain1 + shift1).astype(BF16)
    for c in range(3):
        cols = pl.ds(c * WIDTH, WIDTH)
        qkv_ref[:, cols] = dot_nn(a_ref[...], wqkv_ref[:, cols]).astype(BF16)
    attend(qkv_ref, bias_ref, p_ref, o_ref, s_ref)
    h = (u_ref[...].astype(F32) + dot_nn(o_ref[...], wout_ref[...])).astype(BF16)
    h32 = h.astype(F32)
    normed, inv_std = up_forward(h32, gain2, shift2, m_ref, wup_ref, act_ref, gp_ref)
    out = (h32 + dot_nn(act_ref[...], wdown_ref[...])).astype(BF16)
    send_y.free_slot(step)
    for v, g, s in places:
        src = v * ROWS + g * GROUP + s * 16
        y_stage[step % 2, s, v, pl.ds(g * 16, 16), :] = out[src:src + 16]

    @pl.when(step == 0)
    def _():
        dy_local.wait()

    for d in range(1, N_DEV):
        remote(dyp_ref.at[0, videos_of(step)], dy_ref.at[peer(N_DEV - d), videos_of(step)], dy_send.at[step, d],
               dy_recv.at[step, d], peer(d)).wait_recv()
    for v, g, s in places:
        dv_ref[pl.ds(v * ROWS + g * GROUP + s * 16, 16), :] = dy_ref[s, step * NV + v, pl.ds(g * 16, 16), :]
    send_y.start(step)
    g_gain2, g_shift2 = tail_backward(dv_ref, o_ref, m_ref, normed, inv_std, gain2, gp_ref, act_ref, dup_ref, do_ref,
                                      wout_ref, wup_ref, wdown_ref, sum_ref)
    attend_back(qkv_ref, p_ref, do_ref, dqkv_ref, dp_ref)
    d_in, g_gain1, g_shift1 = qkv_backward(u_ref[...].astype(F32), a_ref, dv_ref, dqkv_ref, gain1, wqkv_ref, sum_ref)
    add_ln_sums(sum_ref, SUM_ROWS, (g_gain1, g_shift1, g_gain2, g_shift2))
    send_dm.free_slot(step)
    for v, g, s in places:
        src = v * ROWS + g * GROUP + s * 16
        dm_stage[step % 2, s, v, pl.ds(g * 16, 16), :] = d_in[src:src + 16]
    send_dm.start(step)

    @pl.when(step == STEPS - 1)
    def _():
        for i in range(STEPS):
            for d in range(1, N_DEV):
                dy_copy(i, d).wait_send()
        send_y.finish(STEPS)
        send_dm.finish(STEPS)


def span(k, idx, n):
    return pl.ds(pl.multiple_of(k * LAP_ROWS + idx * BLOCK, 8), n * BLOCK)


def slot(k, idx, n):
    return pl.ds((k * SLOTS + idx) * BLOCK, n * BLOCK)


class Reduce:
    def __init__(self, sum_ref, first_ref, landing_ref, sems, credits, block, out_sems):
        self.sum, self.first, self.landing = sum_ref, first_ref, landing_ref
        self.sems, self.credits, self.block, self.out_sems = sems, credits, block, out_sems

    def moves(self, phase):
        _, y, x, c, partner, xn, yn = position()
        own0, own1 = c * 8 + x * 2, c * 8 + 4 + y * 2
        return (
            [((1 - c) * 8, 8, 0, partner)],
            [(c * 8 + (1 - x) * 2, 2, 8, xn), (c * 8 + 4 + (1 - y) * 2, 2, 10, yn)],
            [(own0 + 1 - y, 1, 12, yn), (own1 + 1 - x, 1, 13, xn)],
            [(own0 + y, 1, None, yn), (own1 + x, 1, None, xn)],
            [(own0, 2, None, xn), (own1, 2, None, yn)],
            [(c * 8, 8, None, partner)],
        )[phase]

    def copies(self, phase, k):
        source = self.first if phase == 0 else self.sum
        copies = []
        for j, (idx, n, place, device) in enumerate(self.moves(phase)):
            dst = self.sum.at[span(k, idx, n), :] if place is None else self.landing.at[slot(k, place, n), :]
            copies.append(remote(source.at[span(k, idx, n), :], dst, self.sems.at[0, phase, k, j],
                                 self.sems.at[1, phase, k, j], device))
        return copies

    def start(self, phase, k):
        for j, copy in enumerate(self.copies(phase, k)):
            if phase >= 3:
                pl.semaphore_wait(self.credits.at[5 - phase, k, j], 1)
            copy.start()

    def finish(self, phase, k):
        for j, copy in enumerate(self.copies(phase, k)):
            copy.wait()
            if phase < 3:
                pl.semaphore_signal(self.credits.at[phase, k, j], inc=1, device_id={'sp': self.moves(phase)[j][3]},
                                    device_id_type=pl.DeviceIdType.MESH)
        _, y, x, c, _, _, _ = position()
        own0, own1 = c * 8 + x * 2, c * 8 + 4 + y * 2
        adds = ([(c * 8, 8, 0)], [(own0, 2, 8), (own1, 2, 10)], [(own0 + y, 1, 12), (own1 + x, 1, 13)], (), (), ())
        for idx, n, place in adds[phase]:
            def body(i, carry):
                rows = pl.ds(pl.multiple_of((k * SLOTS + place + i) * BLOCK, 8), BLOCK)
                self.sum[span(k, idx + i, 1), :] += self.landing[rows, :]
                return carry
            lax.fori_loop(0, n, body, 0)
        if phase == 5:
            for r in self.pieces(k):
                if r >= 8:
                    rows = pl.ds(r * WIDTH, WIDTH)
                    self.sum[rows, :] = self.sum[rows, :].T

    def pieces(self, k):
        return range(k * LAP_ROWS // WIDTH, (k + 1) * LAP_ROWS // WIDTH)

    def out_copy(self, r, outs):
        qkv_ref, out_ref, up_ref, down_ref = outs
        b = self.block
        if r < 3:
            dst = qkv_ref.at[b, :, pl.ds(r * WIDTH, WIDTH)]
        elif r == 3:
            dst = out_ref.at[b]
        elif r < 8:
            dst = up_ref.at[b, :, pl.ds((r - 4) * WIDTH, WIDTH)]
        else:
            dst = down_ref.at[b, pl.ds((r - 8) * WIDTH, WIDTH), :]
        return pltpu.make_async_copy(self.sum.at[pl.ds(r * WIDTH, WIDTH), :], dst, self.out_sems.at[r])


def reduce_plan():
    lasts = (1.4, 4.75, 2.4, 2.4, 4.75, 1.4)
    free, running, plan, now = [0.0, 0.0], {}, [], 0.0

    def start(lap, phase):
        link = 0 if phase in (0, 5) else 1
        free[link] = max(free[link], now) + lasts[phase]
        running[lap] = (phase, free[link] + 2.5)

    def turn(due):
        turns = []
        for lap in sorted(running, key=lambda lap: running[lap][1]):
            phase, end = running[lap]
            if end <= due:
                turns.append((lap, phase))
        for lap, phase in turns:
            del running[lap]
            if phase < 5:
                start(lap, phase + 1)
        return turns

    begin = {0: [('t', k) for k in (1, 2, 3, 0)], STEPS: [('s', k) for k in (1, 2, 3)]}
    for step in range(2 * STEPS):
        turns = turn(now)
        fresh = begin.get(step, [])
        for lap in fresh:
            start(lap, 0)
        plan.append((turns, fresh))
        now += 6.2 if step < STEPS else 4.2
    start(('s', 0), 0)
    turns, fresh = [], [('s', 0)]
    while running:
        plan.append((turns, fresh))
        fresh = []
        now = max(now, min(end for _, end in running.values()))
        turns = turn(now)
    plan.append((turns, fresh))
    return plan


def ln_copies(ln_ref, sems):
    me = lax.axis_index('sp')
    return [pltpu.make_async_remote_copy(
        src_ref=ln_ref.at[me], dst_ref=ln_ref.at[me], send_sem=sems.at[0, d], recv_sem=sems.at[1, d],
        device_id={'sp': lax.rem(me + d, N_DEV)}, device_id_type=pl.DeviceIdType.MESH) for d in range(1, N_DEV)]


def spatial_backward_kernel(*refs):
    (back_ref, x_ref, h_ref, o_ref, qkv_ref, p_ref,
     ln_ref, wqkv_ref, wout_ref, wup_ref, wdown_ref, perm_ref, gt_ref) = refs[:13]
    (y_ref, dx_ref, gqkv_ref, gout_ref, gup_ref, gdown_ref, gln_ref,
     dv_ref, a_ref, m_ref, act_ref, dup_ref, do_ref, dqkv_ref, dp_ref, gp_ref, dh_all_ref, do_all_ref,
     sum_ref, t_ref, land_s_ref, land_t_ref, ln_s_ref, ln_all_ref, sems_s, sems_t, credits_s, credits_t,
     sems_out_s, sems_out_t, sems_ln, sems_in) = refs[13:]
    step = pl.program_id(0)
    me = lax.axis_index('sp')
    load_t = pltpu.make_async_copy(gt_ref.at[pl.ds(0, SUM_ROWS), :], t_ref, sems_in.at[0])
    load_ln = pltpu.make_async_copy(gt_ref.at[pl.ds(SUM_ROWS, 8), :], ln_all_ref.at[me, pl.ds(0, 8), :], sems_in.at[1])
    sums = {'t': Reduce(t_ref, gt_ref, land_t_ref, sems_t, credits_t, 1, sems_out_t),
            's': Reduce(sum_ref, sum_ref, land_s_ref, sems_s, credits_s, 0, sems_out_s)}
    outs = (gqkv_ref, gout_ref, gup_ref, gdown_ref)
    plan = reduce_plan()
    written = []

    def advance(turns, fresh):
        for (which, k), phase in turns:
            sums[which].finish(phase, k)
        for which, k in fresh:
            sums[which].start(0, k)
        for (which, k), phase in turns:
            if phase < 5:
                sums[which].start(phase + 1, k)
        while written:
            which, k = written.pop()
            for r in sums[which].pieces(k):
                sums[which].out_copy(r, outs).start()
        written.extend(lap for lap, phase in turns if phase == 5)

    @pl.when(step == 0)
    def _():
        enter()
        load_t.start()
        load_ln.start()
        sum_ref[...] = jnp.zeros_like(sum_ref)
        ln_s_ref[...] = jnp.zeros_like(ln_s_ref)

    @pl.when(step == 1)
    def _():
        load_t.wait()
        load_ln.wait()

    for at in range(2 * STEPS):
        if any(plan[at]) or written:
            @pl.when(step == at)
            def _(at=at):
                advance(*plan[at])

    gain1, shift1, gain2, shift2 = gains(ln_ref)

    @pl.when(step < STEPS)
    def _():
        mine = pl.ds(pl.multiple_of(step * STEP_ROWS, STEP_ROWS), STEP_ROWS)
        for v in range(NV):
            rows = pl.ds(v * ROWS, ROWS)
            dv_ref[rows, :] = dot_tn(perm_ref[...], back_ref[:, 1, v].reshape(ROWS, WIDTH)).astype(BF16)
            y_ref[rows, :] = dot_tn(perm_ref[...], back_ref[:, 0, v].reshape(ROWS, WIDTH)).astype(BF16)
        normed, inv_std = up_forward(h_ref[...].astype(F32), gain2, shift2, m_ref, wup_ref, act_ref, gp_ref)
        g_gain2, g_shift2 = tail_backward(dv_ref, o_ref, m_ref, normed, inv_std, gain2, gp_ref, act_ref, dup_ref, do_ref,
                                          wout_ref, wup_ref, wdown_ref, sum_ref)
        dh_all_ref[mine, :] = dv_ref[...]
        do_all_ref[mine, :] = do_ref[...]
        add_ln_sums(ln_s_ref, 2, (g_gain2, g_shift2))

    @pl.when(step >= STEPS)
    def _():
        mine = pl.ds(pl.multiple_of((step - STEPS) * STEP_ROWS, STEP_ROWS), STEP_ROWS)
        dv_ref[...] = dh_all_ref[mine, :]
        do_ref[...] = do_all_ref[mine, :]
        normed1, _ = norm_stats(x_ref[...].astype(F32))
        a_ref[...] = (normed1 * gain1 + shift1).astype(BF16)
        attend_back(qkv_ref, p_ref, do_ref, dqkv_ref, dp_ref)
        d_in, g_gain1, g_shift1 = qkv_backward(x_ref[...].astype(F32), a_ref, dv_ref, dqkv_ref, gain1, wqkv_ref, sum_ref)
        add_ln_sums(ln_s_ref, 0, (g_gain1, g_shift1))
        dx_ref[...] = d_in

    @pl.when(step == 2 * STEPS - 1)
    def _():
        ln_all_ref[me, pl.ds(8, 8), :] = ln_s_ref[...]
        for n, (turns, fresh) in enumerate(plan[2 * STEPS:]):
            advance(turns, fresh)
            if n == 0:
                for copy in ln_copies(ln_all_ref, sems_ln):
                    copy.start()
            if n == 3:
                for copy in ln_copies(ln_all_ref, sems_ln):
                    copy.wait()
                total = ln_all_ref[0]
                for d in range(1, N_DEV):
                    total += ln_all_ref[d]
                gln_ref[0] = total[8:12]
                gln_ref[1] = total[0:4]
        advance((), ())
        for which in 'ts':
            for r in range(12):
                sums[which].out_copy(r, outs).wait()


def full(shape):
    return pl.BlockSpec(shape, lambda i: (0,) * len(shape), pipeline_mode=pl.Buffered(1))


def weight_specs(block):
    shapes = [(4, WIDTH), (WIDTH, QKV), (WIDTH, WIDTH), (WIDTH, HIDDEN), (HIDDEN, WIDTH)]
    return [pl.BlockSpec((None,) + s, lambda i: (block, 0, 0), pipeline_mode=pl.Buffered(1)) for s in shapes]


def rows_spec(width):
    return pl.BlockSpec((STEP_ROWS, width), lambda i: (i, 0))


def swap_spec():
    return pl.BlockSpec((N_DEV, NV, 32, WIDTH), lambda i: (0, i, 0, 0))


ANY = pl.BlockSpec(memory_space=pl.ANY)


def params(collective_id):
    return pltpu.CompilerParams(dimension_semantics=("arbitrary",), vmem_limit_bytes=VMEM_LIMIT,
                                collective_id=collective_id, has_side_effects=True)


def cost(us, mib):
    return pl.CostEstimate(flops=int(us * 9e8), bytes_accessed=int(mib * 2 ** 20), transcendentals=0)


def sds(shape, dtype):
    return jax.ShapeDtypeStruct(shape, dtype)


def vm(width, dtype=BF16):
    return pltpu.VMEM((STEP_ROWS, width), dtype)


TOKENS = VIDEOS * ROWS
PROBS = 6 * GROUP
SWAP = (N_DEV, VIDEOS, 32, WIDTH)
ROW_QKV, ROW_OUT, ROW_UP, ROW_DOWN = 0, 3 * WIDTH, 4 * WIDTH, 8 * WIDTH
SUM_ROWS = 12 * WIDTH
LAPS = 4
LAP_ROWS = SUM_ROWS // LAPS
BLOCK = LAP_ROWS // 16
SLOTS = 14


def spatial_forward_call(x, dy, weights, bias, perm):
    widths = (WIDTH, WIDTH, QKV, PROBS)
    return pl.pallas_call(
        spatial_forward_kernel, grid=(STEPS,), name="spatial_fwd",
        in_specs=[rows_spec(WIDTH)] * 2 + weight_specs(0) + [full((GROUP, 2 * GROUP)), full((ROWS, ROWS))],
        out_specs=[ANY, swap_spec()] + [rows_spec(w) for w in widths],
        out_shape=[sds(SWAP, BF16)] * 2 + [sds((TOKENS, w), BF16) for w in widths],
        scratch_shapes=[vm(HIDDEN), vm(PROBS, F32), pltpu.VMEM((2, N_DEV, NV, 32, WIDTH), BF16)] + EXCHANGE_SEMS,
        compiler_params=params(1), cost_estimate=cost(50, 40),
    )(x, dy, *weights, bias, perm)


def temporal_call(mid, dyp, weights, bias):
    return pl.pallas_call(
        temporal_kernel, grid=(STEPS,), name="temporal",
        in_specs=[swap_spec(), ANY] + weight_specs(1) + [full((GROUP, 2 * GROUP))],
        out_specs=[ANY, full((SUM_ROWS + 8, WIDTH))],
        out_shape=[sds((N_DEV, 2) + SWAP[1:], BF16), sds((SUM_ROWS + 8, WIDTH), F32)],
        scratch_shapes=[vm(w) for w in (WIDTH, WIDTH, WIDTH, QKV, PROBS, WIDTH, WIDTH, HIDDEN, HIDDEN, WIDTH, QKV, PROBS)]
        + [vm(HIDDEN, F32), vm(PROBS, F32), pltpu.VMEM(SWAP, BF16)]
        + [pltpu.VMEM((2, N_DEV, NV, 32, WIDTH), BF16)] * 2 + EXCHANGE_SEMS * 2
        + [pltpu.SemaphoreType.DMA((STEPS, N_DEV))] * 2 + [pltpu.SemaphoreType.DMA],
        compiler_params=params(2), cost_estimate=cost(110, 20),
    )(mid, dyp, *weights, bias)


def spatial_backward_call(back, x, saved, weights, perm, sum_t):
    def early(width):
        return pl.BlockSpec((STEP_ROWS, width), lambda i: (jnp.minimum(i, STEPS - 1), 0))

    def late(width):
        return pl.BlockSpec((STEP_ROWS, width), lambda i: (jnp.maximum(i - STEPS, 0), 0))

    grads = [(2, WIDTH, QKV), (2, WIDTH, WIDTH), (2, WIDTH, HIDDEN), (2, HIDDEN, WIDTH)]
    return pl.pallas_call(
        spatial_backward_kernel, grid=(2 * STEPS,), name="spatial_bwd",
        in_specs=[pl.BlockSpec((N_DEV, 2, NV, 32, WIDTH), lambda i: (0, 0, jnp.minimum(i, STEPS - 1), 0, 0))]
        + [late(WIDTH), early(WIDTH), early(WIDTH), late(QKV), late(PROBS)] + weight_specs(0) + [full((ROWS, ROWS)), ANY],
        out_specs=[early(WIDTH), late(WIDTH)] + [ANY] * 4 + [full((2, 4, WIDTH))],
        out_shape=[sds((TOKENS, WIDTH), BF16)] * 2 + [sds(g, F32) for g in grads] + [sds((2, 4, WIDTH), F32)],
        scratch_shapes=[vm(w) for w in (WIDTH, WIDTH, WIDTH, HIDDEN, HIDDEN, WIDTH, QKV, PROBS)] + [vm(HIDDEN, F32)]
        + [pltpu.VMEM((TOKENS, WIDTH), BF16)] * 2
        + [pltpu.VMEM((SUM_ROWS, WIDTH), F32)] * 2 + [pltpu.VMEM((LAPS * SLOTS * BLOCK, WIDTH), F32)] * 2
        + [pltpu.VMEM((8, WIDTH), F32), pltpu.VMEM((N_DEV, 16, WIDTH), F32)]
        + [pltpu.SemaphoreType.DMA((2, 6, LAPS, 2))] * 2 + [pltpu.SemaphoreType.REGULAR((3, LAPS, 2))] * 2
        + [pltpu.SemaphoreType.DMA((12,))] * 2 + [pltpu.SemaphoreType.DMA((2, N_DEV)), pltpu.SemaphoreType.DMA((2,))],
        compiler_params=params(3), cost_estimate=cost(160, 60),
    )(back, x, *saved, *weights, perm, sum_t)


def constants():
    row = np.arange(ROWS)
    dev, patch, frame = row // 32, (row // 8) % 4, row % 8
    perm = np.zeros((ROWS, ROWS), np.float32)
    perm[row, frame * 32 + dev * 4 + patch] = 1.0
    r = np.arange(GROUP)
    frame_of = r // 32
    patch_of = (r // 8) % 2
    bias_s = np.where(frame_of[:, None] == frame_of[None], 0.0, -np.inf).astype(np.float32)
    bias_t = np.where(patch_of[:, None] == patch_of[None], 0.0, -np.inf).astype(np.float32)
    return perm, np.concatenate([bias_s] * 2, 1), np.concatenate([bias_t] * 2, 1)


def device_step(latents, cotangent, ln_params, w_qkv, w_out, w_up, w_down):
    perm, bias_s, bias_t = constants()
    perm = jnp.asarray(perm, BF16)
    bias_s, bias_t = jnp.asarray(bias_s), jnp.asarray(bias_t)
    weights = (ln_params, w_qkv, w_out.reshape(2, WIDTH, WIDTH), w_up, w_down)
    x = latents.reshape(TOKENS, WIDTH)
    dy = cotangent.reshape(TOKENS, WIDTH)

    mid, dyp, *saved = spatial_forward_call(x, dy, weights, bias_s, perm)
    back, sum_t = temporal_call(mid, dyp, weights, bias_t)
    y, dx, g_qkv, g_out, g_up, g_down, g_ln = spatial_backward_call(back, x, saved, weights, perm, sum_t)
    g_out = g_out.reshape(2, 6, 64, WIDTH)
    shape = latents.shape
    return y.reshape(shape), dx.reshape(shape), g_ln, g_qkv, g_out, g_up, g_down


def solution(mesh):
    act_spec = P('data', 'sp', None, None)
    replicated = P()
    part_spec = P('data')
    return jax.shard_map(device_step, mesh=mesh,
                         in_specs=(act_spec, act_spec, replicated, replicated, replicated, replicated, replicated),
                         out_specs=(act_spec, act_spec, part_spec, part_spec, part_spec, part_spec, part_spec),
                         check_vma=False)
```

```python
import functools

import jax
import jax.numpy as jnp
import numpy as np
from jax import lax
from jax.experimental import pallas as pl
from jax.experimental.pallas import tpu as pltpu
from jax.sharding import PartitionSpec as P

BF16 = jnp.bfloat16
F32 = jnp.float32
N_DEV = 8
WIDTH = 384
HIDDEN = 4 * WIDTH
QKV = 3 * WIDTH
VIDEOS = 16
ROWS = 256
NV = 2
STEP_ROWS = ROWS * NV
GROUP = 128
PAIRS = 3
SCALE = 0.125
LOG2E = 1.4426950408889634
STEPS = VIDEOS // NV
EARLY = 3
GELU_C = 0.7978845608028654
GELU_C3 = GELU_C * 0.044715
VMEM_LIMIT = 62 * 1024 * 1024


def dot_nn(a, b):
    return lax.dot_general(a, b, (((1,), (0,)), ((), ())), preferred_element_type=F32)


def dot_nt(a, b):
    return lax.dot_general(a, b, (((1,), (1,)), ((), ())), preferred_element_type=F32)


def dot_tn(a, b):
    return lax.dot_general(a, b, (((0,), (0,)), ((), ())), preferred_element_type=F32)


def norm_stats(x32):
    centered = x32 - jnp.mean(x32, axis=-1, keepdims=True)
    inv_std = lax.rsqrt(jnp.mean(centered * centered, axis=-1, keepdims=True) + 1e-6)
    return centered * inv_std, inv_std


def norm_back(d_out32, normed, inv_std, gain):
    d_gain = jnp.sum(d_out32 * normed, axis=0, keepdims=True)
    d_shift = jnp.sum(d_out32, axis=0, keepdims=True)
    d_norm = d_out32 * gain
    d_center = d_norm - jnp.mean(d_norm, axis=-1, keepdims=True)
    d_in = inv_std * (d_center - normed * jnp.mean(d_norm * normed, axis=-1, keepdims=True))
    return d_in, d_gain, d_shift


def gelu_parts(x):
    x2 = x * x
    t = jnp.tanh(x * (GELU_C + GELU_C3 * x2))
    half = 0.5 + 0.5 * t
    act = x * half
    return act, half + (act * (1.0 - t)) * (GELU_C + (3.0 * GELU_C3) * x2)


def gelu_value(x):
    t = jnp.tanh(x * (GELU_C + GELU_C3 * (x * x)))
    return x * (0.5 + 0.5 * t)


def lane_masks():
    lane = lax.broadcasted_iota(jnp.int32, (1, GROUP), 1)
    low = (lane < GROUP // 2)
    m_low = jnp.where(low, 1.0, 0.0).astype(BF16)
    m_high = jnp.where(low, 0.0, 1.0).astype(BF16)
    return low, m_low, m_high


def split_heads(k, m_low, m_high):
    return jnp.concatenate([k * m_low, k * m_high], axis=0)


GROUPS = STEP_ROWS // GROUP
BLOCKS = [(g, pair) for g in range(GROUPS) for pair in range(PAIRS)]


def rows_of(g):
    return pl.ds(g * GROUP, GROUP)


def part(kind, pair):
    return pl.ds(kind * WIDTH + pair * GROUP, GROUP)


def both(pair):
    return pl.ds(pair * 2 * GROUP, 2 * GROUP)


def attend(qkv_ref, bias_ref, p_ref, o_ref, s_ref):
    low, m_low, m_high = lane_masks()
    for g, pair in BLOCKS:
        k2 = split_heads(qkv_ref[rows_of(g), part(1, pair)], m_low, m_high)
        s_ref[rows_of(g), both(pair)] = dot_nt(qkv_ref[rows_of(g), part(0, pair)], k2) * (SCALE * LOG2E) + bias_ref[...]
    for g, pair in BLOCKS:
        s = s_ref[rows_of(g), both(pair)]
        probs = []
        for h in range(2):
            s_h = s[:, h * GROUP:(h + 1) * GROUP]
            e_h = jnp.exp2(s_h - jnp.max(s_h, axis=-1, keepdims=True))
            probs.append(e_h * (1.0 / jnp.sum(e_h, axis=-1, keepdims=True)))
        p_ref[rows_of(g), both(pair)] = jnp.concatenate(probs, axis=1).astype(BF16)
    for g, pair in BLOCKS:
        v2 = split_heads(qkv_ref[rows_of(g), part(2, pair)], m_low, m_high)
        o_ref[rows_of(g), part(0, pair)] = dot_nn(p_ref[rows_of(g), both(pair)], v2).astype(BF16)


def attend_back(qkv_ref, p_ref, do_ref, dqkv_ref, dp_ref):
    low, m_low, m_high = lane_masks()
    for g, pair in BLOCKS:
        do = do_ref[rows_of(g), part(0, pair)]
        v2 = split_heads(qkv_ref[rows_of(g), part(2, pair)], m_low, m_high)
        dp_ref[rows_of(g), both(pair)] = dot_nt(do, v2).astype(BF16)
        dv = dot_tn(p_ref[rows_of(g), both(pair)], do)
        dqkv_ref[rows_of(g), part(2, pair)] = jnp.where(low, dv[:GROUP], dv[GROUP:]).astype(BF16)
    for g, pair in BLOCKS:
        p32 = p_ref[rows_of(g), both(pair)].astype(F32)
        t = dp_ref[rows_of(g), both(pair)].astype(F32) * p32
        ds = []
        for h in range(2):
            half = slice(h * GROUP, (h + 1) * GROUP)
            ds.append(t[:, half] - p32[:, half] * jnp.sum(t[:, half], axis=-1, keepdims=True))
        dp_ref[rows_of(g), both(pair)] = jnp.concatenate(ds, axis=1).astype(BF16)
    for g, pair in BLOCKS:
        ds = dp_ref[rows_of(g), both(pair)]
        k2 = split_heads(qkv_ref[rows_of(g), part(1, pair)], m_low, m_high)
        dqkv_ref[rows_of(g), part(0, pair)] = (dot_nn(ds, k2) * SCALE).astype(BF16)
        dk = dot_tn(ds, qkv_ref[rows_of(g), part(0, pair)])
        dqkv_ref[rows_of(g), part(1, pair)] = (jnp.where(low, dk[:GROUP], dk[GROUP:]) * SCALE).astype(BF16)


CHUNK = 512
CHUNKS = HIDDEN // CHUNK


def cut(c):
    return pl.ds(c * CHUNK, CHUNK)


def gains(ln_ref):
    ln = ln_ref[...].astype(F32)
    return [ln[r:r + 1, :] for r in range(4)]


def position():
    me = lax.axis_index('sp')
    y, x, c = me // 4, (me // 2) % 2, me % 2
    return me, y, x, c, 4 * y + 2 * x + 1 - c, 4 * y + 2 * (1 - x) + c, 4 * (1 - y) + 2 * x + c


def peer(d):
    return lax.rem(lax.axis_index('sp') + d, N_DEV)


def enter():
    barrier = pltpu.get_barrier_semaphore()
    for d in range(1, N_DEV):
        pl.semaphore_signal(barrier, inc=1, device_id={'sp': peer(d)}, device_id_type=pl.DeviceIdType.MESH)
    pl.semaphore_wait(barrier, N_DEV - 1)


def remote(src, dst, send_sem, recv_sem, device):
    return pltpu.make_async_remote_copy(src_ref=src, dst_ref=dst, send_sem=send_sem, recv_sem=recv_sem,
                                        device_id={'sp': device}, device_id_type=pl.DeviceIdType.MESH)


def videos_of(i):
    return pl.ds(i * NV, NV)


class Exchange:
    def __init__(self, stage, landing, sems):
        self.stage, self.landing, (self.send, self.recv, self.own) = stage, landing, sems

    def copies(self, i):
        me, slot = lax.axis_index('sp'), i % 2
        return [remote(self.stage.at[slot, peer(d)], self.landing(me, i), self.send.at[slot, d], self.recv.at[i, d], peer(d))
                for d in range(1, N_DEV)]

    def local(self, i):
        me, slot = lax.axis_index('sp'), i % 2
        return pltpu.make_async_copy(self.stage.at[slot, me], self.landing(me, i), self.own.at[slot])

    def start(self, i):
        for copy in self.copies(i):
            copy.start()
        self.local(i).start()

    def wait_sent(self, i):
        for copy in self.copies(i):
            copy.wait_send()
        self.local(i).wait()

    def wait_received(self, i):
        slot = i % 2
        for d in range(1, N_DEV):
            remote(self.stage.at[slot, 0], self.landing(peer(N_DEV - d), i), self.send.at[slot, d], self.recv.at[i, d],
                   peer(d)).wait_recv()

    def free_slot(self, i):
        @pl.when(i >= 2)
        def _():
            self.wait_sent(i - 2)

    def finish(self, n):
        self.wait_sent(n - 2)
        self.wait_sent(n - 1)

        def body(i, carry):
            self.wait_received(i)
            return carry
        lax.fori_loop(0, n, body, 0)


EXCHANGE_SEMS = [pltpu.SemaphoreType.DMA((2, N_DEV)), pltpu.SemaphoreType.DMA((STEPS, N_DEV)),
                 pltpu.SemaphoreType.DMA((2,))]


def spatial_forward_kernel(x_ref, dy_ref, ln_ref, wqkv_ref, wout_ref, wup_ref, wdown_ref, bias_ref, perm_ref,
                           mid_ref, dy_early_ref, dyp_ref, h_ref, o_ref, qkv_ref, p_ref, act_ref, s_ref,
                           stage_ref, dy_stage_ref, *sems):
    step = pl.program_id(0)
    exchange = Exchange(stage_ref, lambda src, i: mid_ref.at[src, videos_of(i)], sems[0:3])
    exchange_dy = Exchange(dy_stage_ref, lambda src, i: dy_early_ref.at[src, videos_of(i)], sems[3:6])

    @pl.when(step == 0)
    def _():
        enter()

    for v in range(NV):
        moved = dot_nn(perm_ref[...], dy_ref[pl.ds(v * ROWS, ROWS), :]).astype(BF16)
        for d in range(N_DEV):
            dyp_ref[d, v] = moved[d * 32:(d + 1) * 32]

    @pl.when(step < EARLY)
    def _():
        exchange_dy.free_slot(step)
        dy_stage_ref[step % 2] = dyp_ref[...]

    gain1, shift1, gain2, shift2 = gains(ln_ref)
    normed, _ = norm_stats(x_ref[...].astype(F32))
    a_in = (normed * gain1 + shift1).astype(BF16)
    for c in range(3):
        cols = pl.ds(c * WIDTH, WIDTH)
        qkv_ref[:, cols] = dot_nn(a_in, wqkv_ref[:, cols]).astype(BF16)

    @pl.when(step < EARLY)
    def _():
        exchange_dy.start(step)

    attend(qkv_ref, bias_ref, p_ref, o_ref, s_ref)
    h_ref[...] = (x_ref[...].astype(F32) + dot_nn(o_ref[...], wout_ref[...])).astype(BF16)
    normed, _ = norm_stats(h_ref[...].astype(F32))
    m_in = (normed * gain2 + shift2).astype(BF16)
    for c in range(CHUNKS):
        act_ref[:, cut(c)] = gelu_value(dot_nn(m_in, wup_ref[:, cut(c)])).astype(BF16)
    out = (h_ref[...].astype(F32) + dot_nn(act_ref[...], wdown_ref[...])).astype(BF16)
    exchange.free_slot(step)
    for v in range(NV):
        moved = dot_nn(perm_ref[...], out[v * ROWS:(v + 1) * ROWS]).astype(BF16)
        for d in range(N_DEV):
            stage_ref[step % 2, d, v] = moved[d * 32:(d + 1) * 32]
    exchange.start(step)

    @pl.when(step == STEPS - 1)
    def _():
        exchange_dy.finish(EARLY)
        exchange.finish(STEPS)


def add_blocks(sum_ref, first, product):
    for c in range(product.shape[1] // WIDTH):
        rows = pl.ds(first + c * WIDTH, WIDTH)
        sum_ref[rows, :] += product[:, c * WIDTH:(c + 1) * WIDTH]


def tail_backward(dv_ref, o_ref, m_ref, normed, inv_std, gain2, gp_ref, act_ref, dup_ref, do_ref,
                  wout_ref, wup_ref, wdown_ref, sum_ref):
    add_blocks(sum_ref, ROW_DOWN, dot_tn(dv_ref[...], act_ref[...]))
    for c in range(CHUNKS):
        d_act = dot_nt(dv_ref[...], wdown_ref[cut(c), :]).astype(BF16).astype(F32)
        dup_ref[:, cut(c)] = (d_act * gp_ref[:, cut(c)]).astype(BF16)
    add_blocks(sum_ref, ROW_UP, dot_tn(m_ref[...], dup_ref[...]))
    d_m = dot_nt(dup_ref[...], wup_ref[...]).astype(BF16).astype(F32)
    d_h, g_gain, g_shift = norm_back(d_m, normed, inv_std, gain2)
    dv_ref[...] = (d_h + dv_ref[...].astype(F32)).astype(BF16)
    add_blocks(sum_ref, ROW_OUT, dot_tn(o_ref[...], dv_ref[...]))
    do_ref[...] = dot_nt(dv_ref[...], wout_ref[...]).astype(BF16)
    return g_gain, g_shift


def qkv_backward(u32, a_ref, dh_ref, dqkv_ref, gain1, wqkv_ref, sum_ref):
    normed, inv_std = norm_stats(u32)
    add_blocks(sum_ref, ROW_QKV, dot_tn(a_ref[...], dqkv_ref[...]))
    d_a = dot_nt(dqkv_ref[...], wqkv_ref[...]).astype(BF16).astype(F32)
    d_in, g_gain, g_shift = norm_back(d_a, normed, inv_std, gain1)
    return (d_in + dh_ref[...].astype(F32)).astype(BF16), g_gain, g_shift


def up_forward(h32, gain2, shift2, m_ref, wup_ref, act_ref, gp_ref):
    normed, inv_std = norm_stats(h32)
    m_ref[...] = (normed * gain2 + shift2).astype(BF16)
    for c in range(CHUNKS):
        act, slope = gelu_parts(dot_nn(m_ref[...], wup_ref[:, cut(c)]))
        act_ref[:, cut(c)] = act.astype(BF16)
        gp_ref[:, cut(c)] = slope
    return normed, inv_std


def add_ln_sums(ref, first, sums):
    for r, g in enumerate(sums):
        ref[first + r:first + r + 1, :] += g


def temporal_kernel(mid_ref, dy_early_ref, dyp_ref, ln_ref, wqkv_ref, wout_ref, wup_ref, wdown_ref, bias_ref,
                    back_ref, sum_ref, u_ref, dv_ref, a_ref, qkv_ref, p_ref, o_ref, m_ref, act_ref,
                    dup_ref, do_ref, dqkv_ref, dp_ref, gp_ref, s_ref, dy_ref, y_stage, dm_stage, *sems):
    step = pl.program_id(0)
    me = lax.axis_index('sp')
    send_y = Exchange(y_stage, lambda src, i: back_ref.at[src, 0, videos_of(i)], sems[0:3])
    send_dm = Exchange(dm_stage, lambda src, i: back_ref.at[src, 1, videos_of(i)], sems[3:6])
    dy_send, dy_recv, dy_own = sems[6:]

    def dy_copy(i, d):
        return remote(dyp_ref.at[peer(d), videos_of(i)], dy_ref.at[me, videos_of(i)], dy_send.at[i, d], dy_recv.at[i, d],
                      peer(d))

    late = pl.ds(EARLY * NV, VIDEOS - EARLY * NV)
    dy_local = pltpu.make_async_copy(dyp_ref.at[me, late], dy_ref.at[me, late], dy_own.at[0])
    dy_early = pltpu.make_async_copy(dy_early_ref, dy_ref.at[:, pl.ds(0, EARLY * NV)], dy_own.at[1])

    @pl.when(step == 0)
    def _():
        enter()
        dy_early.start()
        dy_local.start()
        for i in range(EARLY, STEPS):
            for d in range(1, N_DEV):
                dy_copy(i, d).start()
        sum_ref[...] = jnp.zeros_like(sum_ref)

    gain1, shift1, gain2, shift2 = gains(ln_ref)
    places = [(v, g, s) for v in range(NV) for g in range(2) for s in range(N_DEV)]
    for v, g, s in places:
        u_ref[pl.ds(v * ROWS + g * GROUP + s * 16, 16), :] = mid_ref[s, v, pl.ds(g * 16, 16), :]
    normed1, _ = norm_stats(u_ref[...].astype(F32))
    a_ref[...] = (normed1 * gain1 + shift1).astype(BF16)
    for c in range(3):
        cols = pl.ds(c * WIDTH, WIDTH)
        qkv_ref[:, cols] = dot_nn(a_ref[...], wqkv_ref[:, cols]).astype(BF16)
    attend(qkv_ref, bias_ref, p_ref, o_ref, s_ref)
    h = (u_ref[...].astype(F32) + dot_nn(o_ref[...], wout_ref[...])).astype(BF16)
    h32 = h.astype(F32)
    normed, inv_std = up_forward(h32, gain2, shift2, m_ref, wup_ref, act_ref, gp_ref)
    out = (h32 + dot_nn(act_ref[...], wdown_ref[...])).astype(BF16)
    send_y.free_slot(step)
    for v, g, s in places:
        src = v * ROWS + g * GROUP + s * 16
        y_stage[step % 2, s, v, pl.ds(g * 16, 16), :] = out[src:src + 16]

    @pl.when(step == 0)
    def _():
        dy_early.wait()
        dy_local.wait()

    @pl.when(step >= EARLY)
    def _():
        for d in range(1, N_DEV):
            remote(dyp_ref.at[0, videos_of(step)], dy_ref.at[peer(N_DEV - d), videos_of(step)], dy_send.at[step, d],
                   dy_recv.at[step, d], peer(d)).wait_recv()

    for v, g, s in places:
        dv_ref[pl.ds(v * ROWS + g * GROUP + s * 16, 16), :] = dy_ref[s, step * NV + v, pl.ds(g * 16, 16), :]
    send_y.start(step)
    g_gain2, g_shift2 = tail_backward(dv_ref, o_ref, m_ref, normed, inv_std, gain2, gp_ref, act_ref, dup_ref, do_ref,
                                      wout_ref, wup_ref, wdown_ref, sum_ref)
    attend_back(qkv_ref, p_ref, do_ref, dqkv_ref, dp_ref)
    d_in, g_gain1, g_shift1 = qkv_backward(u_ref[...].astype(F32), a_ref, dv_ref, dqkv_ref, gain1, wqkv_ref, sum_ref)
    add_ln_sums(sum_ref, SUM_ROWS, (g_gain1, g_shift1, g_gain2, g_shift2))
    send_dm.free_slot(step)
    for v, g, s in places:
        src = v * ROWS + g * GROUP + s * 16
        dm_stage[step % 2, s, v, pl.ds(g * 16, 16), :] = d_in[src:src + 16]
    send_dm.start(step)

    @pl.when(step == STEPS - 1)
    def _():
        for i in range(EARLY, STEPS):
            for d in range(1, N_DEV):
                dy_copy(i, d).wait_send()
        send_y.finish(STEPS)
        send_dm.finish(STEPS)


def span(k, idx, n):
    return pl.ds(pl.multiple_of(k * LAP_ROWS + idx * BLOCK, 8), n * BLOCK)


def slot(k, idx, n):
    return pl.ds((k * SLOTS + idx) * BLOCK, n * BLOCK)


class Reduce:
    def __init__(self, sum_ref, first_ref, landing_ref, sems, credits, block, out_sems):
        self.sum, self.first, self.landing = sum_ref, first_ref, landing_ref
        self.sems, self.credits, self.block, self.out_sems = sems, credits, block, out_sems

    def moves(self, phase):
        _, y, x, c, partner, xn, yn = position()
        own0, own1 = c * 8 + x * 2, c * 8 + 4 + y * 2
        return (
            [((1 - c) * 8, 8, 0, partner)],
            [(c * 8 + (1 - x) * 2, 2, 8, xn), (c * 8 + 4 + (1 - y) * 2, 2, 10, yn)],
            [(own0 + 1 - y, 1, 12, yn), (own1 + 1 - x, 1, 13, xn)],
            [(own0 + y, 1, None, yn), (own1 + x, 1, None, xn)],
            [(own0, 2, None, xn), (own1, 2, None, yn)],
            [(c * 8, 8, None, partner)],
        )[phase]

    def copies(self, phase, k):
        source = self.first if phase == 0 else self.sum
        copies = []
        for j, (idx, n, place, device) in enumerate(self.moves(phase)):
            dst = self.sum.at[span(k, idx, n), :] if place is None else self.landing.at[slot(k, place, n), :]
            copies.append(remote(source.at[span(k, idx, n), :], dst, self.sems.at[0, phase, k, j],
                                 self.sems.at[1, phase, k, j], device))
        return copies

    def start(self, phase, k):
        for j, copy in enumerate(self.copies(phase, k)):
            if phase >= 3:
                pl.semaphore_wait(self.credits.at[5 - phase, k, j], 1)
            copy.start()

    def finish(self, phase, k):
        for j, copy in enumerate(self.copies(phase, k)):
            copy.wait()
            if phase < 3:
                pl.semaphore_signal(self.credits.at[phase, k, j], inc=1, device_id={'sp': self.moves(phase)[j][3]},
                                    device_id_type=pl.DeviceIdType.MESH)
        _, y, x, c, _, _, _ = position()
        own0, own1 = c * 8 + x * 2, c * 8 + 4 + y * 2
        adds = ([(c * 8, 8, 0)], [(own0, 2, 8), (own1, 2, 10)], [(own0 + y, 1, 12), (own1 + x, 1, 13)], (), (), ())
        for idx, n, place in adds[phase]:
            def body(i, carry):
                rows = pl.ds(pl.multiple_of((k * SLOTS + place + i) * BLOCK, 8), BLOCK)
                self.sum[span(k, idx + i, 1), :] += self.landing[rows, :]
                return carry
            lax.fori_loop(0, n, body, 0)
        if phase == 5:
            for r in self.pieces(k):
                if r >= 8:
                    rows = pl.ds(r * WIDTH, WIDTH)
                    self.sum[rows, :] = self.sum[rows, :].T

    def pieces(self, k):
        return range(k * LAP_ROWS // WIDTH, (k + 1) * LAP_ROWS // WIDTH)

    def out_copy(self, r, outs):
        qkv_ref, out_ref, up_ref, down_ref = outs
        b = self.block
        if r < 3:
            dst = qkv_ref.at[b, :, pl.ds(r * WIDTH, WIDTH)]
        elif r == 3:
            dst = out_ref.at[b]
        elif r < 8:
            dst = up_ref.at[b, :, pl.ds((r - 4) * WIDTH, WIDTH)]
        else:
            dst = down_ref.at[b, pl.ds((r - 8) * WIDTH, WIDTH), :]
        return pltpu.make_async_copy(self.sum.at[pl.ds(r * WIDTH, WIDTH), :], dst, self.out_sems.at[r])


def reduce_plan():
    lasts = (1.4, 4.75, 2.4, 2.4, 4.75, 1.4)
    free, running, plan, now = [0.0, 0.0], {}, [], 0.0

    def start(lap, phase):
        link = 0 if phase in (0, 5) else 1
        free[link] = max(free[link], now) + lasts[phase]
        running[lap] = (phase, free[link] + 2.0)

    def turn(due):
        nonlocal now
        turns = [(lap, phase) for lap, (phase, end) in sorted(running.items(), key=lambda item: item[1][1]) if end <= due]
        for lap, phase in turns:
            now = max(now, running.pop(lap)[1])
            if phase < 5:
                start(lap, phase + 1)
        return turns

    def begin(laps):
        for lap in laps:
            start(lap, 0)
        return [], laps

    for step in range(2 * STEPS):
        turns = []
        if step == STEPS:
            turns.append(begin([('s', 1), ('s', 2), ('s', 3)]))
        if step == 0:
            turns.append(begin([('t', 1), ('t', 2), ('t', 3), ('t', 0)]))
        turns.append((turn(now), []))
        plan.append([t for t in turns if any(t)])
        now += 6.0 if step < STEPS else 4.3
    turns = [begin([('s', 0)])]
    while running:
        turns.append((turn(min(end for _, end in running.values())), []))
    plan.append(turns)
    return plan


def ln_copies(ln_ref, sems):
    me = lax.axis_index('sp')
    return [pltpu.make_async_remote_copy(
        src_ref=ln_ref.at[me], dst_ref=ln_ref.at[me], send_sem=sems.at[0, d], recv_sem=sems.at[1, d],
        device_id={'sp': lax.rem(me + d, N_DEV)}, device_id_type=pl.DeviceIdType.MESH) for d in range(1, N_DEV)]


def spatial_backward_kernel(*refs):
    (back_ref, x_ref, h_ref, o_ref, qkv_ref, p_ref,
     ln_ref, wqkv_ref, wout_ref, wup_ref, wdown_ref, perm_ref, gt_ref) = refs[:13]
    (y_ref, dx_ref, gqkv_ref, gout_ref, gup_ref, gdown_ref, gln_ref,
     dv_ref, a_ref, m_ref, act_ref, dup_ref, do_ref, dqkv_ref, dp_ref, gp_ref, dh_all_ref, do_all_ref,
     sum_ref, t_ref, land_s_ref, land_t_ref, ln_s_ref, ln_all_ref, sems_s, sems_t, credits_s, credits_t,
     sems_out_s, sems_out_t, sems_ln, sems_in) = refs[13:]
    step = pl.program_id(0)
    me = lax.axis_index('sp')
    load_t = pltpu.make_async_copy(gt_ref.at[pl.ds(0, SUM_ROWS), :], t_ref, sems_in.at[0])
    load_ln = pltpu.make_async_copy(gt_ref.at[pl.ds(SUM_ROWS, 8), :], ln_all_ref.at[me, pl.ds(0, 8), :], sems_in.at[1])
    sums = {'t': Reduce(t_ref, gt_ref, land_t_ref, sems_t, credits_t, 1, sems_out_t),
            's': Reduce(sum_ref, sum_ref, land_s_ref, sems_s, credits_s, 0, sems_out_s)}
    outs = (gqkv_ref, gout_ref, gup_ref, gdown_ref)
    plan = reduce_plan()
    written = []

    def advance(turns, fresh):
        for (which, k), phase in turns:
            sums[which].finish(phase, k)
        for which, k in fresh:
            sums[which].start(0, k)
        for (which, k), phase in turns:
            if phase < 5:
                sums[which].start(phase + 1, k)
        while written:
            which, k = written.pop()
            for r in sums[which].pieces(k):
                sums[which].out_copy(r, outs).start()
        written.extend(lap for lap, phase in turns if phase == 5)

    @pl.when(step == 0)
    def _():
        enter()
        load_t.start()
        load_ln.start()
        advance(*plan[0][0])
        sum_ref[...] = jnp.zeros_like(sum_ref)
        ln_s_ref[...] = jnp.zeros_like(ln_s_ref)
        load_t.wait()
        load_ln.wait()
        for turns in plan[0][1:]:
            advance(*turns)

    for at in range(1, 2 * STEPS):
        if plan[at]:
            @pl.when(step == at)
            def _(at=at):
                for turns in plan[at]:
                    advance(*turns)

    gain1, shift1, gain2, shift2 = gains(ln_ref)

    @pl.when(step < STEPS)
    def _():
        mine = pl.ds(pl.multiple_of(step * STEP_ROWS, STEP_ROWS), STEP_ROWS)
        for v in range(NV):
            rows = pl.ds(v * ROWS, ROWS)
            dv_ref[rows, :] = dot_tn(perm_ref[...], back_ref[:, 1, v].reshape(ROWS, WIDTH)).astype(BF16)
            y_ref[rows, :] = dot_tn(perm_ref[...], back_ref[:, 0, v].reshape(ROWS, WIDTH)).astype(BF16)
        normed, inv_std = up_forward(h_ref[...].astype(F32), gain2, shift2, m_ref, wup_ref, act_ref, gp_ref)
        g_gain2, g_shift2 = tail_backward(dv_ref, o_ref, m_ref, normed, inv_std, gain2, gp_ref, act_ref, dup_ref, do_ref,
                                          wout_ref, wup_ref, wdown_ref, sum_ref)
        dh_all_ref[mine, :] = dv_ref[...]
        do_all_ref[mine, :] = do_ref[...]
        add_ln_sums(ln_s_ref, 2, (g_gain2, g_shift2))

    @pl.when(step >= STEPS)
    def _():
        mine = pl.ds(pl.multiple_of((step - STEPS) * STEP_ROWS, STEP_ROWS), STEP_ROWS)
        dv_ref[...] = dh_all_ref[mine, :]
        do_ref[...] = do_all_ref[mine, :]
        normed1, _ = norm_stats(x_ref[...].astype(F32))
        a_ref[...] = (normed1 * gain1 + shift1).astype(BF16)
        attend_back(qkv_ref, p_ref, do_ref, dqkv_ref, dp_ref)
        d_in, g_gain1, g_shift1 = qkv_backward(x_ref[...].astype(F32), a_ref, dv_ref, dqkv_ref, gain1, wqkv_ref, sum_ref)
        add_ln_sums(ln_s_ref, 0, (g_gain1, g_shift1))
        dx_ref[...] = d_in

    @pl.when(step == 2 * STEPS - 1)
    def _():
        ln_all_ref[me, pl.ds(8, 8), :] = ln_s_ref[...]
        for n, (turns, fresh) in enumerate(plan[2 * STEPS]):
            advance(turns, fresh)
            if n == 0:
                for copy in ln_copies(ln_all_ref, sems_ln):
                    copy.start()
            if n == 3:
                for copy in ln_copies(ln_all_ref, sems_ln):
                    copy.wait()
                total = ln_all_ref[0]
                for d in range(1, N_DEV):
                    total += ln_all_ref[d]
                gln_ref[0] = total[8:12]
                gln_ref[1] = total[0:4]
        advance((), ())
        for which in 'ts':
            for r in range(12):
                sums[which].out_copy(r, outs).wait()


def full(shape):
    return pl.BlockSpec(shape, lambda i: (0,) * len(shape), pipeline_mode=pl.Buffered(1))


def weight_specs(block):
    shapes = [(4, WIDTH), (WIDTH, QKV), (WIDTH, WIDTH), (WIDTH, HIDDEN), (HIDDEN, WIDTH)]
    return [pl.BlockSpec((None,) + s, lambda i: (block, 0, 0), pipeline_mode=pl.Buffered(1)) for s in shapes]


def rows_spec(width):
    return pl.BlockSpec((STEP_ROWS, width), lambda i: (i, 0))


def swap_spec():
    return pl.BlockSpec((N_DEV, NV, 32, WIDTH), lambda i: (0, i, 0, 0))


ANY = pl.BlockSpec(memory_space=pl.ANY)


def params(collective_id):
    return pltpu.CompilerParams(dimension_semantics=("arbitrary",), vmem_limit_bytes=VMEM_LIMIT,
                                collective_id=collective_id, has_side_effects=True)


def cost(us, mib):
    return pl.CostEstimate(flops=int(us * 9e8), bytes_accessed=int(mib * 2 ** 20), transcendentals=0)


def sds(shape, dtype):
    return jax.ShapeDtypeStruct(shape, dtype)


def vm(width, dtype=BF16):
    return pltpu.VMEM((STEP_ROWS, width), dtype)


TOKENS = VIDEOS * ROWS
PROBS = 6 * GROUP
SWAP = (N_DEV, VIDEOS, 32, WIDTH)
SWAP_EARLY = (N_DEV, EARLY * NV, 32, WIDTH)
ROW_QKV, ROW_OUT, ROW_UP, ROW_DOWN = 0, 3 * WIDTH, 4 * WIDTH, 8 * WIDTH
SUM_ROWS = 12 * WIDTH
LAPS = 4
LAP_ROWS = SUM_ROWS // LAPS
BLOCK = LAP_ROWS // 16
SLOTS = 14


def spatial_forward_call(x, dy, weights, bias, perm):
    widths = (WIDTH, WIDTH, QKV, PROBS)
    return pl.pallas_call(
        spatial_forward_kernel, grid=(STEPS,), name="spatial_fwd",
        in_specs=[rows_spec(WIDTH)] * 2 + weight_specs(0) + [full((GROUP, 2 * GROUP)), full((ROWS, ROWS))],
        out_specs=[ANY, ANY, swap_spec()] + [rows_spec(w) for w in widths],
        out_shape=[sds(SWAP, BF16), sds(SWAP_EARLY, BF16), sds(SWAP, BF16)] + [sds((TOKENS, w), BF16) for w in widths],
        scratch_shapes=[vm(HIDDEN), vm(PROBS, F32)] + [pltpu.VMEM((2, N_DEV, NV, 32, WIDTH), BF16)] * 2
        + EXCHANGE_SEMS * 2,
        compiler_params=params(1), cost_estimate=cost(50, 40),
    )(x, dy, *weights, bias, perm)


def temporal_call(mid, dy_early, dyp, weights, bias):
    return pl.pallas_call(
        temporal_kernel, grid=(STEPS,), name="temporal",
        in_specs=[swap_spec(), ANY, ANY] + weight_specs(1) + [full((GROUP, 2 * GROUP))],
        out_specs=[ANY, full((SUM_ROWS + 8, WIDTH))],
        out_shape=[sds((N_DEV, 2) + SWAP[1:], BF16), sds((SUM_ROWS + 8, WIDTH), F32)],
        scratch_shapes=[vm(w) for w in (WIDTH, WIDTH, WIDTH, QKV, PROBS, WIDTH, WIDTH, HIDDEN, HIDDEN, WIDTH, QKV, PROBS)]
        + [vm(HIDDEN, F32), vm(PROBS, F32), pltpu.VMEM(SWAP, BF16)]
        + [pltpu.VMEM((2, N_DEV, NV, 32, WIDTH), BF16)] * 2 + EXCHANGE_SEMS * 2
        + [pltpu.SemaphoreType.DMA((STEPS, N_DEV))] * 2 + [pltpu.SemaphoreType.DMA((2,))],
        compiler_params=params(2), cost_estimate=cost(110, 20),
    )(mid, dy_early, dyp, *weights, bias)


def spatial_backward_call(back, x, saved, weights, perm, sum_t):
    def early(width):
        return pl.BlockSpec((STEP_ROWS, width), lambda i: (jnp.minimum(i, STEPS - 1), 0))

    def late(width):
        return pl.BlockSpec((STEP_ROWS, width), lambda i: (jnp.maximum(i - STEPS, 0), 0))

    grads = [(2, WIDTH, QKV), (2, WIDTH, WIDTH), (2, WIDTH, HIDDEN), (2, HIDDEN, WIDTH)]
    return pl.pallas_call(
        spatial_backward_kernel, grid=(2 * STEPS,), name="spatial_bwd",
        in_specs=[pl.BlockSpec((N_DEV, 2, NV, 32, WIDTH), lambda i: (0, 0, jnp.minimum(i, STEPS - 1), 0, 0))]
        + [late(WIDTH), early(WIDTH), early(WIDTH), late(QKV), late(PROBS)] + weight_specs(0) + [full((ROWS, ROWS)), ANY],
        out_specs=[early(WIDTH), late(WIDTH)] + [ANY] * 4 + [full((2, 4, WIDTH))],
        out_shape=[sds((TOKENS, WIDTH), BF16)] * 2 + [sds(g, F32) for g in grads] + [sds((2, 4, WIDTH), F32)],
        scratch_shapes=[vm(w) for w in (WIDTH, WIDTH, WIDTH, HIDDEN, HIDDEN, WIDTH, QKV, PROBS)] + [vm(HIDDEN, F32)]
        + [pltpu.VMEM((TOKENS, WIDTH), BF16)] * 2
        + [pltpu.VMEM((SUM_ROWS, WIDTH), F32)] * 2 + [pltpu.VMEM((LAPS * SLOTS * BLOCK, WIDTH), F32)] * 2
        + [pltpu.VMEM((8, WIDTH), F32), pltpu.VMEM((N_DEV, 16, WIDTH), F32)]
        + [pltpu.SemaphoreType.DMA((2, 6, LAPS, 2))] * 2 + [pltpu.SemaphoreType.REGULAR((3, LAPS, 2))] * 2
        + [pltpu.SemaphoreType.DMA((12,))] * 2 + [pltpu.SemaphoreType.DMA((2, N_DEV)), pltpu.SemaphoreType.DMA((2,))],
        compiler_params=params(3), cost_estimate=cost(160, 60),
    )(back, x, *saved, *weights, perm, sum_t)


def constants():
    row = np.arange(ROWS)
    dev, patch, frame = row // 32, (row // 8) % 4, row % 8
    perm = np.zeros((ROWS, ROWS), np.float32)
    perm[row, frame * 32 + dev * 4 + patch] = 1.0
    r = np.arange(GROUP)
    frame_of = r // 32
    patch_of = (r // 8) % 2
    bias_s = np.where(frame_of[:, None] == frame_of[None], 0.0, -np.inf).astype(np.float32)
    bias_t = np.where(patch_of[:, None] == patch_of[None], 0.0, -np.inf).astype(np.float32)
    return perm, np.concatenate([bias_s] * 2, 1), np.concatenate([bias_t] * 2, 1)


def device_step(latents, cotangent, ln_params, w_qkv, w_out, w_up, w_down):
    perm, bias_s, bias_t = constants()
    perm = jnp.asarray(perm, BF16)
    bias_s, bias_t = jnp.asarray(bias_s), jnp.asarray(bias_t)
    weights = (ln_params, w_qkv, w_out.reshape(2, WIDTH, WIDTH), w_up, w_down)
    x = latents.reshape(TOKENS, WIDTH)
    dy = cotangent.reshape(TOKENS, WIDTH)

    mid, dy_early, dyp, *saved = spatial_forward_call(x, dy, weights, bias_s, perm)
    back, sum_t = temporal_call(mid, dy_early, dyp, weights, bias_t)
    y, dx, g_qkv, g_out, g_up, g_down, g_ln = spatial_backward_call(back, x, saved, weights, perm, sum_t)
    g_out = g_out.reshape(2, 6, 64, WIDTH)
    shape = latents.shape
    return y.reshape(shape), dx.reshape(shape), g_ln, g_qkv, g_out, g_up, g_down


def solution(mesh):
    act_spec = P('data', 'sp', None, None)
    replicated = P()
    part_spec = P('data')
    return jax.shard_map(device_step, mesh=mesh,
                         in_specs=(act_spec, act_spec, replicated, replicated, replicated, replicated, replicated),
                         out_specs=(act_spec, act_spec, part_spec, part_spec, part_spec, part_spec, part_spec),
                         check_vma=False)
```

```python
import itertools

import jax
import jax.numpy as jnp
import numpy as np
from jax import lax
from jax.experimental import pallas as pl
from jax.experimental.pallas import tpu as pltpu
from jax.sharding import PartitionSpec as P

BF16 = jnp.bfloat16
F32 = jnp.float32
N_DEV = 8
WIDTH = 384
HIDDEN = 4 * WIDTH
QKV = 3 * WIDTH
VIDEOS = 16
ROWS = 256
NV = 2
STEP_ROWS = ROWS * NV
GROUP = 128
PAIRS = 3
SCALE = 0.125
LOG2E = 1.4426950408889634
STEPS = VIDEOS // NV
GELU_C = 0.7978845608028654
GELU_C3 = GELU_C * 0.044715
VMEM_LIMIT = 62 * 1024 * 1024


def dot_nn(a, b):
    return lax.dot_general(a, b, (((1,), (0,)), ((), ())), preferred_element_type=F32)


def dot_nt(a, b):
    return lax.dot_general(a, b, (((1,), (1,)), ((), ())), preferred_element_type=F32)


def dot_tn(a, b):
    return lax.dot_general(a, b, (((0,), (0,)), ((), ())), preferred_element_type=F32)


def norm_stats(x32):
    centered = x32 - jnp.mean(x32, axis=-1, keepdims=True)
    inv_std = lax.rsqrt(jnp.mean(centered * centered, axis=-1, keepdims=True) + 1e-6)
    return centered * inv_std, inv_std


def norm_back(d_out32, normed, inv_std, gain):
    d_gain = jnp.sum(d_out32 * normed, axis=0, keepdims=True)
    d_shift = jnp.sum(d_out32, axis=0, keepdims=True)
    d_norm = d_out32 * gain
    d_center = d_norm - jnp.mean(d_norm, axis=-1, keepdims=True)
    d_in = inv_std * (d_center - normed * jnp.mean(d_norm * normed, axis=-1, keepdims=True))
    return d_in, d_gain, d_shift


def gelu_slope(x, t):
    half = 0.5 + 0.5 * t
    return half + ((x * half) * (1.0 - t)) * (GELU_C + (3.0 * GELU_C3) * (x * x))


def gelu_value(x):
    t = jnp.tanh(x * (GELU_C + GELU_C3 * (x * x)))
    return x * (0.5 + 0.5 * t)


def lane_masks():
    lane = lax.broadcasted_iota(jnp.int32, (1, GROUP), 1)
    low = (lane < GROUP // 2)
    m_low = jnp.where(low, 1.0, 0.0).astype(BF16)
    m_high = jnp.where(low, 0.0, 1.0).astype(BF16)
    return low, m_low, m_high


def split_heads(k, m_low, m_high):
    return jnp.concatenate([k * m_low, k * m_high], axis=0)


GROUPS = STEP_ROWS // GROUP
BLOCKS = [(g, pair) for g in range(GROUPS) for pair in range(PAIRS)]


def rows_of(g):
    return pl.ds(g * GROUP, GROUP)


def part(kind, pair):
    return pl.ds(kind * WIDTH + pair * GROUP, GROUP)


def both(pair):
    return pl.ds(pair * 2 * GROUP, 2 * GROUP)


def attend(qkv_ref, bias_ref, p_ref, o_ref, s_ref):
    low, m_low, m_high = lane_masks()
    for g, pair in BLOCKS:
        k2 = split_heads(qkv_ref[rows_of(g), part(1, pair)], m_low, m_high)
        s_ref[rows_of(g), both(pair)] = dot_nt(qkv_ref[rows_of(g), part(0, pair)], k2) * (SCALE * LOG2E) + bias_ref[...]
    for g, pair in BLOCKS:
        s = s_ref[rows_of(g), both(pair)]
        probs = []
        for h in range(2):
            s_h = s[:, h * GROUP:(h + 1) * GROUP]
            e_h = jnp.exp2(s_h - jnp.max(s_h, axis=-1, keepdims=True))
            probs.append(e_h * (1.0 / jnp.sum(e_h, axis=-1, keepdims=True)))
        p_ref[rows_of(g), both(pair)] = jnp.concatenate(probs, axis=1).astype(BF16)
    for g, pair in BLOCKS:
        v2 = split_heads(qkv_ref[rows_of(g), part(2, pair)], m_low, m_high)
        o_ref[rows_of(g), part(0, pair)] = dot_nn(p_ref[rows_of(g), both(pair)], v2).astype(BF16)


def attend_back(qkv_ref, p_ref, do_ref, dqkv_ref, dp_ref):
    low, m_low, m_high = lane_masks()
    for g, pair in BLOCKS:
        do = do_ref[rows_of(g), part(0, pair)]
        v2 = split_heads(qkv_ref[rows_of(g), part(2, pair)], m_low, m_high)
        dp_ref[rows_of(g), both(pair)] = dot_nt(do, v2).astype(BF16)
        dv = dot_tn(p_ref[rows_of(g), both(pair)], do)
        dqkv_ref[rows_of(g), part(2, pair)] = jnp.where(low, dv[:GROUP], dv[GROUP:]).astype(BF16)
    for g, pair in BLOCKS:
        p32 = p_ref[rows_of(g), both(pair)].astype(F32)
        t = dp_ref[rows_of(g), both(pair)].astype(F32) * p32
        ds = []
        for h in range(2):
            half = slice(h * GROUP, (h + 1) * GROUP)
            ds.append(t[:, half] - p32[:, half] * jnp.sum(t[:, half], axis=-1, keepdims=True))
        dp_ref[rows_of(g), both(pair)] = jnp.concatenate(ds, axis=1).astype(BF16)
    for g, pair in BLOCKS:
        ds = dp_ref[rows_of(g), both(pair)]
        k2 = split_heads(qkv_ref[rows_of(g), part(1, pair)], m_low, m_high)
        dqkv_ref[rows_of(g), part(0, pair)] = (dot_nn(ds, k2) * SCALE).astype(BF16)
        dk = dot_tn(ds, qkv_ref[rows_of(g), part(0, pair)])
        dqkv_ref[rows_of(g), part(1, pair)] = (jnp.where(low, dk[:GROUP], dk[GROUP:]) * SCALE).astype(BF16)


CHUNK = 512
CHUNKS = HIDDEN // CHUNK


def cut(c):
    return pl.ds(c * CHUNK, CHUNK)


def gains(ln_ref):
    ln = ln_ref[...].astype(F32)
    return [ln[r:r + 1, :] for r in range(4)]


def position():
    me = lax.axis_index('sp')
    y, x, c = me // 4, (me // 2) % 2, me % 2
    return me, y, x, c, me + 1 - 2 * c, me + 2 - 4 * x, me + 4 - 8 * y


def flip(bit, by):
    return bit + by - 2 * bit * by


def peer(d):
    _, y, x, c, _, _, _ = position()
    return 4 * flip(y, d // 4) + 2 * flip(x, (d // 2) % 2) + flip(c, d % 2)


ORDER = (*range(2, N_DEV), 1)


def enter():
    barrier = pltpu.get_barrier_semaphore()
    for d in range(1, N_DEV):
        pl.semaphore_signal(barrier, inc=1, device_id={'sp': peer(d)}, device_id_type=pl.DeviceIdType.MESH)
    pl.semaphore_wait(barrier, N_DEV - 1)


def remote(src, dst, send_sem, recv_sem, device):
    return pltpu.make_async_remote_copy(src_ref=src, dst_ref=dst, send_sem=send_sem, recv_sem=recv_sem,
                                        device_id={'sp': device}, device_id_type=pl.DeviceIdType.MESH)


def videos_of(i):
    return pl.ds(i * NV, NV)


class Exchange:
    def __init__(self, stage, landing, sems, local=True):
        self.stage, self.landing, (self.send, self.recv, self.own) = stage, landing, sems
        self.slots, self.has_local = stage.shape[0], local

    def copies(self, i):
        me, slot = lax.axis_index('sp'), lax.rem(i, self.slots)
        return [remote(self.stage.at[slot, peer(d)], self.landing(me, i), self.send.at[slot, d], self.recv.at[i, d], peer(d))
                for d in ORDER]

    def local(self, i):
        me, slot = lax.axis_index('sp'), lax.rem(i, self.slots)
        return pltpu.make_async_copy(self.stage.at[slot, me], self.landing(me, i), self.own.at[slot])

    def start(self, i):
        for copy in self.copies(i):
            copy.start()
        if self.has_local:
            self.local(i).start()

    def wait_sent(self, i):
        for copy in self.copies(i):
            copy.wait_send()
        if self.has_local:
            self.local(i).wait()

    def wait_received(self, i):
        for d in range(1, N_DEV):
            remote(self.stage.at[0, 0], self.landing(peer(d), i), self.send.at[0, d], self.recv.at[i, d],
                   peer(d)).wait_recv()

    def free_slot(self, i):
        @pl.when(i >= self.slots)
        def _():
            self.wait_sent(i - self.slots)

    def finish_sends(self, n):
        for j in range(self.slots):
            self.wait_sent(jnp.int32(n - self.slots + j))

    def finish(self, n):
        self.finish_sends(n)

        def body(i, carry):
            self.wait_received(i)
            return carry
        lax.fori_loop(0, n, body, 0)


def exchange_sems(slots):
    return [pltpu.SemaphoreType.DMA((slots, N_DEV)), pltpu.SemaphoreType.DMA((STEPS, N_DEV)),
            pltpu.SemaphoreType.DMA((slots,))]


def spatial_forward_step(i, x_ref, dy_ref, ln_ref, wqkv_ref, wout_ref, wup_ref, wdown_ref, bias_ref, perm_ref,
                         h_ref, o_ref, qkv_ref, p_ref, act_ref, s_ref, send_mid, send_dy, mid_ref, dyx_ref):
    me = lax.axis_index('sp')
    slot = lax.rem(i, send_mid.slots)
    send_mid.free_slot(i)
    send_dy.free_slot(i)
    for v in range(NV):
        moved = dot_nn(perm_ref[...], dy_ref[pl.ds(v * ROWS, ROWS), :]).astype(BF16)
        for d in range(N_DEV):
            send_dy.stage[slot, d, v] = moved[d * 32:(d + 1) * 32]
    gain1, shift1, gain2, shift2 = gains(ln_ref)
    normed, _ = norm_stats(x_ref[...].astype(F32))
    a_in = (normed * gain1 + shift1).astype(BF16)
    for c in range(3):
        cols = pl.ds(c * WIDTH, WIDTH)
        qkv_ref[:, cols] = dot_nn(a_in, wqkv_ref[:, cols]).astype(BF16)
    attend(qkv_ref, bias_ref, p_ref, o_ref, s_ref)
    h_ref[...] = (x_ref[...].astype(F32) + dot_nn(o_ref[...], wout_ref[...])).astype(BF16)
    normed, _ = norm_stats(h_ref[...].astype(F32))
    m_in = (normed * gain2 + shift2).astype(BF16)
    for c in range(CHUNKS):
        act_ref[:, cut(c)] = gelu_value(dot_nn(m_in, wup_ref[:, cut(c)])).astype(BF16)
    out = (h_ref[...].astype(F32) + dot_nn(act_ref[...], wdown_ref[...])).astype(BF16)
    for v in range(NV):
        moved = dot_nn(perm_ref[...], out[v * ROWS:(v + 1) * ROWS]).astype(BF16)
        for d in range(N_DEV):
            send_mid.stage[slot, d, v] = moved[d * 32:(d + 1) * 32]
    for v in range(NV):
        dyx_ref[me, i * NV + v] = send_dy.stage[slot, me, v]
        mid_ref[me, i * NV + v] = send_mid.stage[slot, me, v]
    send_mid.start(i)
    send_dy.start(i)


def add_blocks(sum_ref, first, product):
    for c in range(product.shape[1] // WIDTH):
        rows = pl.ds(first + c * WIDTH, WIDTH)
        sum_ref[rows, :] += product[:, c * WIDTH:(c + 1) * WIDTH]


def tail_backward(dv_ref, o_ref, m_ref, normed, inv_std, gain2, pre_ref, tanh_ref, act_ref, dup_ref, do_ref,
                  wout_ref, wup_ref, wdown_ref, sum_ref):
    add_blocks(sum_ref, ROW_DOWN, dot_tn(dv_ref[...], act_ref[...]))
    for c in range(CHUNKS):
        d_act = dot_nt(dv_ref[...], wdown_ref[cut(c), :]).astype(BF16).astype(F32)
        dup_ref[:, cut(c)] = (d_act * gelu_slope(pre_ref[:, cut(c)], tanh_ref[:, cut(c)])).astype(BF16)
    add_blocks(sum_ref, ROW_UP, dot_tn(m_ref[...], dup_ref[...]))
    d_m = dot_nt(dup_ref[...], wup_ref[...]).astype(BF16).astype(F32)
    d_h, g_gain, g_shift = norm_back(d_m, normed, inv_std, gain2)
    dv_ref[...] = (d_h + dv_ref[...].astype(F32)).astype(BF16)
    add_blocks(sum_ref, ROW_OUT, dot_tn(o_ref[...], dv_ref[...]))
    do_ref[...] = dot_nt(dv_ref[...], wout_ref[...]).astype(BF16)
    return g_gain, g_shift


def qkv_backward(u32, a_ref, dh_ref, dqkv_ref, gain1, wqkv_ref, sum_ref):
    normed, inv_std = norm_stats(u32)
    add_blocks(sum_ref, ROW_QKV, dot_tn(a_ref[...], dqkv_ref[...]))
    d_a = dot_nt(dqkv_ref[...], wqkv_ref[...]).astype(BF16).astype(F32)
    d_in, g_gain, g_shift = norm_back(d_a, normed, inv_std, gain1)
    return (d_in + dh_ref[...].astype(F32)).astype(BF16), g_gain, g_shift


def up_forward(h32, gain2, shift2, m_ref, wup_ref, act_ref, pre_ref, tanh_ref):
    normed, inv_std = norm_stats(h32)
    m_ref[...] = (normed * gain2 + shift2).astype(BF16)
    for c in range(CHUNKS):
        x = dot_nn(m_ref[...], wup_ref[:, cut(c)])
        t = jnp.tanh(x * (GELU_C + GELU_C3 * (x * x)))
        act_ref[:, cut(c)] = (x * (0.5 + 0.5 * t)).astype(BF16)
        pre_ref[:, cut(c)] = x
        tanh_ref[:, cut(c)] = t
    return normed, inv_std


def add_ln_sums(ref, first, sums):
    for r, g in enumerate(sums):
        ref[first + r:first + r + 1, :] += g


def temporal_step(i, ln_ref, wqkv_ref, wout_ref, wup_ref, wdown_ref, bias_ref, sum_ref, mid_ref, dyx_ref,
                  send_mid, send_dy, send_y, send_dm, u_ref, dv_ref, a_ref, qkv_ref, p_ref, o_ref, m_ref, act_ref,
                  dup_ref, do_ref, dqkv_ref, dp_ref, pre_ref, tanh_ref, s_ref):
    send_mid.wait_received(i)
    send_dy.wait_received(i)
    send_y.free_slot(i)
    send_dm.free_slot(i)
    gain1, shift1, gain2, shift2 = gains(ln_ref)
    places = [(v, g, s) for v in range(NV) for g in range(2) for s in range(N_DEV)]
    for v, g, s in places:
        dst = pl.ds(v * ROWS + g * GROUP + s * 16, 16)
        u_ref[dst, :] = mid_ref[s, i * NV + v, pl.ds(g * 16, 16), :]
        dv_ref[dst, :] = dyx_ref[s, i * NV + v, pl.ds(g * 16, 16), :]
    normed1, _ = norm_stats(u_ref[...].astype(F32))
    a_ref[...] = (normed1 * gain1 + shift1).astype(BF16)
    for c in range(3):
        cols = pl.ds(c * WIDTH, WIDTH)
        qkv_ref[:, cols] = dot_nn(a_ref[...], wqkv_ref[:, cols]).astype(BF16)
    attend(qkv_ref, bias_ref, p_ref, o_ref, s_ref)
    h = (u_ref[...].astype(F32) + dot_nn(o_ref[...], wout_ref[...])).astype(BF16)
    h32 = h.astype(F32)
    normed, inv_std = up_forward(h32, gain2, shift2, m_ref, wup_ref, act_ref, pre_ref, tanh_ref)
    out = (h32 + dot_nn(act_ref[...], wdown_ref[...])).astype(BF16)
    for v, g, s in places:
        src = v * ROWS + g * GROUP + s * 16
        send_y.stage[lax.rem(i, send_y.slots), s, v, pl.ds(g * 16, 16), :] = out[src:src + 16]
    send_y.start(i)
    g_gain2, g_shift2 = tail_backward(dv_ref, o_ref, m_ref, normed, inv_std, gain2, pre_ref, tanh_ref, act_ref, dup_ref, do_ref,
                                      wout_ref, wup_ref, wdown_ref, sum_ref)
    attend_back(qkv_ref, p_ref, do_ref, dqkv_ref, dp_ref)
    d_in, g_gain1, g_shift1 = qkv_backward(u_ref[...].astype(F32), a_ref, dv_ref, dqkv_ref, gain1, wqkv_ref, sum_ref)
    add_ln_sums(sum_ref, SUM_ROWS, (g_gain1, g_shift1, g_gain2, g_shift2))
    for v, g, s in places:
        src = v * ROWS + g * GROUP + s * 16
        send_dm.stage[lax.rem(i, send_dm.slots), s, v, pl.ds(g * 16, 16), :] = d_in[src:src + 16]
    send_dm.start(i)


def forward_kernel(x_ref, dy_ref, *refs):
    refs = iter(refs)

    def take(n):
        return list(itertools.islice(refs, n))

    spatial_w, temporal_w, (bias_s_ref, bias_t_ref, perm_ref) = take(5), take(5), take(3)
    back_ref, sum_ref, h_ref, o_ref, qkv_ref, p_ref = take(6)
    mine, (pre_ref, tanh_ref, s_ref), (mid_ref, dyx_ref) = take(12), take(3), take(2)
    mid_stage, dy_stage, y_stage, dm_stage = take(4)
    mid_sems, dy_sems, y_sems, dm_sems = [take(3) for _ in BLOCKS[:4]]
    step = pl.program_id(0)
    send_mid = Exchange(mid_stage, lambda src, i: mid_ref.at[src, videos_of(i)], mid_sems, local=False)
    send_dy = Exchange(dy_stage, lambda src, i: dyx_ref.at[src, videos_of(i)], dy_sems, local=False)
    send_y = Exchange(y_stage, lambda src, i: back_ref.at[src, 0, videos_of(i)], y_sems)
    send_dm = Exchange(dm_stage, lambda src, i: back_ref.at[src, 1, videos_of(i)], dm_sems)

    @pl.when(step == 0)
    def _():
        enter()
        sum_ref[...] = jnp.zeros_like(sum_ref)

    @pl.when(step < STEPS)
    def _():
        spatial_forward_step(step, x_ref, dy_ref, *spatial_w, bias_s_ref, perm_ref, h_ref, o_ref, qkv_ref, p_ref,
                             mine[7], s_ref, send_mid, send_dy, mid_ref, dyx_ref)

    @pl.when(step >= STEPS)
    def _():
        temporal_step(step - STEPS, *temporal_w, bias_t_ref, sum_ref, mid_ref, dyx_ref,
                      send_mid, send_dy, send_y, send_dm, *mine, pre_ref, tanh_ref, s_ref)

    @pl.when(step == 2 * STEPS - 1)
    def _():
        send_mid.finish_sends(STEPS)
        send_dy.finish_sends(STEPS)
        send_y.finish(STEPS)
        send_dm.finish(STEPS)


def span(k, idx, n):
    return pl.ds(pl.multiple_of(k * LAP_ROWS + idx * BLOCK, 8), n * BLOCK)


def slot(k, idx, n):
    return pl.ds((k * SLOTS + idx) * BLOCK, n * BLOCK)


class Reduce:
    def __init__(self, sum_ref, first_ref, landing_ref, sems, credits, block, out_sems):
        self.sum, self.first, self.landing = sum_ref, first_ref, landing_ref
        self.sems, self.credits, self.block, self.out_sems = sems, credits, block, out_sems

    def owned(self):
        _, y, x, c, _, _, _ = position()
        half = c * 8
        return half, half + x * 2, half + 4 + y * 2

    def moves(self, phase):
        _, y, x, c, partner, xn, yn = position()
        half, own0, own1 = self.owned()
        return (
            [(8 - half, 8, 0, partner)],
            [(own0 + 2 - x * 4, 2, 8, xn), (own1 + 2 - y * 4, 2, 10, yn)],
            [(own0 + 1 - y, 1, 12, yn), (own1 + 1 - x, 1, 13, xn)],
            [(own0 + y, 1, None, yn), (own1 + x, 1, None, xn)],
            [(own0, 2, None, xn), (own1, 2, None, yn)],
            [(half, 8, None, partner)],
        )[phase]

    def copies(self, phase, k):
        source = self.first if phase == 0 else self.sum
        copies = []
        for j, (idx, n, place, device) in enumerate(self.moves(phase)):
            dst = self.sum.at[span(k, idx, n), :] if place is None else self.landing.at[slot(k, place, n), :]
            copies.append(remote(source.at[span(k, idx, n), :], dst, self.sems.at[0, phase, k, j],
                                 self.sems.at[1, phase, k, j], device))
        return copies

    def start(self, phase, k):
        for j, copy in enumerate(self.copies(phase, k)):
            if phase >= 3:
                pl.semaphore_wait(self.credits.at[5 - phase, k, j], 1)
            copy.start()

    def finish(self, phase, k):
        for j, copy in enumerate(self.copies(phase, k)):
            copy.wait()
            if phase < 3:
                pl.semaphore_signal(self.credits.at[phase, k, j], inc=1, device_id={'sp': self.moves(phase)[j][3]},
                                    device_id_type=pl.DeviceIdType.MESH)
        _, y, x, _, _, _, _ = position()
        half, own0, own1 = self.owned()
        adds = ([(half, 8, 0)], [(own0, 2, 8), (own1, 2, 10)], [(own0 + y, 1, 12), (own1 + x, 1, 13)], (), (), ())
        for idx, n, place in adds[phase]:
            def body(i, carry):
                rows = pl.ds(pl.multiple_of((k * SLOTS + place + i) * BLOCK, 8), BLOCK)
                self.sum[span(k, idx + i, 1), :] += self.landing[rows, :]
                return carry
            lax.fori_loop(0, n, body, 0)

    def turn_down(self, k):
        for r in self.pieces(k):
            if r >= 8:
                rows = pl.ds(r * WIDTH, WIDTH)
                self.sum[rows, :] = self.sum[rows, :].T

    def pieces(self, k):
        return range(k * LAP_ROWS // WIDTH, (k + 1) * LAP_ROWS // WIDTH)

    def out_copy(self, r, outs):
        qkv_ref, out_ref, up_ref, down_ref = outs
        b = self.block
        if r < 3:
            dst = qkv_ref.at[b, :, pl.ds(r * WIDTH, WIDTH)]
        elif r == 3:
            dst = out_ref.at[b]
        elif r < 8:
            dst = up_ref.at[b, :, pl.ds((r - 4) * WIDTH, WIDTH)]
        else:
            dst = down_ref.at[b, pl.ds((r - 8) * WIDTH, WIDTH), :]
        return pltpu.make_async_copy(self.sum.at[pl.ds(r * WIDTH, WIDTH), :], dst, self.out_sems.at[r])


def reduce_plan():
    lasts = (1.4, 4.75, 2.4, 2.4, 4.75, 1.4)
    free, running, plan, now = [0.0, 0.0], {}, [], 0.0

    def start(lap, phase):
        link = 0 if phase in (0, 5) else 1
        free[link] = max(free[link], now) + lasts[phase]
        running[lap] = (phase, free[link] + 1.5)

    def turn(due):
        turns = []
        for lap in sorted(running, key=lambda lap: running[lap][1]):
            phase, end = running[lap]
            if end <= due:
                turns.append((lap, phase))
        for lap, phase in turns:
            del running[lap]
            if phase < 5:
                start(lap, phase + 1)
        return turns

    tail_laps = range(1, LAPS)
    begin = {0: [('t', k) for k in (*tail_laps, 0)], STEPS: [('s', k) for k in tail_laps]}
    for step in range(2 * STEPS):
        turns = turn(now)
        fresh = begin.get(step, [])
        for lap in fresh:
            start(lap, 0)
        plan.append((turns, fresh))
        now += 6.2 if step < STEPS else 4.2
    start(('s', 0), 0)
    turns, fresh = [], [('s', 0)]
    while running:
        plan.append((turns, fresh))
        fresh = []
        now = max(now, min(end for _, end in running.values()))
        turns = turn(now)
    plan.append((turns, fresh))
    return plan


def ln_copies(ln_ref, sems):
    me = lax.axis_index('sp')
    return [pltpu.make_async_remote_copy(
        src_ref=ln_ref.at[me], dst_ref=ln_ref.at[me], send_sem=sems.at[0, d], recv_sem=sems.at[1, d],
        device_id={'sp': lax.rem(me + d, N_DEV)}, device_id_type=pl.DeviceIdType.MESH) for d in range(1, N_DEV)]


def spatial_backward_kernel(*refs):
    (back_ref, x_ref, h_ref, o_ref, qkv_ref, p_ref,
     ln_ref, wqkv_ref, wout_ref, wup_ref, wdown_ref, perm_ref, gt_ref) = refs[:13]
    (dx_ref, gqkv_ref, gout_ref, gup_ref, gdown_ref, gln_ref,
     dv_ref, a_ref, m_ref, act_ref, dup_ref, do_ref, dqkv_ref, dp_ref, pre_ref, tanh_ref, dh_all_ref, do_all_ref,
     sum_ref, t_ref, land_s_ref, land_t_ref, ln_s_ref, ln_all_ref, sems_s, sems_t, credits_s, credits_t,
     sems_out_s, sems_out_t, sems_ln, sems_in) = refs[13:]
    step = pl.program_id(0)
    me = lax.axis_index('sp')
    load_t = pltpu.make_async_copy(gt_ref.at[pl.ds(0, SUM_ROWS), :], t_ref, sems_in.at[0])
    load_ln = pltpu.make_async_copy(gt_ref.at[pl.ds(SUM_ROWS, 8), :], ln_all_ref.at[me, pl.ds(0, 8), :], sems_in.at[1])
    sums = {'t': Reduce(t_ref, gt_ref, land_t_ref, sems_t, credits_t, 1, sems_out_t),
            's': Reduce(sum_ref, sum_ref, land_s_ref, sems_s, credits_s, 0, sems_out_s)}
    outs = (gqkv_ref, gout_ref, gup_ref, gdown_ref)
    plan = reduce_plan()
    ready, turned = [], []

    def advance(turns, fresh):
        for (which, k), phase in turns:
            sums[which].finish(phase, k)
        for which, k in fresh:
            sums[which].start(0, k)
        for (which, k), phase in turns:
            if phase < 5:
                sums[which].start(phase + 1, k)
        ready.extend(lap for lap, phase in turns if phase == 5)

    def write_totals():
        while turned:
            which, k = turned.pop()
            for r in sums[which].pieces(k):
                sums[which].out_copy(r, outs).start()
        if ready:
            which, k = ready.pop(0)
            sums[which].turn_down(k)
            turned.append((which, k))

    @pl.when(step == 0)
    def _():
        enter()
        load_t.start()
        load_ln.start()
        sum_ref[...] = jnp.zeros_like(sum_ref)
        ln_s_ref[...] = jnp.zeros_like(ln_s_ref)

    @pl.when(step == 1)
    def _():
        load_t.wait()
        load_ln.wait()

    for at in range(2 * STEPS):
        if any(plan[at]):
            @pl.when(step == at)
            def _(at=at):
                advance(*plan[at])

    gain1, shift1, gain2, shift2 = gains(ln_ref)

    @pl.when(step < STEPS)
    def _():
        mine = pl.ds(pl.multiple_of(step * STEP_ROWS, STEP_ROWS), STEP_ROWS)
        for v in range(NV):
            rows = pl.ds(v * ROWS, ROWS)
            dv_ref[rows, :] = dot_tn(perm_ref[...], back_ref[:, v].reshape(ROWS, WIDTH)).astype(BF16)
        normed, inv_std = up_forward(h_ref[...].astype(F32), gain2, shift2, m_ref, wup_ref, act_ref, pre_ref, tanh_ref)
        g_gain2, g_shift2 = tail_backward(dv_ref, o_ref, m_ref, normed, inv_std, gain2, pre_ref, tanh_ref, act_ref, dup_ref, do_ref,
                                          wout_ref, wup_ref, wdown_ref, sum_ref)
        dh_all_ref[mine, :] = dv_ref[...]
        do_all_ref[mine, :] = do_ref[...]
        add_ln_sums(ln_s_ref, 2, (g_gain2, g_shift2))

    @pl.when(step >= STEPS)
    def _():
        mine = pl.ds(pl.multiple_of((step - STEPS) * STEP_ROWS, STEP_ROWS), STEP_ROWS)
        dv_ref[...] = dh_all_ref[mine, :]
        do_ref[...] = do_all_ref[mine, :]
        normed1, _ = norm_stats(x_ref[...].astype(F32))
        a_ref[...] = (normed1 * gain1 + shift1).astype(BF16)
        attend_back(qkv_ref, p_ref, do_ref, dqkv_ref, dp_ref)
        d_in, g_gain1, g_shift1 = qkv_backward(x_ref[...].astype(F32), a_ref, dv_ref, dqkv_ref, gain1, wqkv_ref, sum_ref)
        add_ln_sums(ln_s_ref, 0, (g_gain1, g_shift1))
        dx_ref[...] = d_in

    @pl.when(step == 2 * STEPS - 1)
    def _():
        ln_all_ref[me, pl.ds(8, 8), :] = ln_s_ref[...]
        for n, (turns, fresh) in enumerate(plan[2 * STEPS:]):
            advance(turns, fresh)
            write_totals()
            if n == 0:
                for copy in ln_copies(ln_all_ref, sems_ln):
                    copy.start()
            if n == 3:
                for copy in ln_copies(ln_all_ref, sems_ln):
                    copy.wait()
                total = ln_all_ref[0]
                for d in range(1, N_DEV):
                    total += ln_all_ref[d]
                gln_ref[0] = total[8:12]
                gln_ref[1] = total[0:4]
        while ready or turned:
            write_totals()
        for which in 'ts':
            for r in range(12):
                sums[which].out_copy(r, outs).wait()


def finish_kernel(back_ref, perm_ref, *refs):
    n = len(refs) // 2
    ins, (y_ref, *outs) = refs[:n], refs[n:]
    for v in range(NV):
        y_ref[pl.ds(v * ROWS, ROWS), :] = dot_tn(perm_ref[...], back_ref[:, v].reshape(ROWS, WIDTH)).astype(BF16)
    for in_ref, out_ref in zip(ins, outs):
        out_ref[...] = in_ref[...]


def full(shape):
    return pl.BlockSpec(shape, lambda i: (0,) * len(shape), pipeline_mode=pl.Buffered(1))


def weight_specs(block):
    shapes = [(4, WIDTH), (WIDTH, QKV), (WIDTH, WIDTH), (WIDTH, HIDDEN), (HIDDEN, WIDTH)]
    return [pl.BlockSpec((None,) + s, lambda i: (block, 0, 0), pipeline_mode=pl.Buffered(1)) for s in shapes]


def rows_spec(width):
    return pl.BlockSpec((STEP_ROWS, width), lambda i: (i, 0))


ANY = pl.BlockSpec(memory_space=pl.ANY)


def params(collective_id):
    return pltpu.CompilerParams(dimension_semantics=("arbitrary",), vmem_limit_bytes=VMEM_LIMIT,
                                collective_id=collective_id, has_side_effects=True)


def cost(us, mib):
    return pl.CostEstimate(flops=int(us * 9e8), bytes_accessed=int(mib * 2 ** 20), transcendentals=0)


def sds(shape, dtype):
    return jax.ShapeDtypeStruct(shape, dtype)


def vm(width, dtype=BF16):
    return pltpu.VMEM((STEP_ROWS, width), dtype)


TOKENS = VIDEOS * ROWS
GRADS = [(2, WIDTH, QKV), (2, WIDTH, WIDTH), (2, WIDTH, HIDDEN), (2, HIDDEN, WIDTH)]
PROBS = 6 * GROUP
SWAP = (N_DEV, VIDEOS, 32, WIDTH)
ROW_QKV, ROW_OUT, ROW_UP, ROW_DOWN = 0, 3 * WIDTH, 4 * WIDTH, 8 * WIDTH
SUM_ROWS = 12 * WIDTH
LAPS = 4
LAP_ROWS = SUM_ROWS // LAPS
BLOCK = LAP_ROWS // 16
SLOTS = 14


def forward_call(x, dy, weights, bias_s, bias_t, perm):
    def early(width):
        return pl.BlockSpec((STEP_ROWS, width), lambda i: (jnp.minimum(i, STEPS - 1), 0))

    widths = (WIDTH, WIDTH, QKV, PROBS)
    stage = (N_DEV, NV, 32, WIDTH)
    return pl.pallas_call(
        forward_kernel, grid=(2 * STEPS,), name="forward",
        in_specs=[early(WIDTH)] * 2 + weight_specs(0) + weight_specs(1) + [full((GROUP, 2 * GROUP))] * 2 + [full((ROWS, ROWS))],
        out_specs=[ANY, full((SUM_ROWS + 8, WIDTH))] + [early(w) for w in widths],
        out_shape=[sds((N_DEV, 2) + SWAP[1:], BF16), sds((SUM_ROWS + 8, WIDTH), F32)] + [sds((TOKENS, w), BF16) for w in widths],
        scratch_shapes=[vm(w) for w in (WIDTH, WIDTH, WIDTH, QKV, PROBS, WIDTH, WIDTH, HIDDEN, HIDDEN, WIDTH, QKV, PROBS)]
        + [vm(HIDDEN, F32)] * 2 + [vm(PROBS, F32)] + [pltpu.VMEM(SWAP, BF16)] * 2
        + [pltpu.VMEM((6,) + stage, BF16)] * 2 + [pltpu.VMEM((4,) + stage, BF16)] * 2
        + exchange_sems(6) * 2 + exchange_sems(4) * 2,
        compiler_params=params(1), cost_estimate=cost(160, 60),
    )(x, dy, *weights, *weights, bias_s, bias_t, perm)


def spatial_backward_call(back, x, saved, weights, perm, sum_t):
    def early(width):
        return pl.BlockSpec((STEP_ROWS, width), lambda i: (jnp.minimum(i, STEPS - 1), 0))

    def late(width):
        return pl.BlockSpec((STEP_ROWS, width), lambda i: (jnp.maximum(i - STEPS, 0), 0))

    grads = GRADS
    return pl.pallas_call(
        spatial_backward_kernel, grid=(2 * STEPS,), name="spatial_bwd",
        in_specs=[pl.BlockSpec((N_DEV, None, NV, 32, WIDTH), lambda i: (0, 1, jnp.minimum(i, STEPS - 1), 0, 0))]
        + [late(WIDTH), early(WIDTH), early(WIDTH), late(QKV), late(PROBS)] + weight_specs(0) + [full((ROWS, ROWS)), ANY],
        out_specs=[late(WIDTH)] + [ANY] * 4 + [full((2, 4, WIDTH))],
        out_shape=[sds((TOKENS, WIDTH), BF16)] + [sds(g, F32) for g in grads] + [sds((2, 4, WIDTH), F32)],
        scratch_shapes=[vm(w) for w in (WIDTH, WIDTH, WIDTH, HIDDEN, HIDDEN, WIDTH, QKV, PROBS)] + [vm(HIDDEN, F32)] * 2
        + [pltpu.VMEM((TOKENS, WIDTH), BF16)] * 2
        + [pltpu.VMEM((SUM_ROWS, WIDTH), F32)] * 2 + [pltpu.VMEM((LAPS * SLOTS * BLOCK, WIDTH), F32)] * 2
        + [pltpu.VMEM((8, WIDTH), F32), pltpu.VMEM((N_DEV, 16, WIDTH), F32)]
        + [pltpu.SemaphoreType.DMA((2, 6, LAPS, 2))] * 2 + [pltpu.SemaphoreType.REGULAR((3, LAPS, 2))] * 2
        + [pltpu.SemaphoreType.DMA((12,))] * 2 + [pltpu.SemaphoreType.DMA((2, N_DEV)), pltpu.SemaphoreType.DMA((2,))],
        compiler_params=params(3), cost_estimate=cost(160, 60),
    )(back, x, *saved, *weights, perm, sum_t)


def finish_call(back, perm, dx, grads, g_ln):
    flat = [g.reshape(-1, g.shape[-1]) for g in grads]
    parts = [pl.BlockSpec((g.shape[0] // STEPS, g.shape[1]), lambda i: (i, 0)) for g in flat]
    ln_spec = pl.BlockSpec((2, 4, WIDTH), lambda i: (0, 0, 0))
    y, dx, *flat, g_ln = pl.pallas_call(
        finish_kernel, grid=(STEPS,), name="finish",
        in_specs=[pl.BlockSpec((N_DEV, None, NV, 32, WIDTH), lambda i: (0, 0, i, 0, 0)), full((ROWS, ROWS)), rows_spec(WIDTH)]
        + parts + [ln_spec],
        out_specs=[rows_spec(WIDTH)] * 2 + parts + [ln_spec],
        out_shape=[sds((TOKENS, WIDTH), BF16)] * 2 + [sds(g.shape, F32) for g in flat] + [sds((2, 4, WIDTH), F32)],
        compiler_params=pltpu.CompilerParams(dimension_semantics=("arbitrary",), vmem_limit_bytes=VMEM_LIMIT),
        cost_estimate=cost(12, 40),
    )(back, perm, dx, *flat, g_ln)
    return y, dx, [f.reshape(g.shape) for f, g in zip(flat, grads)], g_ln


def constants():
    row = np.arange(ROWS)
    dev, patch, frame = row // 32, (row // 8) % 4, row % 8
    perm = np.zeros((ROWS, ROWS), np.float32)
    perm[row, frame * 32 + dev * 4 + patch] = 1.0
    r = np.arange(GROUP)
    frame_of = r // 32
    patch_of = (r // 8) % 2
    bias_s = np.where(frame_of[:, None] == frame_of[None], 0.0, -np.inf).astype(np.float32)
    bias_t = np.where(patch_of[:, None] == patch_of[None], 0.0, -np.inf).astype(np.float32)
    return perm, np.concatenate([bias_s] * 2, 1), np.concatenate([bias_t] * 2, 1)


def device_step(latents, cotangent, ln_params, w_qkv, w_out, w_up, w_down):
    perm, bias_s, bias_t = constants()
    perm = jnp.asarray(perm, BF16)
    bias_s, bias_t = jnp.asarray(bias_s), jnp.asarray(bias_t)
    weights = (ln_params, w_qkv, w_out.reshape(2, WIDTH, WIDTH), w_up, w_down)
    x = latents.reshape(TOKENS, WIDTH)
    dy = cotangent.reshape(TOKENS, WIDTH)

    back, sum_t, *saved = forward_call(x, dy, weights, bias_s, bias_t, perm)
    dx, *grads, g_ln = spatial_backward_call(back, x, saved, weights, perm, sum_t)
    y, dx, (g_qkv, g_out, g_up, g_down), g_ln = finish_call(back, perm, dx, grads, g_ln)
    g_out = g_out.reshape(2, 6, 64, WIDTH)
    shape = latents.shape
    return y.reshape(shape), dx.reshape(shape), g_ln, g_qkv, g_out, g_up, g_down


def solution(mesh):
    act_spec = P('data', 'sp', None, None)
    replicated = P()
    part_spec = P('data')
    return jax.shard_map(device_step, mesh=mesh,
                         in_specs=(act_spec, act_spec, replicated, replicated, replicated, replicated, replicated),
                         out_specs=(act_spec, act_spec, part_spec, part_spec, part_spec, part_spec, part_spec),
                         check_vma=False)
```

```python
import itertools

import jax
import jax.numpy as jnp
import numpy as np
from jax import lax
from jax.experimental import pallas as pl
from jax.experimental.pallas import tpu as pltpu
from jax.sharding import PartitionSpec as P

BF16 = jnp.bfloat16
F32 = jnp.float32
N_DEV = 8
WIDTH = 384
HIDDEN = 4 * WIDTH
QKV = 3 * WIDTH
VIDEOS = 16
ROWS = 256
NV = 2
STEP_ROWS = ROWS * NV
GROUP = 128
PAIRS = 3
SCALE = 0.125
LOG2E = 1.4426950408889634
STEPS = VIDEOS // NV
GELU_C = 0.7978845608028654
GELU_C3 = GELU_C * 0.044715
VMEM_LIMIT = 62 * 1024 * 1024


def dot_nn(a, b):
    return lax.dot_general(a, b, (((1,), (0,)), ((), ())), preferred_element_type=F32)


def dot_nt(a, b):
    return lax.dot_general(a, b, (((1,), (1,)), ((), ())), preferred_element_type=F32)


def dot_tn(a, b):
    return lax.dot_general(a, b, (((0,), (0,)), ((), ())), preferred_element_type=F32)


def norm_stats(x32):
    centered = x32 - jnp.mean(x32, axis=-1, keepdims=True)
    inv_std = lax.rsqrt(jnp.mean(centered * centered, axis=-1, keepdims=True) + 1e-6)
    return centered * inv_std, inv_std


def norm_back(d_out32, normed, inv_std, gain):
    d_gain = jnp.sum(d_out32 * normed, axis=0, keepdims=True)
    d_shift = jnp.sum(d_out32, axis=0, keepdims=True)
    d_norm = d_out32 * gain
    d_center = d_norm - jnp.mean(d_norm, axis=-1, keepdims=True)
    d_in = inv_std * (d_center - normed * jnp.mean(d_norm * normed, axis=-1, keepdims=True))
    return d_in, d_gain, d_shift


def gelu_slope(x, t):
    half = 0.5 + 0.5 * t
    return half + ((x * half) * (1.0 - t)) * (GELU_C + (3.0 * GELU_C3) * (x * x))


def gelu_value(x):
    t = jnp.tanh(x * (GELU_C + GELU_C3 * (x * x)))
    return x * (0.5 + 0.5 * t)


def lane_masks():
    lane = lax.broadcasted_iota(jnp.int32, (1, GROUP), 1)
    low = (lane < GROUP // 2)
    m_low = jnp.where(low, 1.0, 0.0).astype(BF16)
    m_high = jnp.where(low, 0.0, 1.0).astype(BF16)
    return low, m_low, m_high


def split_heads(k, m_low, m_high):
    return jnp.concatenate([k * m_low, k * m_high], axis=0)


GROUPS = STEP_ROWS // GROUP
BLOCKS = [(g, pair) for g in range(GROUPS) for pair in range(PAIRS)]


def rows_of(g):
    return pl.ds(g * GROUP, GROUP)


def part(kind, pair):
    return pl.ds(kind * WIDTH + pair * GROUP, GROUP)


def both(pair):
    return pl.ds(pair * 2 * GROUP, 2 * GROUP)


def attend(qkv_ref, bias_ref, p_ref, o_ref, s_ref):
    low, m_low, m_high = lane_masks()
    for g, pair in BLOCKS:
        k2 = split_heads(qkv_ref[rows_of(g), part(1, pair)], m_low, m_high)
        s_ref[rows_of(g), both(pair)] = dot_nt(qkv_ref[rows_of(g), part(0, pair)], k2) * (SCALE * LOG2E) + bias_ref[...]
    for g, pair in BLOCKS:
        s = s_ref[rows_of(g), both(pair)]
        probs = []
        for h in range(2):
            s_h = s[:, h * GROUP:(h + 1) * GROUP]
            e_h = jnp.exp2(s_h - jnp.max(s_h, axis=-1, keepdims=True))
            probs.append(e_h * (1.0 / jnp.sum(e_h, axis=-1, keepdims=True)))
        p_ref[rows_of(g), both(pair)] = jnp.concatenate(probs, axis=1).astype(BF16)
    for g, pair in BLOCKS:
        v2 = split_heads(qkv_ref[rows_of(g), part(2, pair)], m_low, m_high)
        o_ref[rows_of(g), part(0, pair)] = dot_nn(p_ref[rows_of(g), both(pair)], v2).astype(BF16)


def attend_back(qkv_ref, p_ref, do_ref, dqkv_ref, dp_ref):
    low, m_low, m_high = lane_masks()
    for g, pair in BLOCKS:
        do = do_ref[rows_of(g), part(0, pair)]
        v2 = split_heads(qkv_ref[rows_of(g), part(2, pair)], m_low, m_high)
        dp_ref[rows_of(g), both(pair)] = dot_nt(do, v2).astype(BF16)
        dv = dot_tn(p_ref[rows_of(g), both(pair)], do)
        dqkv_ref[rows_of(g), part(2, pair)] = jnp.where(low, dv[:GROUP], dv[GROUP:]).astype(BF16)
    for g, pair in BLOCKS:
        p32 = p_ref[rows_of(g), both(pair)].astype(F32)
        t = dp_ref[rows_of(g), both(pair)].astype(F32) * p32
        ds = []
        for h in range(2):
            half = slice(h * GROUP, (h + 1) * GROUP)
            ds.append(t[:, half] - p32[:, half] * jnp.sum(t[:, half], axis=-1, keepdims=True))
        dp_ref[rows_of(g), both(pair)] = jnp.concatenate(ds, axis=1).astype(BF16)
    for g, pair in BLOCKS:
        ds = dp_ref[rows_of(g), both(pair)]
        k2 = split_heads(qkv_ref[rows_of(g), part(1, pair)], m_low, m_high)
        dqkv_ref[rows_of(g), part(0, pair)] = (dot_nn(ds, k2) * SCALE).astype(BF16)
        dk = dot_tn(ds, qkv_ref[rows_of(g), part(0, pair)])
        dqkv_ref[rows_of(g), part(1, pair)] = (jnp.where(low, dk[:GROUP], dk[GROUP:]) * SCALE).astype(BF16)


CHUNK = 512
CHUNKS = HIDDEN // CHUNK


def cut(c):
    return pl.ds(c * CHUNK, CHUNK)


def gains(ln_ref):
    ln = ln_ref[...].astype(F32)
    return [ln[r:r + 1, :] for r in range(4)]


def position():
    me = lax.axis_index('sp')
    y, x, c = me // 4, (me // 2) % 2, me % 2
    return me, y, x, c, me + 1 - 2 * c, me + 2 - 4 * x, me + 4 - 8 * y


def flip(bit, by):
    return bit + by - 2 * bit * by


def peer(d):
    _, y, x, c, _, _, _ = position()
    return 4 * flip(y, d // 4) + 2 * flip(x, (d // 2) % 2) + flip(c, d % 2)


ORDER = (*range(2, N_DEV), 1)


def enter():
    barrier = pltpu.get_barrier_semaphore()
    for d in range(1, N_DEV):
        pl.semaphore_signal(barrier, inc=1, device_id={'sp': peer(d)}, device_id_type=pl.DeviceIdType.MESH)
    pl.semaphore_wait(barrier, N_DEV - 1)


def remote(src, dst, send_sem, recv_sem, device):
    return pltpu.make_async_remote_copy(src_ref=src, dst_ref=dst, send_sem=send_sem, recv_sem=recv_sem,
                                        device_id={'sp': device}, device_id_type=pl.DeviceIdType.MESH)


def videos_of(i):
    return pl.ds(i * NV, NV)


class Exchange:
    def __init__(self, stage, landing, sems, local=True):
        self.stage, self.landing, (self.send, self.recv, self.own) = stage, landing, sems
        self.slots, self.has_local = stage.shape[0], local

    def copies(self, i):
        me, slot = lax.axis_index('sp'), lax.rem(i, self.slots)
        return [remote(self.stage.at[slot, peer(d)], self.landing(me, i), self.send.at[slot, d], self.recv.at[i, d], peer(d))
                for d in ORDER]

    def local(self, i):
        me, slot = lax.axis_index('sp'), lax.rem(i, self.slots)
        return pltpu.make_async_copy(self.stage.at[slot, me], self.landing(me, i), self.own.at[slot])

    def start(self, i):
        for copy in self.copies(i):
            copy.start()
        if self.has_local:
            self.local(i).start()

    def wait_sent(self, i):
        for copy in self.copies(i):
            copy.wait_send()
        if self.has_local:
            self.local(i).wait()

    def wait_received(self, i):
        for d in range(1, N_DEV):
            remote(self.stage.at[0, 0], self.landing(peer(d), i), self.send.at[0, d], self.recv.at[i, d],
                   peer(d)).wait_recv()

    def free_slot(self, i):
        @pl.when(i >= self.slots)
        def _():
            self.wait_sent(i - self.slots)

    def finish_sends(self, n):
        for j in range(self.slots):
            self.wait_sent(jnp.int32(n - self.slots + j))

    def finish(self, n):
        self.finish_sends(n)

        def body(i, carry):
            self.wait_received(i)
            return carry
        lax.fori_loop(0, n, body, 0)


def exchange_sems(slots):
    return [pltpu.SemaphoreType.DMA((slots, N_DEV)), pltpu.SemaphoreType.DMA((STEPS, N_DEV)),
            pltpu.SemaphoreType.DMA((slots,))]


def spatial_forward_step(i, x_ref, dy_ref, ln_ref, wqkv_ref, wout_ref, wup_ref, wdown_ref, bias_ref, perm_ref,
                         h_ref, o_ref, qkv_ref, p_ref, act_ref, s_ref, send_mid, send_dy, mid_ref, dyx_ref):
    me = lax.axis_index('sp')
    slot = lax.rem(i, send_mid.slots)
    send_mid.free_slot(i)
    send_dy.free_slot(i)
    for v in range(NV):
        moved = dot_nn(perm_ref[...], dy_ref[pl.ds(v * ROWS, ROWS), :]).astype(BF16)
        for d in range(N_DEV):
            send_dy.stage[slot, d, v] = moved[d * 32:(d + 1) * 32]
    gain1, shift1, gain2, shift2 = gains(ln_ref)
    normed, _ = norm_stats(x_ref[...].astype(F32))
    a_in = (normed * gain1 + shift1).astype(BF16)
    for c in range(3):
        cols = pl.ds(c * WIDTH, WIDTH)
        qkv_ref[:, cols] = dot_nn(a_in, wqkv_ref[:, cols]).astype(BF16)
    attend(qkv_ref, bias_ref, p_ref, o_ref, s_ref)
    h_ref[...] = (x_ref[...].astype(F32) + dot_nn(o_ref[...], wout_ref[...])).astype(BF16)
    normed, _ = norm_stats(h_ref[...].astype(F32))
    m_in = (normed * gain2 + shift2).astype(BF16)
    for c in range(CHUNKS):
        act_ref[:, cut(c)] = gelu_value(dot_nn(m_in, wup_ref[:, cut(c)])).astype(BF16)
    out = (h_ref[...].astype(F32) + dot_nn(act_ref[...], wdown_ref[...])).astype(BF16)
    for v in range(NV):
        moved = dot_nn(perm_ref[...], out[v * ROWS:(v + 1) * ROWS]).astype(BF16)
        for d in range(N_DEV):
            send_mid.stage[slot, d, v] = moved[d * 32:(d + 1) * 32]
    for v in range(NV):
        dyx_ref[me, i * NV + v] = send_dy.stage[slot, me, v]
        mid_ref[me, i * NV + v] = send_mid.stage[slot, me, v]
    send_mid.start(i)
    send_dy.start(i)


def add_blocks(sum_ref, first, product):
    for c in range(product.shape[1] // WIDTH):
        rows = pl.ds(first + c * WIDTH, WIDTH)
        sum_ref[rows, :] += product[:, c * WIDTH:(c + 1) * WIDTH]


def tail_backward(dv_ref, o_ref, m_ref, normed, inv_std, gain2, pre_ref, tanh_ref, act_ref, dup_ref, do_ref,
                  wout_ref, wup_ref, wdown_ref, sum_ref):
    add_blocks(sum_ref, ROW_DOWN, dot_tn(dv_ref[...], act_ref[...]))
    for c in range(CHUNKS):
        d_act = dot_nt(dv_ref[...], wdown_ref[cut(c), :]).astype(BF16).astype(F32)
        dup_ref[:, cut(c)] = (d_act * gelu_slope(pre_ref[:, cut(c)], tanh_ref[:, cut(c)])).astype(BF16)
    add_blocks(sum_ref, ROW_UP, dot_tn(m_ref[...], dup_ref[...]))
    d_m = dot_nt(dup_ref[...], wup_ref[...]).astype(BF16).astype(F32)
    d_h, g_gain, g_shift = norm_back(d_m, normed, inv_std, gain2)
    dv_ref[...] = (d_h + dv_ref[...].astype(F32)).astype(BF16)
    add_blocks(sum_ref, ROW_OUT, dot_tn(o_ref[...], dv_ref[...]))
    do_ref[...] = dot_nt(dv_ref[...], wout_ref[...]).astype(BF16)
    return g_gain, g_shift


def qkv_backward(u32, a_ref, dh_ref, dqkv_ref, gain1, wqkv_ref, sum_ref):
    normed, inv_std = norm_stats(u32)
    add_blocks(sum_ref, ROW_QKV, dot_tn(a_ref[...], dqkv_ref[...]))
    d_a = dot_nt(dqkv_ref[...], wqkv_ref[...]).astype(BF16).astype(F32)
    d_in, g_gain, g_shift = norm_back(d_a, normed, inv_std, gain1)
    return (d_in + dh_ref[...].astype(F32)).astype(BF16), g_gain, g_shift


def up_forward(h32, gain2, shift2, m_ref, wup_ref, act_ref, pre_ref, tanh_ref):
    normed, inv_std = norm_stats(h32)
    m_ref[...] = (normed * gain2 + shift2).astype(BF16)
    for c in range(CHUNKS):
        x = dot_nn(m_ref[...], wup_ref[:, cut(c)])
        t = jnp.tanh(x * (GELU_C + GELU_C3 * (x * x)))
        act_ref[:, cut(c)] = (x * (0.5 + 0.5 * t)).astype(BF16)
        pre_ref[:, cut(c)] = x
        tanh_ref[:, cut(c)] = t
    return normed, inv_std


def add_ln_sums(ref, first, sums):
    for r, g in enumerate(sums):
        ref[first + r:first + r + 1, :] += g


def temporal_step(i, ln_ref, wqkv_ref, wout_ref, wup_ref, wdown_ref, bias_ref, sum_ref, mid_ref, dyx_ref,
                  send_mid, send_dy, send_y, send_dm, u_ref, dv_ref, a_ref, qkv_ref, p_ref, o_ref, m_ref, act_ref,
                  dup_ref, do_ref, dqkv_ref, dp_ref, pre_ref, tanh_ref, s_ref):
    send_mid.wait_received(i)
    send_dy.wait_received(i)
    send_y.free_slot(i)
    send_dm.free_slot(i)
    gain1, shift1, gain2, shift2 = gains(ln_ref)
    places = [(v, g, s) for v in range(NV) for g in range(2) for s in range(N_DEV)]
    for v, g, s in places:
        dst = pl.ds(v * ROWS + g * GROUP + s * 16, 16)
        u_ref[dst, :] = mid_ref[s, i * NV + v, pl.ds(g * 16, 16), :]
        dv_ref[dst, :] = dyx_ref[s, i * NV + v, pl.ds(g * 16, 16), :]
    normed1, _ = norm_stats(u_ref[...].astype(F32))
    a_ref[...] = (normed1 * gain1 + shift1).astype(BF16)
    for c in range(3):
        cols = pl.ds(c * WIDTH, WIDTH)
        qkv_ref[:, cols] = dot_nn(a_ref[...], wqkv_ref[:, cols]).astype(BF16)
    attend(qkv_ref, bias_ref, p_ref, o_ref, s_ref)
    h = (u_ref[...].astype(F32) + dot_nn(o_ref[...], wout_ref[...])).astype(BF16)
    h32 = h.astype(F32)
    normed, inv_std = up_forward(h32, gain2, shift2, m_ref, wup_ref, act_ref, pre_ref, tanh_ref)
    out = (h32 + dot_nn(act_ref[...], wdown_ref[...])).astype(BF16)
    for v, g, s in places:
        src = v * ROWS + g * GROUP + s * 16
        send_y.stage[lax.rem(i, send_y.slots), s, v, pl.ds(g * 16, 16), :] = out[src:src + 16]
    send_y.start(i)
    g_gain2, g_shift2 = tail_backward(dv_ref, o_ref, m_ref, normed, inv_std, gain2, pre_ref, tanh_ref, act_ref, dup_ref, do_ref,
                                      wout_ref, wup_ref, wdown_ref, sum_ref)
    attend_back(qkv_ref, p_ref, do_ref, dqkv_ref, dp_ref)
    d_in, g_gain1, g_shift1 = qkv_backward(u_ref[...].astype(F32), a_ref, dv_ref, dqkv_ref, gain1, wqkv_ref, sum_ref)
    add_ln_sums(sum_ref, SUM_ROWS, (g_gain1, g_shift1, g_gain2, g_shift2))
    for v, g, s in places:
        src = v * ROWS + g * GROUP + s * 16
        send_dm.stage[lax.rem(i, send_dm.slots), s, v, pl.ds(g * 16, 16), :] = d_in[src:src + 16]
    send_dm.start(i)


def forward_kernel(x_ref, dy_ref, *refs):
    refs = iter(refs)

    def take(n):
        return list(itertools.islice(refs, n))

    spatial_w, temporal_w, (bias_s_ref, bias_t_ref, perm_ref) = take(5), take(5), take(3)
    back_ref, sum_ref, h_ref, o_ref, qkv_ref, p_ref = take(6)
    mine, (pre_ref, tanh_ref, s_ref), (mid_ref, dyx_ref) = take(12), take(3), take(2)
    mid_stage, dy_stage, y_stage, dm_stage = take(4)
    mid_sems, dy_sems, y_sems, dm_sems = [take(3) for _ in BLOCKS[:4]]
    step = pl.program_id(0)
    send_mid = Exchange(mid_stage, lambda src, i: mid_ref.at[src, videos_of(i)], mid_sems, local=False)
    send_dy = Exchange(dy_stage, lambda src, i: dyx_ref.at[src, videos_of(i)], dy_sems, local=False)
    send_y = Exchange(y_stage, lambda src, i: back_ref.at[src, 0, videos_of(i)], y_sems)
    send_dm = Exchange(dm_stage, lambda src, i: back_ref.at[src, 1, videos_of(i)], dm_sems)

    @pl.when(step == 0)
    def _():
        enter()
        sum_ref[...] = jnp.zeros_like(sum_ref)

    @pl.when(step < STEPS)
    def _():
        spatial_forward_step(step, x_ref, dy_ref, *spatial_w, bias_s_ref, perm_ref, h_ref, o_ref, qkv_ref, p_ref,
                             mine[7], s_ref, send_mid, send_dy, mid_ref, dyx_ref)

    @pl.when(step >= STEPS)
    def _():
        temporal_step(step - STEPS, *temporal_w, bias_t_ref, sum_ref, mid_ref, dyx_ref,
                      send_mid, send_dy, send_y, send_dm, *mine, pre_ref, tanh_ref, s_ref)

    @pl.when(step == 2 * STEPS - 1)
    def _():
        send_mid.finish_sends(STEPS)
        send_dy.finish_sends(STEPS)
        send_y.finish(STEPS)
        send_dm.finish(STEPS)


def span(k, idx, n):
    return pl.ds(pl.multiple_of(k * LAP_ROWS + idx * BLOCK, 8), n * BLOCK)


def slot(k, idx, n):
    return pl.ds((k * SLOTS + idx) * BLOCK, n * BLOCK)


class Reduce:
    def __init__(self, sum_ref, first_ref, landing_ref, sems, credits, block, out_sems):
        self.sum, self.first, self.landing = sum_ref, first_ref, landing_ref
        self.sems, self.credits, self.block, self.out_sems = sems, credits, block, out_sems

    def owned(self):
        _, y, x, c, _, _, _ = position()
        half = c * 8
        return half, half + x * 2, half + 4 + y * 2

    def moves(self, phase):
        _, y, x, c, partner, xn, yn = position()
        half, own0, own1 = self.owned()
        return (
            [(8 - half, 8, 0, partner)],
            [(own0 + 2 - x * 4, 2, 8, xn), (own1 + 2 - y * 4, 2, 10, yn)],
            [(own0 + 1 - y, 1, 12, yn), (own1 + 1 - x, 1, 13, xn)],
            [(own0 + y, 1, None, yn), (own1 + x, 1, None, xn)],
            [(own0, 2, None, xn), (own1, 2, None, yn)],
            [(half, 8, None, partner)],
        )[phase]

    def copies(self, phase, k):
        source = self.first if phase == 0 else self.sum
        copies = []
        for j, (idx, n, place, device) in enumerate(self.moves(phase)):
            dst = self.sum.at[span(k, idx, n), :] if place is None else self.landing.at[slot(k, place, n), :]
            copies.append(remote(source.at[span(k, idx, n), :], dst, self.sems.at[0, phase, k, j],
                                 self.sems.at[1, phase, k, j], device))
        return copies

    def start(self, phase, k):
        for j, copy in enumerate(self.copies(phase, k)):
            if phase >= 3:
                pl.semaphore_wait(self.credits.at[5 - phase, k, j], 1)
            copy.start()

    def finish(self, phase, k):
        for j, copy in enumerate(self.copies(phase, k)):
            copy.wait()
            if phase < 3:
                pl.semaphore_signal(self.credits.at[phase, k, j], inc=1, device_id={'sp': self.moves(phase)[j][3]},
                                    device_id_type=pl.DeviceIdType.MESH)
        _, y, x, _, _, _, _ = position()
        half, own0, own1 = self.owned()
        adds = ([(half, 8, 0)], [(own0, 2, 8), (own1, 2, 10)], [(own0 + y, 1, 12), (own1 + x, 1, 13)], (), (), ())
        for idx, n, place in adds[phase]:
            def body(i, carry):
                rows = pl.ds(pl.multiple_of((k * SLOTS + place + i) * BLOCK, 8), BLOCK)
                self.sum[span(k, idx + i, 1), :] += self.landing[rows, :]
                return carry
            lax.fori_loop(0, n, body, 0)

    def turn_down(self, k):
        for r in self.pieces(k):
            if r >= 8:
                rows = pl.ds(r * WIDTH, WIDTH)
                self.sum[rows, :] = self.sum[rows, :].T

    def pieces(self, k):
        return range(k * LAP_ROWS // WIDTH, (k + 1) * LAP_ROWS // WIDTH)

    def out_copy(self, r, outs):
        qkv_ref, out_ref, up_ref, down_ref = outs
        b = self.block
        if r < 3:
            dst = qkv_ref.at[b, :, pl.ds(r * WIDTH, WIDTH)]
        elif r == 3:
            dst = out_ref.at[b]
        elif r < 8:
            dst = up_ref.at[b, :, pl.ds((r - 4) * WIDTH, WIDTH)]
        else:
            dst = down_ref.at[b, pl.ds((r - 8) * WIDTH, WIDTH), :]
        return pltpu.make_async_copy(self.sum.at[pl.ds(r * WIDTH, WIDTH), :], dst, self.out_sems.at[r])


def reduce_plan():
    lasts = (1.4, 4.75, 2.4, 2.4, 4.75, 1.4)
    free, running, plan, now = [0.0, 0.0], {}, [], 0.0

    def start(lap, phase):
        link = 0 if phase in (0, 5) else 1
        free[link] = max(free[link], now) + lasts[phase]
        running[lap] = (phase, free[link] + 1.0)

    def turn(due):
        turns = []
        for lap in sorted(running, key=lambda lap: running[lap][1]):
            phase, end = running[lap]
            if end <= due:
                turns.append((lap, phase))
        for lap, phase in turns:
            del running[lap]
            if phase < 5:
                start(lap, phase + 1)
        return turns

    tail_laps = range(1, LAPS)
    begin = {0: [('t', k) for k in (*tail_laps, 0)], STEPS: [('s', k) for k in tail_laps]}
    for step in range(2 * STEPS):
        turns = turn(now)
        fresh = begin.get(step, [])
        for lap in fresh:
            start(lap, 0)
        plan.append((turns, fresh))
        now += 6.2 if step < STEPS else 4.2
    start(('s', 0), 0)
    turns, fresh = [], [('s', 0)]
    while running:
        plan.append((turns, fresh))
        fresh = []
        now = max(now, min(end for _, end in running.values()))
        turns = turn(now)
    plan.append((turns, fresh))
    return plan


def ln_copies(ln_ref, sems):
    me = lax.axis_index('sp')
    return [pltpu.make_async_remote_copy(
        src_ref=ln_ref.at[me], dst_ref=ln_ref.at[me], send_sem=sems.at[0, d], recv_sem=sems.at[1, d],
        device_id={'sp': lax.rem(me + d, N_DEV)}, device_id_type=pl.DeviceIdType.MESH) for d in range(1, N_DEV)]


def spatial_backward_kernel(*refs):
    (back_ref, x_ref, h_ref, o_ref, qkv_ref, p_ref,
     ln_ref, wqkv_ref, wout_ref, wup_ref, wdown_ref, perm_ref, gt_ref) = refs[:13]
    (dx_ref, gqkv_ref, gout_ref, gup_ref, gdown_ref, gln_ref,
     dv_ref, a_ref, m_ref, act_ref, dup_ref, do_ref, dqkv_ref, dp_ref, pre_ref, tanh_ref, dh_all_ref, do_all_ref,
     sum_ref, t_ref, land_s_ref, land_t_ref, ln_s_ref, ln_all_ref, sems_s, sems_t, credits_s, credits_t,
     sems_out_s, sems_out_t, sems_ln, sems_in) = refs[13:]
    step = pl.program_id(0)
    me = lax.axis_index('sp')
    load_t = pltpu.make_async_copy(gt_ref.at[pl.ds(0, SUM_ROWS), :], t_ref, sems_in.at[0])
    load_ln = pltpu.make_async_copy(gt_ref.at[pl.ds(SUM_ROWS, 8), :], ln_all_ref.at[me, pl.ds(0, 8), :], sems_in.at[1])
    sums = {'t': Reduce(t_ref, gt_ref, land_t_ref, sems_t, credits_t, 1, sems_out_t),
            's': Reduce(sum_ref, sum_ref, land_s_ref, sems_s, credits_s, 0, sems_out_s)}
    outs = (gqkv_ref, gout_ref, gup_ref, gdown_ref)
    plan = reduce_plan()
    ready, turned = [], []

    def advance(turns, fresh):
        for (which, k), phase in turns:
            sums[which].finish(phase, k)
        for which, k in fresh:
            sums[which].start(0, k)
        for (which, k), phase in turns:
            if phase < 5:
                sums[which].start(phase + 1, k)
        ready.extend(lap for lap, phase in turns if phase == 5)

    def write_totals():
        while turned:
            which, k = turned.pop()
            for r in sums[which].pieces(k):
                sums[which].out_copy(r, outs).start()
        if ready:
            which, k = ready.pop(0)
            sums[which].turn_down(k)
            turned.append((which, k))

    @pl.when(step == 0)
    def _():
        enter()
        load_t.start()
        load_ln.start()
        sum_ref[...] = jnp.zeros_like(sum_ref)
        ln_s_ref[...] = jnp.zeros_like(ln_s_ref)

    @pl.when(step == 1)
    def _():
        load_t.wait()
        load_ln.wait()

    for at in range(2 * STEPS):
        if any(plan[at]):
            @pl.when(step == at)
            def _(at=at):
                advance(*plan[at])

    gain1, shift1, gain2, shift2 = gains(ln_ref)

    @pl.when(step < STEPS)
    def _():
        mine = pl.ds(pl.multiple_of(step * STEP_ROWS, STEP_ROWS), STEP_ROWS)
        for v in range(NV):
            rows = pl.ds(v * ROWS, ROWS)
            dv_ref[rows, :] = dot_tn(perm_ref[...], back_ref[:, v].reshape(ROWS, WIDTH)).astype(BF16)
        normed, inv_std = up_forward(h_ref[...].astype(F32), gain2, shift2, m_ref, wup_ref, act_ref, pre_ref, tanh_ref)
        g_gain2, g_shift2 = tail_backward(dv_ref, o_ref, m_ref, normed, inv_std, gain2, pre_ref, tanh_ref, act_ref, dup_ref, do_ref,
                                          wout_ref, wup_ref, wdown_ref, sum_ref)
        dh_all_ref[mine, :] = dv_ref[...]
        do_all_ref[mine, :] = do_ref[...]
        add_ln_sums(ln_s_ref, 2, (g_gain2, g_shift2))

    @pl.when(step >= STEPS)
    def _():
        mine = pl.ds(pl.multiple_of((step - STEPS) * STEP_ROWS, STEP_ROWS), STEP_ROWS)
        dv_ref[...] = dh_all_ref[mine, :]
        do_ref[...] = do_all_ref[mine, :]
        normed1, _ = norm_stats(x_ref[...].astype(F32))
        a_ref[...] = (normed1 * gain1 + shift1).astype(BF16)
        attend_back(qkv_ref, p_ref, do_ref, dqkv_ref, dp_ref)
        d_in, g_gain1, g_shift1 = qkv_backward(x_ref[...].astype(F32), a_ref, dv_ref, dqkv_ref, gain1, wqkv_ref, sum_ref)
        add_ln_sums(ln_s_ref, 0, (g_gain1, g_shift1))
        dx_ref[...] = d_in

    @pl.when(step == 2 * STEPS - 1)
    def _():
        ln_all_ref[me, pl.ds(8, 8), :] = ln_s_ref[...]
        for n, (turns, fresh) in enumerate(plan[2 * STEPS:]):
            advance(turns, fresh)
            write_totals()
            if n == 0:
                for copy in ln_copies(ln_all_ref, sems_ln):
                    copy.start()
            if n == 3:
                for copy in ln_copies(ln_all_ref, sems_ln):
                    copy.wait()
                total = ln_all_ref[0]
                for d in range(1, N_DEV):
                    total += ln_all_ref[d]
                gln_ref[0] = total[8:12]
                gln_ref[1] = total[0:4]
        while ready or turned:
            write_totals()
        for which in 'ts':
            for r in range(12):
                sums[which].out_copy(r, outs).wait()


def finish_kernel(back_ref, perm_ref, *refs):
    n = len(refs) // 2
    ins, (y_ref, *outs) = refs[:n], refs[n:]
    y_ref[...] = dot_tn(perm_ref[...], back_ref[...].reshape(ROWS, WIDTH)).astype(BF16)
    for in_ref, out_ref in zip(ins, outs):
        out_ref[...] = in_ref[...]


def full(shape):
    return pl.BlockSpec(shape, lambda i: (0,) * len(shape), pipeline_mode=pl.Buffered(1))


def weight_specs(block):
    shapes = [(4, WIDTH), (WIDTH, QKV), (WIDTH, WIDTH), (WIDTH, HIDDEN), (HIDDEN, WIDTH)]
    return [pl.BlockSpec((None,) + s, lambda i: (block, 0, 0), pipeline_mode=pl.Buffered(1)) for s in shapes]


def rows_spec(width):
    return pl.BlockSpec((STEP_ROWS, width), lambda i: (i, 0))


ANY = pl.BlockSpec(memory_space=pl.ANY)


def params(collective_id):
    return pltpu.CompilerParams(dimension_semantics=("arbitrary",), vmem_limit_bytes=VMEM_LIMIT,
                                collective_id=collective_id, has_side_effects=True)


def cost(us, mib):
    return pl.CostEstimate(flops=int(us * 9e8), bytes_accessed=int(mib * 2 ** 20), transcendentals=0)


def sds(shape, dtype):
    return jax.ShapeDtypeStruct(shape, dtype)


def vm(width, dtype=BF16):
    return pltpu.VMEM((STEP_ROWS, width), dtype)


TOKENS = VIDEOS * ROWS
GRADS = [(2, WIDTH, QKV), (2, WIDTH, WIDTH), (2, WIDTH, HIDDEN), (2, HIDDEN, WIDTH)]
PROBS = 6 * GROUP
SWAP = (N_DEV, VIDEOS, 32, WIDTH)
ROW_QKV, ROW_OUT, ROW_UP, ROW_DOWN = 0, 3 * WIDTH, 4 * WIDTH, 8 * WIDTH
SUM_ROWS = 12 * WIDTH
LAPS = 4
LAP_ROWS = SUM_ROWS // LAPS
BLOCK = LAP_ROWS // 16
SLOTS = 14


def forward_call(x, dy, weights, bias_s, bias_t, perm):
    def early(width):
        return pl.BlockSpec((STEP_ROWS, width), lambda i: (jnp.minimum(i, STEPS - 1), 0))

    widths = (WIDTH, WIDTH, QKV, PROBS)
    stage = (N_DEV, NV, 32, WIDTH)
    return pl.pallas_call(
        forward_kernel, grid=(2 * STEPS,), name="forward",
        in_specs=[early(WIDTH)] * 2 + weight_specs(0) + weight_specs(1) + [full((GROUP, 2 * GROUP))] * 2 + [full((ROWS, ROWS))],
        out_specs=[ANY, full((SUM_ROWS + 8, WIDTH))] + [early(w) for w in widths],
        out_shape=[sds((N_DEV, 2) + SWAP[1:], BF16), sds((SUM_ROWS + 8, WIDTH), F32)] + [sds((TOKENS, w), BF16) for w in widths],
        scratch_shapes=[vm(w) for w in (WIDTH, WIDTH, WIDTH, QKV, PROBS, WIDTH, WIDTH, HIDDEN, HIDDEN, WIDTH, QKV, PROBS)]
        + [vm(HIDDEN, F32)] * 2 + [vm(PROBS, F32)] + [pltpu.VMEM(SWAP, BF16)] * 2
        + [pltpu.VMEM((6,) + stage, BF16)] * 2 + [pltpu.VMEM((4,) + stage, BF16)] * 2
        + exchange_sems(6) * 2 + exchange_sems(4) * 2,
        compiler_params=params(1), cost_estimate=cost(160, 60),
    )(x, dy, *weights, *weights, bias_s, bias_t, perm)


def spatial_backward_call(back, x, saved, weights, perm, sum_t):
    def early(width):
        return pl.BlockSpec((STEP_ROWS, width), lambda i: (jnp.minimum(i, STEPS - 1), 0))

    def late(width):
        return pl.BlockSpec((STEP_ROWS, width), lambda i: (jnp.maximum(i - STEPS, 0), 0))

    grads = GRADS
    return pl.pallas_call(
        spatial_backward_kernel, grid=(2 * STEPS,), name="spatial_bwd",
        in_specs=[pl.BlockSpec((N_DEV, None, NV, 32, WIDTH), lambda i: (0, 1, jnp.minimum(i, STEPS - 1), 0, 0))]
        + [late(WIDTH), early(WIDTH), early(WIDTH), late(QKV), late(PROBS)] + weight_specs(0) + [full((ROWS, ROWS)), ANY],
        out_specs=[late(WIDTH)] + [ANY] * 4 + [full((2, 4, WIDTH))],
        out_shape=[sds((TOKENS, WIDTH), BF16)] + [sds(g, F32) for g in grads] + [sds((2, 4, WIDTH), F32)],
        scratch_shapes=[vm(w) for w in (WIDTH, WIDTH, WIDTH, HIDDEN, HIDDEN, WIDTH, QKV, PROBS)] + [vm(HIDDEN, F32)] * 2
        + [pltpu.VMEM((TOKENS, WIDTH), BF16)] * 2
        + [pltpu.VMEM((SUM_ROWS, WIDTH), F32)] * 2 + [pltpu.VMEM((LAPS * SLOTS * BLOCK, WIDTH), F32)] * 2
        + [pltpu.VMEM((8, WIDTH), F32), pltpu.VMEM((N_DEV, 16, WIDTH), F32)]
        + [pltpu.SemaphoreType.DMA((2, 6, LAPS, 2))] * 2 + [pltpu.SemaphoreType.REGULAR((3, LAPS, 2))] * 2
        + [pltpu.SemaphoreType.DMA((12,))] * 2 + [pltpu.SemaphoreType.DMA((2, N_DEV)), pltpu.SemaphoreType.DMA((2,))],
        compiler_params=params(3), cost_estimate=cost(160, 60),
    )(back, x, *saved, *weights, perm, sum_t)


def finish_call(back, perm, dx, grads, g_ln):
    flat = [g.reshape(-1, g.shape[-1]) for g in grads]
    parts = [pl.BlockSpec((g.shape[0] // VIDEOS, g.shape[1]), lambda i: (i, 0)) for g in flat]
    video = pl.BlockSpec((ROWS, WIDTH), lambda i: (i, 0))
    ln_spec = pl.BlockSpec((2, 4, WIDTH), lambda i: (0, 0, 0))
    y, dx, *flat, g_ln = pl.pallas_call(
        finish_kernel, grid=(VIDEOS,), name="finish",
        in_specs=[pl.BlockSpec((N_DEV, None, None, 32, WIDTH), lambda i: (0, 0, i, 0, 0)), full((ROWS, ROWS)), video]
        + parts + [ln_spec],
        out_specs=[video] * 2 + parts + [ln_spec],
        out_shape=[sds((TOKENS, WIDTH), BF16)] * 2 + [sds(g.shape, F32) for g in flat] + [sds((2, 4, WIDTH), F32)],
        compiler_params=pltpu.CompilerParams(dimension_semantics=("arbitrary",), vmem_limit_bytes=VMEM_LIMIT),
        cost_estimate=cost(12, 40),
    )(back, perm, dx, *flat, g_ln)
    return y, dx, [f.reshape(g.shape) for f, g in zip(flat, grads)], g_ln


def constants():
    row = np.arange(ROWS)
    dev, patch, frame = row // 32, (row // 8) % 4, row % 8
    perm = np.zeros((ROWS, ROWS), np.float32)
    perm[row, frame * 32 + dev * 4 + patch] = 1.0
    r = np.arange(GROUP)
    frame_of = r // 32
    patch_of = (r // 8) % 2
    bias_s = np.where(frame_of[:, None] == frame_of[None], 0.0, -np.inf).astype(np.float32)
    bias_t = np.where(patch_of[:, None] == patch_of[None], 0.0, -np.inf).astype(np.float32)
    return perm, np.concatenate([bias_s] * 2, 1), np.concatenate([bias_t] * 2, 1)


def device_step(latents, cotangent, ln_params, w_qkv, w_out, w_up, w_down):
    perm, bias_s, bias_t = constants()
    perm = jnp.asarray(perm, BF16)
    bias_s, bias_t = jnp.asarray(bias_s), jnp.asarray(bias_t)
    weights = (ln_params, w_qkv, w_out.reshape(2, WIDTH, WIDTH), w_up, w_down)
    x = latents.reshape(TOKENS, WIDTH)
    dy = cotangent.reshape(TOKENS, WIDTH)

    back, sum_t, *saved = forward_call(x, dy, weights, bias_s, bias_t, perm)
    dx, *grads, g_ln = spatial_backward_call(back, x, saved, weights, perm, sum_t)
    y, dx, (g_qkv, g_out, g_up, g_down), g_ln = finish_call(back, perm, dx, grads, g_ln)
    g_out = g_out.reshape(2, 6, 64, WIDTH)
    shape = latents.shape
    return y.reshape(shape), dx.reshape(shape), g_ln, g_qkv, g_out, g_up, g_down


def solution(mesh):
    act_spec = P('data', 'sp', None, None)
    replicated = P()
    part_spec = P('data')
    return jax.shard_map(device_step, mesh=mesh,
                         in_specs=(act_spec, act_spec, replicated, replicated, replicated, replicated, replicated),
                         out_specs=(act_spec, act_spec, part_spec, part_spec, part_spec, part_spec, part_spec),
                         check_vma=False)
```
